8 devices in a mesh: data: 1 (over z), ys: 2 (over y), xs: 4 (over x, core).
Axes of the slice: x: 2, y: 2, z: 1, core: 2. Of those that a mesh axis runs over, the one named last changes fastest.
Arguments:
- field: float32 [48, 64, 64, 40, 20], P('data', 'xs', 'ys')
- spec_real: float32 [2, 16, 16, 8, 20, 20], replicated
- spec_imag: float32 [2, 16, 16, 8, 20, 20], replicated
- mix_weight: float32 [2, 20, 20], replicated
- bias: float32 [2, 20], replicated
Outputs:
- output: float32 [48, 64, 64, 40, 20], P('data', 'xs', 'ys')
All inputs are finite; a program needn't handle non-finite values.
Results may differ from the reference program's by a relative error of at most 0.001.
Values are sent between devices in bfloat16 or wider.
A program may use at most 1 GiB of HBM per device.

```python
import jax
import jax.numpy as jnp
from jax import lax

PART_BATCH = 48
GRID_X = 64
GRID_Y = 64
GRID_Z = 40
WIDTH = 20
MODES = 8
LAYERS = 2


def spread_modes(kept, first):
    dims = kept.shape
    gap_x = dims[:first] + (GRID_X - 2 * MODES,) + dims[first + 1:]
    full_x = jnp.concatenate([lax.slice_in_dim(kept, 0, MODES, axis=first), jnp.zeros(gap_x, kept.dtype), lax.slice_in_dim(kept, MODES, 2 * MODES, axis=first)], axis=first)
    dims = full_x.shape
    gap_y = dims[:first + 1] + (GRID_Y - 2 * MODES,) + dims[first + 2:]
    full_y = jnp.concatenate([lax.slice_in_dim(full_x, 0, MODES, axis=first + 1), jnp.zeros(gap_y, kept.dtype), lax.slice_in_dim(full_x, MODES, 2 * MODES, axis=first + 1)], axis=first + 1)
    dims = full_y.shape
    gap_z = dims[:first + 2] + (GRID_Z // 2 + 1 - MODES,) + dims[first + 3:]
    return jnp.concatenate([full_y, jnp.zeros(gap_z, kept.dtype)], axis=first + 2)


def setup_inputs(seed: int = 0, part: int = 0) -> dict:
    part_keys = jax.random.split(jax.random.fold_in(jax.random.key(seed), part), 3)
    shared_keys = jax.random.split(jax.random.key(seed + 1), 4)
    kept_shape = (PART_BATCH, 2 * MODES, 2 * MODES, MODES, WIDTH)
    coef_scale = 0.25 * MODES ** -1.5
    kept = lax.complex(jax.random.normal(part_keys[0], kept_shape, jnp.float32), jax.random.normal(part_keys[1], kept_shape, jnp.float32)) * coef_scale
    smooth = jnp.fft.irfftn(spread_modes(kept, 1), s=(GRID_X, GRID_Y, GRID_Z), axes=(1, 2, 3), norm='forward')
    noise = 0.3 * jax.random.normal(part_keys[2], (PART_BATCH, GRID_X, GRID_Y, GRID_Z, WIDTH), jnp.float32)
    kernel_shape = (LAYERS, 2 * MODES, 2 * MODES, MODES, WIDTH, WIDTH)
    kernel_scale = (2.0 * WIDTH) ** -0.5
    return dict(
        field=smooth + noise,
        spec_real=kernel_scale * jax.random.normal(shared_keys[0], kernel_shape, jnp.float32),
        spec_imag=kernel_scale * jax.random.normal(shared_keys[1], kernel_shape, jnp.float32),
        mix_weight=WIDTH ** -0.5 * jax.random.normal(shared_keys[2], (LAYERS, WIDTH, WIDTH), jnp.float32),
        bias=0.5 * jax.random.normal(shared_keys[3], (LAYERS, WIDTH), jnp.float32),
    )


def spectral_conv(sample, kernel):
    spec = jnp.fft.rfftn(sample, axes=(0, 1, 2))
    kept_x = jnp.concatenate([spec[:MODES], spec[GRID_X - MODES:]], axis=0)
    kept = jnp.concatenate([kept_x[:, :MODES], kept_x[:, GRID_Y - MODES:]], axis=1)[:, :, :MODES]
    mixed = jnp.einsum('abci,abcio->abco', kept, kernel)
    return jnp.fft.irfftn(spread_modes(mixed, 0), s=(GRID_X, GRID_Y, GRID_Z), axes=(0, 1, 2))


def reference(field, spec_real, spec_imag, mix_weight, bias):
    def layer_step(carry, weights):
        real_part, imag_part, w_mix, b_vec = weights
        kernel = lax.complex(real_part, imag_part)
        spectral = lax.map(lambda sample: spectral_conv(sample, kernel), carry)
        pointwise = jnp.dot(carry, w_mix, preferred_element_type=jnp.float32)
        return jax.nn.gelu(spectral + pointwise + b_vec, approximate=True), None

    final_field, unused = lax.scan(layer_step, field, (spec_real, spec_imag, mix_weight, bias))
    return final_field
```

```python
import functools
import math

import jax
import jax.numpy as jnp
import ml_dtypes
import numpy as np
from jax import lax
from jax.experimental import pallas as pl
from jax.experimental.pallas import tpu as pltpu
from jax.sharding import PartitionSpec as P

F32 = jnp.float32
BF16 = jnp.bfloat16
VMEM_LIMIT = 64 * 1024 * 1024 - 65536

X_GROUP = 8
Y_BLOCK = 4
Z_BLOCK = 8
KZ_CLASS = ((0, 5), (1, 6, 4), (2, 7, 3))
KZ_ORDER = tuple(kz for group in KZ_CLASS for kz in group)
CLASS_ROWS = (0, 64, 160, 256)
ROOT5_4 = math.sqrt(5.0) / 4.0
SIN_1 = math.sin(2.0 * math.pi / 5.0)
SIN_RATIO = math.sin(4.0 * math.pi / 5.0) / SIN_1


def kz_sign(kz):
    return 0 if kz % 5 == 0 else (1 if kz % 5 < 3 else -1)


def kept(modes, size):
    return np.concatenate([np.arange(modes), np.arange(size - modes, size)])


def pieces(table):
    rest = np.asarray(table, np.float32)
    out = []
    for _ in range(3):
        out.append(rest.astype(ml_dtypes.bfloat16))
        rest = rest - out[-1].astype(np.float32)
    return out


def yz_angles(kz, y_pos, ky, grid_y, grid_z):
    z_pos = np.arange(Z_BLOCK)
    turn = (ky[:, None, None] * y_pos[None, :, None] % grid_y) / grid_y + kz * z_pos[None, None, :] / grid_z
    return 2.0 * math.pi * turn


def forward_table(group, y_pos, ky, grid_y, grid_z):
    rows = []
    for kz in group:
        t, s = yz_angles(kz, y_pos, ky, grid_y, grid_z), kz_sign(kz)
        real, imag = [np.cos(t)], [-np.sin(t)]
        if s:
            real.append(-s * SIN_1 * np.sin(t))
            imag.append(-s * SIN_1 * np.cos(t))
        rows += [np.stack(part, 1).reshape(len(ky), -1) for part in (real, imag)]
    return np.concatenate(rows, 0)


def inverse_table(group, y_pos, ky, grid_y, grid_z, points):
    cols = []
    for kz in group:
        t, s = yz_angles(kz, y_pos, ky, grid_y, grid_z).transpose(1, 2, 0), kz_sign(kz)
        w = (1.0 if kz == 0 else 2.0) / points
        real, imag = [w * np.cos(t)], [-w * np.sin(t)]
        if s:
            real.append(s * SIN_1 * w * np.sin(t))
            imag.append(s * SIN_1 * w * np.cos(t))
        cols += [np.stack(part, 0).reshape(-1, len(ky)) for part in (real, imag)]
    return np.concatenate(cols, 1)


def all_tables(blocks, ky, grid_y, grid_z, points):
    fwd, inv = [[], [], []], [[], [], [], [], []]
    for block in range(blocks):
        y_pos = np.arange(Y_BLOCK) + block * Y_BLOCK
        for k, group in enumerate(KZ_CLASS):
            a, b, c = pieces(forward_table(group, y_pos, ky, grid_y, grid_z))
            n = np.zeros_like(a)
            if k == 0:
                fwd[k].append(np.concatenate([a, a, a, b, b, c], 1))
            else:
                fwd[k].append(np.block([[a, a, a, b], [c, b, n, n]]))
            a, b, c = pieces(inverse_table(group, y_pos, ky, grid_y, grid_z, points))
            n = np.zeros_like(a)
            if k == 0:
                inv[0].append(np.block([[a, a, a], [b, b, n], [c, n, n]]))
            else:
                inv[2 * k - 1].append(np.block([[a, a], [b, b]]))
                inv[2 * k].append(np.concatenate([c, a], 1))
    return [np.stack(t) for t in fwd], [np.stack(t) for t in inv]


def split3(v):
    d1 = v.astype(BF16)
    rest = v - d1.astype(F32)
    d2 = rest.astype(BF16)
    return d1, d2, (rest - d2.astype(F32)).astype(BF16)


def dot(a, b):
    return jnp.dot(a, b, preferred_element_type=F32)


def z_forward(v):
    v0, v1, v2, v3, v4 = v
    t1, t2, e1, e2 = v1 + v4, v2 + v3, v1 - v4, v2 - v3
    total = t1 + t2
    mid, dif = v0 - 0.25 * total, ROOT5_4 * (t1 - t2)
    return v0 + total, mid + dif, e1 + SIN_RATIO * e2, mid - dif, SIN_RATIO * e1 - e2


def z_inverse(a0, a1, b1, a2, b2):
    total = a1 + a2
    mid, dif = a0 - 0.25 * total, ROOT5_4 * (a1 - a2)
    p, q = mid + dif, mid - dif
    r, s = b1 + SIN_RATIO * b2, SIN_RATIO * b1 - b2
    return a0 + total, p - r, q - s, q + s, p + r


def forward_yz(v, tables):
    lanes = v[0].shape[-1]
    chan = [split3(c.reshape(Y_BLOCK * Z_BLOCK, lanes)) for c in z_forward(v)]
    outs = [dot(tables[0], jnp.concatenate([chan[0][i] for i in (0, 1, 2, 0, 1, 0)], 0))]
    for k, (p, q) in ((1, (1, 2)), (2, (3, 4))):
        o = dot(tables[k], jnp.concatenate([chan[c][i] for i in (0, 1, 2, 0) for c in (p, q)], 0))
        half = o.shape[0] // 2
        outs.append(o[:half] + o[half:])
    return outs


def inverse_yz(part, tables):
    n = Y_BLOCK * Z_BLOCK
    o = dot(tables[0], jnp.concatenate([part(i, 0) for i in range(3)], 0))
    chan = [o[:n] + o[n:2 * n] + o[2 * n:]]
    for k in (1, 2):
        d1, d2, d3 = (part(i, k) for i in range(3))
        o = dot(tables[2 * k - 1], jnp.concatenate([d1, d2], 0))
        o = o[:2 * n] + o[2 * n:] + dot(tables[2 * k], jnp.concatenate([d1, d3], 0))
        chan += [o[:n], o[n:]]
    return chan


def gelu(u):
    k = math.sqrt(2.0 / math.pi)
    h = 0.5 * u
    return h + h * jnp.tanh(u * (k + (0.044715 * k) * (u * u)))


def field_lanes(x_ref, y, c):
    return jnp.concatenate([x_ref[x, y, c] for x in range(X_GROUP)], -1)


def zero_spectrum(f_ref):
    def clear(c, _):
        f_ref[c] = jnp.zeros(f_ref.shape[1:], F32)
        return 0
    lax.fori_loop(0, f_ref.shape[0], clear, 0)


def add_spectrum(f_ref, c, outs, unit):
    lanes = f_ref.shape[-1]
    for u in range(unit):
        for k, o in enumerate(outs):
            f_ref[c + u, CLASS_ROWS[k]:CLASS_ROWS[k + 1]] += o[:, u * lanes:(u + 1) * lanes]


def forward_kernel(unit, x_ref, t0, t1, t2, f_ref):
    f_ref = f_ref.at[0]
    width = x_ref.shape[2]

    @pl.when(pl.program_id(1) == 0)
    def _():
        zero_spectrum(f_ref)

    def body(i, _):
        c = i * unit
        rows = [jnp.concatenate([field_lanes(x_ref, y, c + u) for u in range(unit)], -1) for y in range(Y_BLOCK)]
        v = [jnp.stack([r[8 * j:8 * j + 8] for r in rows], 0) for j in range(5)]
        add_spectrum(f_ref, c, forward_yz(v, (t0[0], t1[0], t2[0])), unit)
        return 0
    lax.fori_loop(0, width // unit, body, 0)


def layer_kernel(unit, first, *refs):
    if first:
        bias, x_ref, w_ref, s_ref, *tabs, v_ref, f_hbm, f_ref, sem = refs
    else:
        bias, x_ref, w_ref, s_ref, *tabs, o_ref, v_ref = refs
        x_ref = x_ref.at[0]
    inv = [t[0] for t in tabs[:5]]
    width = w_ref.shape[1] // Z_BLOCK
    lanes = v_ref.shape[-1]
    batch = lanes // X_GROUP
    if first:
        v_ref = v_ref.at[0]

    def channels(y, z):
        if first:
            v = jnp.concatenate([x_ref[x, y, :, z, :] for x in range(X_GROUP)], -1)
        else:
            v = x_ref[y, :, z, :]
        d1, d2, d3 = split3(v.reshape(width * 8, lanes))
        a, b, c = w_ref[0], w_ref[1], w_ref[2]
        p = dot(a, d1) + dot(a, d2) + dot(a, d3) + dot(b, d1) + dot(b, d2) + dot(c, d1)
        v_ref[y, :, z, :] = p.reshape(width, 8, lanes)

    def z_block(j, _):
        for y in range(Y_BLOCK):
            channels(y, pl.ds(pl.multiple_of(j * 8, 8), 8))
        return 0
    lax.fori_loop(0, 5, z_block, 0)

    if first:
        @pl.when(pl.program_id(1) == 0)
        def _():
            zero_spectrum(f_ref)

    pair, per_step = unit

    def inverse(c):
        def part(p, k):
            return jnp.concatenate([s_ref[0, p, c + u, CLASS_ROWS[k]:CLASS_ROWS[k + 1]] for u in range(pair)], -1)
        return inverse_yz(part, inv)

    def finish(c, chan):
        new = []
        for j, s in enumerate(z_inverse(*chan)):
            s = s.reshape(Y_BLOCK, 8, pair * lanes)
            got = []
            for u in range(pair):
                g = gelu(s[..., u * lanes:(u + 1) * lanes] + v_ref[:, c + u, 8 * j:8 * j + 8, :] + bias[c + u])
                if first:
                    v_ref[:, c + u, 8 * j:8 * j + 8, :] = g
                else:
                    for x in range(X_GROUP):
                        o_ref[x, :, c + u, 8 * j:8 * j + 8, :] = g[..., batch * x:batch * (x + 1)]
                got.append(g)
            new.append(jnp.concatenate(got, -1))
        if first:
            add_spectrum(f_ref, c, forward_yz(new, [t[0] for t in tabs[5:]]), pair)

    def body(i, _):
        c = i * per_step
        chan = inverse(c)
        for u in range(0, per_step, pair):
            ahead = inverse(c + u + pair) if u + pair < per_step else None
            finish(c + u, chan)
            chan = ahead
        return 0
    lax.fori_loop(0, width // per_step, body, 0)

    if first:
        @pl.when(pl.program_id(1) == pl.num_programs(1) - 1)
        def _():
            copy = pltpu.make_async_copy(f_ref, f_hbm.at[pl.program_id(0)], sem)
            copy.start()
            copy.wait()


def split_dot(left, right):
    a, b, c = left
    d1, d2, d3 = split3(right)
    return dot(a, d1) + dot(a, d2) + dot(a, d3) + dot(b, d1) + dot(b, d2) + dot(c, d1)


def x_forward_kernel(m_ref, f_ref, s_ref):
    groups, width, lanes = f_ref.shape[0], f_ref.shape[1], f_ref.shape[-1]
    batch = lanes // X_GROUP
    rows = []
    for g in range(groups):
        for x in range(X_GROUP):
            for p in range(2):
                rows.append(jnp.concatenate([f_ref[g, c, 0, p, 0, :, x * batch:(x + 1) * batch] for c in range(width)], -1))
    out = split_dot((m_ref[0], m_ref[1], m_ref[2]), jnp.concatenate(rows, 0))
    s_ref[:, 0] = out.reshape(s_ref.shape[0], 2, 8, width * batch)


def x_inverse_kernel(m_ref, t_ref, s_ref):
    groups, width, lanes = s_ref.shape[0], s_ref.shape[2], s_ref.shape[-1]
    batch = lanes // X_GROUP
    n = t_ref.shape[0]
    right = t_ref[:, 0].reshape(n * 16, width * batch)
    out = split_dot((m_ref[0], m_ref[1], m_ref[2]), right).reshape(groups, X_GROUP, 2, 8, width * batch)
    for g in range(groups):
        for p in range(2):
            for c in range(width):
                row = jnp.concatenate([out[g, x, p, :, c * batch:(c + 1) * batch] for x in range(X_GROUP)], -1)
                for i, d in enumerate(split3(row)):
                    s_ref[g, i, c, 0, p, 0] = d


def mix_kernel(owner, s_ref, r_ref, i_ref, t_ref, rows, re_rows, im_rows, re_s, im_s, re_t, im_t):
    n_ky, width = r_ref.shape[2], r_ref.shape[3]
    slots = s_ref.shape[1]
    lanes = s_ref.shape[-1]
    batch = lanes // width
    modes = slots * n_ky

    for w_ref, out in ((r_ref, re_rows), (i_ref, im_rows)):
        def lay(c, _):
            for ky in range(n_ky):
                rows[ky * 8:ky * 8 + 8, 0:width] = w_ref[0, 0, ky, c]
            mat = jnp.concatenate([rows[pl.ds(h * 64 + kz, 8, stride=8), :] for kz in KZ_ORDER for h in range(n_ky // 8)], 0)
            out[c] = mat.T[0:24]
            return 0
        lax.fori_loop(0, width, lay, 0)
    re_s[...] = s_ref[0, :, 0].reshape(modes, lanes).T
    im_s[...] = s_ref[0, :, 1].reshape(modes, lanes).T

    pair = 2

    def outputs(i, _):
        d = i * pair

        def inner(c, acc):
            at = pl.ds(pl.multiple_of(c * batch, 8), batch)
            a, b = re_s[at, :], im_s[at, :]
            new = []
            for u in range(pair):
                p = jnp.broadcast_to(re_rows[c, pl.ds(d + u, 1), :], a.shape)
                q = jnp.broadcast_to(im_rows[c, pl.ds(d + u, 1), :], a.shape)
                new += [acc[2 * u] + (a * p - b * q), acc[2 * u + 1] + (a * q + b * p)]
            return tuple(new)
        zero = jnp.zeros((batch, modes), F32)
        acc = lax.fori_loop(0, width, inner, (zero,) * (2 * pair))
        for u in range(pair):
            at = pl.ds(pl.multiple_of((d + u) * batch, 8), batch)
            re_t[at, :] = acc[2 * u]
            im_t[at, :] = acc[2 * u + 1]
        return 0
    lax.fori_loop(0, width // pair, outputs, 0)
    t_ref[0, :, 0] = re_t[...].T.reshape(slots, n_ky, lanes)
    t_ref[0, :, 1] = im_t[...].T.reshape(slots, n_ky, lanes)


class Place:
    def __init__(self):
        xs, ys = lax.axis_index('xs'), lax.axis_index('ys')
        data = lax.axis_index('data')
        c, x, y = xs % 2, xs // 2, ys
        self.core = (data, ys, 2 * x + 1 - c)
        self.x_chip = (data, ys, 2 * (1 - x) + c)
        self.y_chip = (data, 1 - ys, xs)
        p, q = lambda a, b: 2 * a + b, lambda a, b: 4 + 2 * a + b
        self.mine, self.theirs = 8 * c, 8 * (1 - c)
        self.order = (p(1 - x, 1 - y), q(1 - y, 1 - x), p(1 - x, y), q(1 - y, x),
                      p(x, 1 - y), q(y, 1 - x), p(x, y), q(y, x))

    def enter(self):
        barrier = pltpu.get_barrier_semaphore()
        for device in (self.core, self.x_chip, self.y_chip):
            pl.semaphore_signal(barrier, inc=1, device_id=device, device_id_type=pl.DeviceIdType.MESH)
        pl.semaphore_wait(barrier, 3)


def remote(src, dst, send, recv, device):
    return pltpu.make_async_remote_copy(src_ref=src, dst_ref=dst, send_sem=send, recv_sem=recv, device_id=device,
                                        device_id_type=pl.DeviceIdType.MESH)


def reduce_kernel(s_hbm, out_ref, acc, r1, r2, r3, local_sem, send1, recv1, send2, recv2, send3, recv3):
    me = Place()
    local = [pltpu.make_async_copy(s_hbm.at[me.mine + me.order[t]], acc.at[t], local_sem.at[t]) for t in range(8)]
    for copy in local:
        copy.start()
    me.enter()
    first = [remote(s_hbm.at[me.theirs + me.order[t]], r1.at[t], send1.at[t], recv1.at[t], me.core) for t in range(8)]
    for copy in first:
        copy.start()
    slots = acc.shape[1]

    def add(dst, a, b):
        def row(i, _):
            dst[i] = a[i] + b[i]
            return 0
        lax.fori_loop(0, slots, row, 0)

    second = []
    for t in range(8):
        local[t].wait()
        first[t].wait_recv()
        add(acc.at[t], acc.at[t], r1.at[t])
        if t < 4:
            copy = remote(acc.at[t], r2.at[t], send2.at[t], recv2.at[t], (me.x_chip, me.y_chip)[t % 2])
            copy.start()
            second.append(copy)
    third = []
    for t in range(4):
        second[t].wait_recv()
        add(acc.at[4 + t], acc.at[4 + t], r2.at[t])
        if t < 2:
            copy = remote(acc.at[4 + t], r3.at[t], send3.at[t], recv3.at[t], (me.y_chip, me.x_chip)[t])
            copy.start()
            third.append(copy)
    for t in range(2):
        third[t].wait_recv()
        add(out_ref.at[t], acc.at[6 + t], r3.at[t])
    for copy in first + second + third:
        copy.wait_send()


def gather_kernel(t_ref, out, local_sem, send, recv):
    me = Place()
    p3, q3, p2, q2, p1, q1, p0, q0 = (me.mine + o for o in me.order)
    local = [pltpu.make_async_copy(t_ref.at[i], out.at[k], local_sem.at[i]) for i, k in enumerate((p0, q0))]
    for copy in local:
        copy.start()
    me.enter()
    count = [0]

    def push(src, k, device):
        n = count[0]
        count[0] += 1
        copy = remote(src, out.at[k], send.at[n], recv.at[n], device)
        copy.start()
        return copy
    a = push(t_ref.at[0], p0, me.y_chip)
    b = push(t_ref.at[1], q0, me.x_chip)
    c = push(t_ref.at[0], p0, me.x_chip)
    d = push(t_ref.at[1], q0, me.y_chip)
    sent = [a, b, c, d, push(t_ref.at[0], p0, me.core), push(t_ref.at[1], q0, me.core)]
    core = sent[4:]
    a.wait_recv()
    e = push(out.at[p1], p1, me.x_chip)
    b.wait_recv()
    f = push(out.at[q1], q1, me.y_chip)
    sent += [e, f]
    late = [push(out.at[p1], p1, me.core), push(out.at[q1], q1, me.core)]
    for copy, k in ((c, p2), (d, q2), (e, p3), (f, q3)):
        copy.wait_recv()
        late.append(push(out.at[k], k, me.core))
    for copy in core + late:
        copy.wait_recv()
    for copy in sent + late:
        copy.wait_send()
    for copy in local:
        copy.wait()


def block(shape, index, **kwargs):
    def index_map(*at):
        return tuple(0 if k == 'o' else at['ij'.index(k)] for k in index)
    return pl.BlockSpec(shape, index_map, **kwargs)


def bf16_addends(table):
    out = []
    for _ in range(3):
        out.append(lax.reduce_precision(table, exponent_bits=8, mantissa_bits=7))
        table = table - out[-1]
    return jnp.stack(out).astype(BF16)


def solution(mesh):
    row_devs, col_devs = mesh.shape['ys'], mesh.shape['xs']

    def local_layers(field, spec_real, spec_imag, mix_weight, bias):
        batch, x_loc, y_loc, grid_z, width = field.shape
        modes = spec_real.shape[3]
        grid_x, grid_y = x_loc * col_devs, y_loc * row_devs
        groups, blocks = x_loc // X_GROUP, y_loc // Y_BLOCK
        lanes = X_GROUP * batch
        kx, ky = kept(modes, grid_x), kept(modes, grid_y)
        n_kx, n_ky = len(kx), len(ky)
        x_index, y_index = lax.axis_index('xs'), lax.axis_index('ys')
        fwd_np, inv_np = all_tables(blocks, ky, grid_y, grid_z, grid_x * grid_y * grid_z)
        fwd, inv = [jnp.asarray(t) for t in fwd_np], [jnp.asarray(t) for t in inv_np]

        turn = 2.0 * math.pi * (kx[:, None] * np.arange(grid_x)[None, :] % grid_x) / grid_x
        cos, sin = np.cos(turn), np.sin(turn)
        fwd_x = np.stack([np.stack([cos, sin], -1), np.stack([-sin, cos], -1)], 1)
        inv_x = np.transpose(fwd_x, (2, 3, 0, 1))
        fwd_x = fwd_x.reshape(n_kx, 2, col_devs, x_loc, 2).transpose(2, 0, 1, 3, 4).reshape(col_devs, 2 * n_kx, 2 * x_loc)
        inv_x = inv_x.reshape(col_devs, 2 * x_loc, 2 * n_kx)
        odd = (jnp.arange(16 * x_loc) % 2 * y_index)[:, None]

        def x_table(tables):
            wide = np.kron(tables, np.eye(8)).astype(np.float32)
            t = lax.dynamic_index_in_dim(jnp.asarray(wide), x_index, 0, keepdims=False)
            return bf16_addends(jnp.where(odd == 1, -t, t))
        fwd_x, inv_x = x_table(fwd_x), x_table(inv_x)
        eye = jnp.eye(Z_BLOCK, dtype=F32)
        point_w = [bf16_addends((mix_weight[layer].T[:, None, :, None] * eye[None, :, None, :]).reshape(width * 8, width * 8))
                   for layer in range(2)]

        real_w, imag_w = (jnp.transpose(w, (0, 1, 2, 4, 3, 5)) for w in (spec_real, spec_imag))
        v = jnp.transpose(field, (1, 2, 4, 3, 0))
        grid = (groups, blocks)
        params = pltpu.CompilerParams(vmem_limit_bytes=VMEM_LIMIT)
        one = pl.Buffered(1)
        spec_shape = jax.ShapeDtypeStruct((groups, width, 256, lanes), F32)
        in_block = block((X_GROUP, Y_BLOCK, width, grid_z, batch), 'ijooo')
        mid_block = block((1, Y_BLOCK, width, grid_z, lanes), 'ijooo')
        part_block = block((1, 3, width, 256, lanes), 'ioooo', pipeline_mode=one)
        w_block = block((3, width * 8, width * 8), 'ooo')

        def table_specs(tables):
            return [block((1,) + t.shape[1:], 'joo') for t in tables]

        f = pl.pallas_call(
            functools.partial(forward_kernel, 4), grid=grid, out_shape=spec_shape,
            in_specs=[in_block] + table_specs(fwd),
            out_specs=block((1, width, 256, lanes), 'iooo'),
            compiler_params=params, name='forward')(v, *fwd)

        own = 2
        core, x_chip = x_index % 2, x_index // 2
        owner = jnp.stack([8 * core + 2 * x_chip + y_index, 8 * core + 4 + 2 * y_index + x_chip]).astype(jnp.int32)
        full = (n_kx, 8, 2, n_ky, width * batch)

        def across(f, layer):
            s = pl.pallas_call(
                x_forward_kernel, grid=(8, n_ky // 8), out_shape=jax.ShapeDtypeStruct(full, F32),
                in_specs=[block((3, 256, 256), 'ooo'),
                          block((groups, width, 1, 2, 1, 8, lanes), 'ooiojoo')],
                out_specs=block((n_kx, 1, 2, 8, width * batch), 'oiojo'),
                compiler_params=params, name='x_forward')(
                    fwd_x, f.reshape(groups, width, 8, 2, n_ky // 8, 8, lanes))
            unit = full[1:]
            s = pl.pallas_call(
                reduce_kernel, out_shape=jax.ShapeDtypeStruct((own,) + unit, F32),
                in_specs=[pl.BlockSpec(memory_space=pl.ANY)], out_specs=pl.BlockSpec(memory_space=pltpu.VMEM),
                scratch_shapes=[pltpu.VMEM((n,) + unit, F32) for n in (8, 8, 4, 2)]
                + [pltpu.SemaphoreType.DMA((n,)) for n in (8, 8, 8, 4, 4, 2, 2)],
                compiler_params=pltpu.CompilerParams(
                    vmem_limit_bytes=VMEM_LIMIT, collective_id=2 * layer, has_side_effects=True), name='reduce')(s)
            r_spec = pl.BlockSpec((1, 1, n_ky, width, 8, width), lambda i, o: (layer, o[i], 0, 0, 0, 0))
            s_spec = block((1,) + full[1:], 'ioooo')
            t = pl.pallas_call(
                mix_kernel, out_shape=jax.ShapeDtypeStruct((own,) + full[1:], F32),
                grid_spec=pltpu.PrefetchScalarGridSpec(
                    num_scalar_prefetch=1, grid=(own,), in_specs=[s_spec, r_spec, r_spec], out_specs=s_spec,
                    scratch_shapes=[pltpu.VMEM((n_ky * 8, 128), F32)] + [pltpu.VMEM((width, 24, 128), F32)] * 2
                    + [pltpu.VMEM((width * batch, 8 * n_ky), F32)] * 4),
                compiler_params=params, name='mix')(owner, s, real_w, imag_w)
            t = pl.pallas_call(
                gather_kernel, out_shape=jax.ShapeDtypeStruct(full, F32),
                in_specs=[pl.BlockSpec(memory_space=pltpu.VMEM)], out_specs=pl.BlockSpec(memory_space=pl.ANY),
                scratch_shapes=[pltpu.SemaphoreType.DMA((2,)), pltpu.SemaphoreType.DMA((14,)), pltpu.SemaphoreType.DMA((14,))],
                compiler_params=pltpu.CompilerParams(
                    vmem_limit_bytes=VMEM_LIMIT, collective_id=2 * layer + 1, has_side_effects=True), name='gather')(t)
            parts = pl.pallas_call(
                x_inverse_kernel, grid=(8, n_ky // 8),
                out_shape=jax.ShapeDtypeStruct((groups, 3, width, 8, 2, n_ky // 8, 8, lanes), BF16),
                in_specs=[block((3, 256, 256), 'ooo'),
                          block((n_kx, 1, 2, 8, width * batch), 'oiojo')],
                out_specs=block((groups, 3, width, 1, 2, 1, 8, lanes), 'oooiojoo'),
                compiler_params=params, name='x_inverse')(inv_x, t)
            return parts.reshape(groups, 3, width, 256, lanes)

        smem = pl.BlockSpec(memory_space=pltpu.SMEM)
        parts = across(f, 0)
        v1, f = pl.pallas_call(
            functools.partial(layer_kernel, (2, 10), True), grid=grid,
            out_shape=(jax.ShapeDtypeStruct((groups, y_loc, width, grid_z, lanes), F32), spec_shape),
            in_specs=[smem, in_block, w_block, part_block] + table_specs(inv) + table_specs(fwd),
            out_specs=(mid_block, pl.BlockSpec(memory_space=pl.ANY)),
            scratch_shapes=[pltpu.VMEM((width, 256, lanes), F32), pltpu.SemaphoreType.DMA],
            compiler_params=params, name='layer_first')(bias[0], v, point_w[0], parts, *inv, *fwd)
        parts = across(f, 1)
        out = pl.pallas_call(
            functools.partial(layer_kernel, (1, 10), False), grid=grid,
            out_shape=jax.ShapeDtypeStruct((x_loc, y_loc, width, grid_z, batch), F32),
            in_specs=[smem, mid_block, w_block, part_block] + table_specs(inv),
            out_specs=in_block,
            scratch_shapes=[pltpu.VMEM((Y_BLOCK, width, grid_z, lanes), F32)],
            compiler_params=params, name='layer_last')(bias[1], v1, point_w[1], parts, *inv)
        return jnp.transpose(out, (4, 0, 1, 3, 2))

    field_spec = P('data', 'xs', 'ys', None, None)
    return jax.shard_map(local_layers, mesh=mesh, in_specs=(field_spec, P(), P(), P(), P()), out_specs=field_spec, check_vma=False)
```

```python
import functools
import math

import jax
import jax.numpy as jnp
import ml_dtypes
import numpy as np
from jax import lax
from jax.experimental import pallas as pl
from jax.experimental.pallas import tpu as pltpu
from jax.sharding import PartitionSpec as P

F32 = jnp.float32
BF16 = jnp.bfloat16
VMEM_LIMIT = 64 * 1024 * 1024 - 65536

SUB = 8
X_GROUP = 8
Y_BLOCK = 4
HALF_BLOCK = 2
Z_BLOCK = 8
KZ_CLASS = ((0, 5), (1, 6, 4), (2, 7, 3))
KZ_ORDER = tuple(kz for group in KZ_CLASS for kz in group)
CLASS_ROWS = (0, 64, 160, 256)
ROOT5_4 = math.sqrt(5.0) / 4.0
SIN_1 = math.sin(2.0 * math.pi / 5.0)
SIN_RATIO = math.sin(4.0 * math.pi / 5.0) / SIN_1


def kz_sign(kz):
    return 0 if kz % 5 == 0 else (1 if kz % 5 < 3 else -1)


def kept(modes, size):
    return np.concatenate([np.arange(modes), np.arange(size - modes, size)])


def pieces(table):
    rest = np.asarray(table, np.float32)
    out = []
    for _ in range(3):
        out.append(rest.astype(ml_dtypes.bfloat16))
        rest = rest - out[-1].astype(np.float32)
    return out


def yz_angles(kz, y_pos, ky, grid_y, grid_z):
    z_pos = np.arange(Z_BLOCK)
    turn = (ky[:, None, None] * y_pos[None, :, None] % grid_y) / grid_y + kz * z_pos[None, None, :] / grid_z
    return 2.0 * math.pi * turn


def forward_table(group, y_pos, ky, grid_y, grid_z):
    rows = []
    for kz in group:
        t, s = yz_angles(kz, y_pos, ky, grid_y, grid_z), kz_sign(kz)
        real, imag = [np.cos(t)], [-np.sin(t)]
        if s:
            real.append(-s * SIN_1 * np.sin(t))
            imag.append(-s * SIN_1 * np.cos(t))
        rows += [np.stack(part, 1).reshape(len(ky), -1) for part in (real, imag)]
    return np.concatenate(rows, 0)


def inverse_table(group, y_pos, ky, grid_y, grid_z, points):
    cols = []
    for kz in group:
        t, s = yz_angles(kz, y_pos, ky, grid_y, grid_z).transpose(1, 2, 0), kz_sign(kz)
        w = (1.0 if kz == 0 else 2.0) / points
        real, imag = [w * np.cos(t)], [-w * np.sin(t)]
        if s:
            real.append(s * SIN_1 * w * np.sin(t))
            imag.append(s * SIN_1 * w * np.cos(t))
        cols += [np.stack(part, 0).reshape(-1, len(ky)) for part in (real, imag)]
    return np.concatenate(cols, 1)


def all_tables(blocks, ky, grid_y, grid_z, points):
    fwd, inv = [[], [], []], [[], [], [], [], []]
    for block in range(blocks):
        y_pos = np.arange(Y_BLOCK) + block * Y_BLOCK
        for k, group in enumerate(KZ_CLASS):
            a, b, c = pieces(forward_table(group, y_pos, ky, grid_y, grid_z))
            n = np.zeros_like(a)
            if k == 0:
                fwd[k].append(np.concatenate([a, a, a, b, b, c], 1))
            else:
                fwd[k].append(np.block([[a, a, a, b], [c, b, n, n]]))
            a, b, c = pieces(inverse_table(group, y_pos, ky, grid_y, grid_z, points))
            n = np.zeros_like(a)
            if k == 0:
                inv[0].append(np.block([[a, a, a], [b, b, n], [c, n, n]]))
            else:
                inv[2 * k - 1].append(np.block([[a, a], [b, b]]))
                inv[2 * k].append(np.concatenate([c, a], 1))
    return [np.stack(t) for t in fwd], [np.stack(t) for t in inv]


def split3(v):
    d1 = v.astype(BF16)
    rest = v - d1.astype(F32)
    d2 = rest.astype(BF16)
    return d1, d2, (rest - d2.astype(F32)).astype(BF16)


def dot(a, b):
    return jnp.dot(a, b, preferred_element_type=F32)


def z_forward(v):
    v0, v1, v2, v3, v4 = v
    t1, t2, e1, e2 = v1 + v4, v2 + v3, v1 - v4, v2 - v3
    total = t1 + t2
    mid, dif = v0 - 0.25 * total, ROOT5_4 * (t1 - t2)
    return v0 + total, mid + dif, e1 + SIN_RATIO * e2, mid - dif, SIN_RATIO * e1 - e2


def z_inverse(a0, a1, b1, a2, b2):
    total = a1 + a2
    mid, dif = a0 - 0.25 * total, ROOT5_4 * (a1 - a2)
    p, q = mid + dif, mid - dif
    r, s = b1 + SIN_RATIO * b2, SIN_RATIO * b1 - b2
    return a0 + total, p - r, q - s, q + s, p + r


def forward_yz(v, tables):
    lanes = v[0].shape[-1]
    chan = [split3(c.reshape(Y_BLOCK * Z_BLOCK, lanes)) for c in z_forward(v)]
    outs = [dot(tables[0], jnp.concatenate([chan[0][i] for i in (0, 1, 2, 0, 1, 0)], 0))]
    for k, (p, q) in ((1, (1, 2)), (2, (3, 4))):
        o = dot(tables[k], jnp.concatenate([chan[c][i] for i in (0, 1, 2, 0) for c in (p, q)], 0))
        half = o.shape[0] // 2
        outs.append(o[:half] + o[half:])
    return outs


def inverse_yz(part, tables):
    n = Y_BLOCK * Z_BLOCK
    o = dot(tables[0], jnp.concatenate([part(i, 0) for i in range(3)], 0))
    chan = [o[:n] + o[n:2 * n] + o[2 * n:]]
    for k in (1, 2):
        d1, d2, d3 = (part(i, k) for i in range(3))
        o = dot(tables[2 * k - 1], jnp.concatenate([d1, d2], 0))
        o = o[:2 * n] + o[2 * n:] + dot(tables[2 * k], jnp.concatenate([d1, d3], 0))
        chan += [o[:n], o[n:]]
    return chan


def gelu(u):
    k = math.sqrt(2.0 / math.pi)
    h = 0.5 * u
    return h + h * jnp.tanh(u * (k + (0.044715 * k) * (u * u)))


def field_lanes(x_ref, y, c):
    return jnp.concatenate([x_ref[x, y, c] for x in range(X_GROUP)], -1)


def zero_spectrum(f_ref):
    def clear(c, _):
        f_ref[c] = jnp.zeros(f_ref.shape[1:], F32)
        return 0
    lax.fori_loop(0, f_ref.shape[0], clear, 0)


def add_spectrum(f_ref, c, outs, unit):
    lanes = f_ref.shape[-1]
    for u in range(unit):
        for k, o in enumerate(outs):
            f_ref[c + u, CLASS_ROWS[k]:CLASS_ROWS[k + 1]] += o[:, u * lanes:(u + 1) * lanes]


def forward_kernel(unit, x_ref, t0, t1, t2, f_ref):
    f_ref = f_ref.at[0]
    width = x_ref.shape[2]

    @pl.when(pl.program_id(1) == 0)
    def _():
        zero_spectrum(f_ref)

    def body(i, _):
        c = i * unit
        rows = [jnp.concatenate([field_lanes(x_ref, y, c + u) for u in range(unit)], -1) for y in range(Y_BLOCK)]
        v = [jnp.stack([r[SUB * j:SUB * j + SUB] for r in rows], 0) for j in range(5)]
        add_spectrum(f_ref, c, forward_yz(v, (t0[0], t1[0], t2[0])), unit)
        return 0
    lax.fori_loop(0, width // unit, body, 0)


def channel_product(first, x_ref, w_ref, p_ref):
    blocks, width, _, lanes = p_ref.shape

    def z_block(j, _):
        z = pl.ds(pl.multiple_of(j * SUB, SUB), SUB)
        for y in range(blocks):
            if first:
                v = jnp.concatenate([x_ref[x, y, :, z, :] for x in range(X_GROUP)], -1)
            else:
                v = x_ref[0, y, :, z, :]
            p_ref[y, :, z, :] = split_dot((w_ref[0], w_ref[1], w_ref[2]), v.reshape(width * SUB, lanes)).reshape(width, SUB, lanes)
        return 0
    lax.fori_loop(0, p_ref.shape[2] // SUB, z_block, 0)


def layer_kernel(unit, first, *refs):
    bias, p_ref, s_ref, *tabs = refs
    p_ref = p_ref.at[0]
    width, lanes = p_ref.shape[1], p_ref.shape[-1]
    batch = lanes // X_GROUP
    if first:
        *tabs, v_ref, f_hbm, f_ref, sem = tabs
        v_ref = v_ref.at[0]
    else:
        *tabs, o_ref = tabs
    inv = [t[0] for t in tabs[:5]]

    if first:
        @pl.when(pl.program_id(1) == 0)
        def _():
            zero_spectrum(f_ref)

    pair, per_step = unit

    def inverse(c):
        def part(p, k):
            return jnp.concatenate([s_ref[0, p, c + u, CLASS_ROWS[k]:CLASS_ROWS[k + 1]] for u in range(pair)], -1)
        return inverse_yz(part, inv)

    def finish(c, chan):
        new = []
        for j, s in enumerate(z_inverse(*chan)):
            s = s.reshape(Y_BLOCK, SUB, pair * lanes)
            got = []
            for u in range(pair):
                g = gelu(s[..., u * lanes:(u + 1) * lanes] + p_ref[:, c + u, SUB * j:SUB * j + SUB, :] + bias[c + u])
                if first:
                    v_ref[:, c + u, SUB * j:SUB * j + SUB, :] = g
                else:
                    for x in range(X_GROUP):
                        o_ref[x, :, c + u, SUB * j:SUB * j + SUB, :] = g[..., batch * x:batch * (x + 1)]
                got.append(g)
            new.append(jnp.concatenate(got, -1))
        if first:
            add_spectrum(f_ref, c, forward_yz(new, [t[0] for t in tabs[5:]]), pair)

    def body(i, _):
        c = i * per_step
        chan = inverse(c)
        for u in range(0, per_step, pair):
            ahead = inverse(c + u + pair) if u + pair < per_step else None
            finish(c + u, chan)
            chan = ahead
        return 0
    lax.fori_loop(0, width // per_step, body, 0)

    if first:
        @pl.when(pl.program_id(1) == pl.num_programs(1) - 1)
        def _():
            copy = pltpu.make_async_copy(f_ref, f_hbm.at[pl.program_id(0)], sem)
            copy.start()
            copy.wait()


def split_dot(left, right):
    a, b, c = left
    d1, d2, d3 = split3(right)
    return dot(a, d1) + dot(a, d2) + dot(a, d3) + dot(b, d1) + dot(b, d2) + dot(c, d1)


def x_forward_kernel(m_ref, f_ref, s_ref):
    groups, width, lanes = f_ref.shape[0], f_ref.shape[1], f_ref.shape[-1]
    batch = lanes // X_GROUP
    rows = []
    for g in range(groups):
        for x in range(X_GROUP):
            for p in range(2):
                rows.append(jnp.concatenate([f_ref[g, c, 0, p, 0, :, x * batch:(x + 1) * batch] for c in range(width)], -1))
    out = split_dot((m_ref[0], m_ref[1], m_ref[2]), jnp.concatenate(rows, 0))
    s_ref[:, 0] = out.reshape(s_ref.shape[0], 2, SUB, width * batch)


def x_inverse_kernel(m_ref, t_ref, s_ref):
    groups, width, lanes = s_ref.shape[0], s_ref.shape[2], s_ref.shape[-1]
    batch = lanes // X_GROUP
    n = t_ref.shape[0]
    right = t_ref[:, 0].reshape(n * 16, width * batch)
    out = split_dot((m_ref[0], m_ref[1], m_ref[2]), right).reshape(groups, X_GROUP, 2, SUB, width * batch)
    for g in range(groups):
        for p in range(2):
            for c in range(width):
                row = jnp.concatenate([out[g, x, p, :, c * batch:(c + 1) * batch] for x in range(X_GROUP)], -1)
                for i, d in enumerate(split3(row)):
                    s_ref[g, i, c, 0, p, 0] = d


def mix_kernel(owner, s_ref, r_ref, i_ref, t_ref, rows, re_rows, im_rows, re_s, im_s, re_t, im_t):
    n_ky, width = r_ref.shape[2], r_ref.shape[3]
    slots = s_ref.shape[1]
    lanes = s_ref.shape[-1]
    batch = lanes // width
    modes = slots * n_ky

    for w_ref, out in ((r_ref, re_rows), (i_ref, im_rows)):
        def lay(c, _):
            for ky in range(n_ky):
                rows[ky * SUB:ky * SUB + SUB, 0:width] = w_ref[0, 0, ky, c]
            mat = jnp.concatenate([rows[pl.ds(h * 64 + kz, SUB, stride=SUB), :] for kz in KZ_ORDER for h in range(n_ky // SUB)], 0)
            out[c] = mat.T[0:24]
            return 0
        lax.fori_loop(0, width, lay, 0)
    re_s[...] = s_ref[0, :, 0].reshape(modes, lanes).T
    im_s[...] = s_ref[0, :, 1].reshape(modes, lanes).T

    pair = 2

    def outputs(i, _):
        d = i * pair

        def inner(c, acc):
            at = pl.ds(pl.multiple_of(c * batch, SUB), batch)
            a, b = re_s[at, :], im_s[at, :]
            new = []
            for u in range(pair):
                p = jnp.broadcast_to(re_rows[c, pl.ds(d + u, 1), :], a.shape)
                q = jnp.broadcast_to(im_rows[c, pl.ds(d + u, 1), :], a.shape)
                new += [acc[2 * u] + (a * p - b * q), acc[2 * u + 1] + (a * q + b * p)]
            return tuple(new)
        zero = jnp.zeros((batch, modes), F32)
        acc = lax.fori_loop(0, width, inner, (zero,) * (2 * pair))
        for u in range(pair):
            at = pl.ds(pl.multiple_of((d + u) * batch, SUB), batch)
            re_t[at, :] = acc[2 * u]
            im_t[at, :] = acc[2 * u + 1]
        return 0
    lax.fori_loop(0, width // pair, outputs, 0)
    t_ref[0, :, 0] = re_t[...].T.reshape(slots, n_ky, lanes)
    t_ref[0, :, 1] = im_t[...].T.reshape(slots, n_ky, lanes)


class Place:
    def __init__(self):
        xs, ys = lax.axis_index('xs'), lax.axis_index('ys')
        data = lax.axis_index('data')
        c, x, y = xs % 2, xs // 2, ys
        self.core = (data, ys, 2 * x + 1 - c)
        self.x_chip = (data, ys, 2 * (1 - x) + c)
        self.y_chip = (data, 1 - ys, xs)
        p, q = lambda a, b: 2 * a + b, lambda a, b: 4 + 2 * a + b
        self.mine, self.theirs = SUB * c, SUB * (1 - c)
        self.order = (p(1 - x, 1 - y), q(1 - y, 1 - x), p(1 - x, y), q(1 - y, x),
                      p(x, 1 - y), q(y, 1 - x), p(x, y), q(y, x))

    def enter(self):
        barrier = pltpu.get_barrier_semaphore()
        for device in (self.core, self.x_chip, self.y_chip):
            pl.semaphore_signal(barrier, inc=1, device_id=device, device_id_type=pl.DeviceIdType.MESH)
        pl.semaphore_wait(barrier, 3)


def remote(src, dst, send, recv, device):
    return pltpu.make_async_remote_copy(src_ref=src, dst_ref=dst, send_sem=send, recv_sem=recv, device_id=device,
                                        device_id_type=pl.DeviceIdType.MESH)


def reduce_kernel(first, s_hbm, x_ref, w_ref, out_ref, p_ref, acc, r1, r2, r3, local_sem, send1, recv1, send2, recv2, send3, recv3):
    me = Place()
    step, last = pl.program_id(0), pl.num_programs(0) - 1
    local = [pltpu.make_async_copy(s_hbm.at[me.mine + me.order[t]], acc.at[t], local_sem.at[t]) for t in range(SUB)]
    one = [remote(s_hbm.at[me.theirs + me.order[t]], r1.at[t], send1.at[t], recv1.at[t], me.core) for t in range(SUB)]
    two = [remote(acc.at[t], r2.at[t], send2.at[t], recv2.at[t], (me.x_chip, me.y_chip)[t % 2]) for t in range(4)]
    three = [remote(acc.at[4 + t], r3.at[t], send3.at[t], recv3.at[t], (me.y_chip, me.x_chip)[t]) for t in range(2)]

    def add(dst, a, b):
        def row(i, _):
            dst[i] = a[i] + b[i]
            return 0
        lax.fori_loop(0, acc.shape[1], row, 0)

    def from_core(t):
        local[t].wait()
        one[t].wait_recv()
        add(acc.at[t], acc.at[t], r1.at[t])

    def from_chip(t):
        two[t].wait_recv()
        add(acc.at[4 + t], acc.at[4 + t], r2.at[t])

    @pl.when(step == 0)
    def _():
        for copy in local:
            copy.start()
        me.enter()
        for copy in one:
            copy.start()

    @pl.when(step == 1)
    def _():
        for t in range(4):
            from_core(t)
            two[t].start()

    @pl.when(step == 2)
    def _():
        for t in range(4, SUB):
            from_core(t)

    @pl.when(step == last // 2)
    def _():
        for t in range(2):
            from_chip(t)
            three[t].start()

    channel_product(first, x_ref, w_ref, p_ref.at[0])

    @pl.when(step == last)
    def _():
        for t in range(2, 4):
            from_chip(t)
        for t in range(2):
            three[t].wait_recv()
            add(out_ref.at[t], acc.at[6 + t], r3.at[t])
        for copy in one + two + three:
            copy.wait_send()


def gather_kernel(first, t_ref, x_ref, w_ref, p_in, out, p_ref, local_sem, send, recv):
    me = Place()
    step, last = pl.program_id(0), pl.num_programs(0) - 1
    p3, q3, p2, q2, p1, q1, p0, q0 = (me.mine + o for o in me.order)
    own = (t_ref.at[0], t_ref.at[1])
    local = [pltpu.make_async_copy(own[i], out.at[k], local_sem.at[i]) for i, k in enumerate((p0, q0))]
    plan = [(own[0], p0, me.y_chip), (own[1], q0, me.x_chip), (own[0], p0, me.x_chip), (own[1], q0, me.y_chip),
            (own[0], p0, me.core), (own[1], q0, me.core),
            (out.at[p1], p1, me.x_chip), (out.at[q1], q1, me.y_chip)]
    plan += [(out.at[k], k, me.core) for k in (p1, q1, p2, q2, p3, q3)]
    copies = [remote(src, out.at[k], send.at[n], recv.at[n], device) for n, (src, k, device) in enumerate(plan)]

    @pl.when(step == 0)
    def _():
        for copy in local:
            copy.start()
        me.enter()
        for copy in copies[:6]:
            copy.start()

    @pl.when(step == last // 2)
    def _():
        for n in range(2):
            copies[n].wait_recv()
            copies[6 + n].start()
        for n in range(2):
            copies[SUB + n].start()

    channel_product(first, x_ref, w_ref, p_ref.at[0])

    @pl.when(step == last)
    def _():
        for n, arrived in enumerate((2, 3, 6, 7)):
            copies[arrived].wait_recv()
            copies[10 + n].start()
        for n in (4, 5, SUB, 9, 10, 11, 12, 13):
            copies[n].wait_recv()
        for copy in copies:
            copy.wait_send()
        for copy in local:
            copy.wait()


def block(shape, index, **kwargs):
    def index_map(*at):
        return tuple(0 if k == 'o' else at['ij'.index(k)] for k in index)
    return pl.BlockSpec(shape, index_map, **kwargs)


def bf16_addends(table):
    out = []
    for _ in range(3):
        out.append(lax.reduce_precision(table, exponent_bits=SUB, mantissa_bits=7))
        table = table - out[-1]
    return jnp.stack(out).astype(BF16)


def solution(mesh):
    row_devs, col_devs = mesh.shape['ys'], mesh.shape['xs']

    def local_layers(field, spec_real, spec_imag, mix_weight, bias):
        batch, x_loc, y_loc, grid_z, width = field.shape
        modes = spec_real.shape[3]
        grid_x, grid_y = x_loc * col_devs, y_loc * row_devs
        groups, blocks = x_loc // X_GROUP, y_loc // Y_BLOCK
        lanes = X_GROUP * batch
        kx, ky = kept(modes, grid_x), kept(modes, grid_y)
        n_kx, n_ky = len(kx), len(ky)
        x_index, y_index = lax.axis_index('xs'), lax.axis_index('ys')
        fwd_np, inv_np = all_tables(blocks, ky, grid_y, grid_z, grid_x * grid_y * grid_z)
        fwd, inv = [jnp.asarray(t) for t in fwd_np], [jnp.asarray(t) for t in inv_np]

        turn = 2.0 * math.pi * (kx[:, None] * np.arange(grid_x)[None, :] % grid_x) / grid_x
        cos, sin = np.cos(turn), np.sin(turn)
        fwd_x = np.stack([np.stack([cos, sin], -1), np.stack([-sin, cos], -1)], 1)
        inv_x = np.transpose(fwd_x, (2, 3, 0, 1))
        fwd_x = fwd_x.reshape(n_kx, 2, col_devs, x_loc, 2).transpose(2, 0, 1, 3, 4).reshape(col_devs, 2 * n_kx, 2 * x_loc)
        inv_x = inv_x.reshape(col_devs, 2 * x_loc, 2 * n_kx)
        odd = (jnp.arange(16 * x_loc) % 2 * y_index)[:, None]

        def x_table(tables):
            wide = np.kron(tables, np.eye(SUB)).astype(np.float32)
            t = lax.dynamic_index_in_dim(jnp.asarray(wide), x_index, 0, keepdims=False)
            return bf16_addends(jnp.where(odd == 1, -t, t))
        fwd_x, inv_x = x_table(fwd_x), x_table(inv_x)
        eye = jnp.eye(Z_BLOCK, dtype=F32)
        point_w = [bf16_addends((mix_weight[layer].T[:, None, :, None] * eye[None, :, None, :]).reshape(width * SUB, width * SUB))
                   for layer in range(2)]

        real_w, imag_w = (jnp.transpose(w, (0, 1, 2, 4, 3, 5)) for w in (spec_real, spec_imag))
        v = jnp.transpose(field, (1, 2, 4, 3, 0))
        grid = (groups, blocks)
        params = pltpu.CompilerParams(vmem_limit_bytes=VMEM_LIMIT)
        one = pl.Buffered(1)
        spec_shape = jax.ShapeDtypeStruct((groups, width, 256, lanes), F32)
        in_block = block((X_GROUP, Y_BLOCK, width, grid_z, batch), 'ijooo')
        mid_block = block((1, Y_BLOCK, width, grid_z, lanes), 'ijooo')
        part_block = block((1, 3, width, 256, lanes), 'ioooo', pipeline_mode=one)
        mid_shape = jax.ShapeDtypeStruct((groups, y_loc, width, grid_z, lanes), F32)
        steps = y_loc // HALF_BLOCK
        anywhere, vmem = pl.BlockSpec(memory_space=pl.ANY), pl.BlockSpec(memory_space=pltpu.VMEM)
        w_block = block((3, width * SUB, width * SUB), 'ooo')

        def half_block(first, half):
            shape = (HALF_BLOCK, width, grid_z)
            if first:
                return pl.BlockSpec((X_GROUP,) + shape + (batch,), lambda j: (half, j, 0, 0, 0))
            return pl.BlockSpec((1,) + shape + (lanes,), lambda j: (half, j, 0, 0, 0))

        def table_specs(tables):
            return [block((1,) + t.shape[1:], 'joo') for t in tables]

        f = pl.pallas_call(
            functools.partial(forward_kernel, 4), grid=grid, out_shape=spec_shape,
            in_specs=[in_block] + table_specs(fwd),
            out_specs=block((1, width, 256, lanes), 'iooo'),
            compiler_params=params, name='forward')(v, *fwd)

        own = 2
        core, x_chip = x_index % 2, x_index // 2
        owner = jnp.stack([SUB * core + 2 * x_chip + y_index, SUB * core + 4 + 2 * y_index + x_chip]).astype(jnp.int32)
        full = (n_kx, SUB, 2, n_ky, width * batch)

        def across(f, layer, source):
            s = pl.pallas_call(
                x_forward_kernel, grid=(SUB, n_ky // SUB), out_shape=jax.ShapeDtypeStruct(full, F32),
                in_specs=[block((3, 256, 256), 'ooo'),
                          block((groups, width, 1, 2, 1, SUB, lanes), 'ooiojoo')],
                out_specs=block((n_kx, 1, 2, SUB, width * batch), 'oiojo'),
                compiler_params=params, name='x_forward')(
                    fwd_x, f.reshape(groups, width, SUB, 2, n_ky // SUB, SUB, lanes))
            unit = full[1:]
            first = layer == 0
            own_block = block((own,) + unit, 'ooooo')
            s, p = pl.pallas_call(
                functools.partial(reduce_kernel, first), grid=(steps,),
                out_shape=(jax.ShapeDtypeStruct((own,) + unit, F32), mid_shape),
                in_specs=[anywhere, half_block(first, 0), w_block],
                out_specs=(own_block, half_block(False, 0)),
                scratch_shapes=[pltpu.VMEM((n,) + unit, F32) for n in (SUB, SUB, 4, 2)]
                + [pltpu.SemaphoreType.DMA((n,)) for n in (SUB, SUB, SUB, 4, 4, 2, 2)],
                compiler_params=pltpu.CompilerParams(
                    vmem_limit_bytes=VMEM_LIMIT, collective_id=2 * layer, has_side_effects=True),
                name='reduce')(s, source, point_w[layer])
            r_spec = pl.BlockSpec((1, 1, n_ky, width, SUB, width), lambda i, o: (layer, o[i], 0, 0, 0, 0))
            s_spec = block((1,) + full[1:], 'ioooo')
            t = pl.pallas_call(
                mix_kernel, out_shape=jax.ShapeDtypeStruct((own,) + full[1:], F32),
                grid_spec=pltpu.PrefetchScalarGridSpec(
                    num_scalar_prefetch=1, grid=(own,), in_specs=[s_spec, r_spec, r_spec], out_specs=s_spec,
                    scratch_shapes=[pltpu.VMEM((n_ky * SUB, 128), F32)] + [pltpu.VMEM((width, 24, 128), F32)] * 2
                    + [pltpu.VMEM((width * batch, SUB * n_ky), F32)] * 4),
                compiler_params=params, name='mix')(owner, s, real_w, imag_w)
            t, p = pl.pallas_call(
                functools.partial(gather_kernel, first), grid=(steps,),
                out_shape=(jax.ShapeDtypeStruct(full, F32), mid_shape),
                in_specs=[own_block, half_block(first, 1), w_block, anywhere],
                out_specs=(anywhere, half_block(False, 1)), input_output_aliases={3: 1},
                scratch_shapes=[pltpu.SemaphoreType.DMA((2,)), pltpu.SemaphoreType.DMA((14,)), pltpu.SemaphoreType.DMA((14,))],
                compiler_params=pltpu.CompilerParams(
                    vmem_limit_bytes=VMEM_LIMIT, collective_id=2 * layer + 1, has_side_effects=True),
                name='gather')(t, source, point_w[layer], p)
            parts = pl.pallas_call(
                x_inverse_kernel, grid=(SUB, n_ky // SUB),
                out_shape=jax.ShapeDtypeStruct((groups, 3, width, SUB, 2, n_ky // SUB, SUB, lanes), BF16),
                in_specs=[block((3, 256, 256), 'ooo'),
                          block((n_kx, 1, 2, SUB, width * batch), 'oiojo')],
                out_specs=block((groups, 3, width, 1, 2, 1, SUB, lanes), 'oooiojoo'),
                compiler_params=params, name='x_inverse')(inv_x, t)
            return parts.reshape(groups, 3, width, 256, lanes), p

        smem = pl.BlockSpec(memory_space=pltpu.SMEM)
        parts, p = across(f, 0, v)
        v1, f = pl.pallas_call(
            functools.partial(layer_kernel, (2, 10), True), grid=grid, out_shape=(mid_shape, spec_shape),
            in_specs=[smem, mid_block, part_block] + table_specs(inv) + table_specs(fwd),
            out_specs=(mid_block, anywhere),
            scratch_shapes=[pltpu.VMEM((width, 256, lanes), F32), pltpu.SemaphoreType.DMA],
            compiler_params=params, name='layer_first')(bias[0], p, parts, *inv, *fwd)
        parts, p = across(f, 1, v1)
        out = pl.pallas_call(
            functools.partial(layer_kernel, (1, 10), False), grid=grid,
            out_shape=jax.ShapeDtypeStruct((x_loc, y_loc, width, grid_z, batch), F32),
            in_specs=[smem, mid_block, part_block] + table_specs(inv), out_specs=in_block,
            compiler_params=params, name='layer_last')(bias[1], p, parts, *inv)
        return jnp.transpose(out, (4, 0, 1, 3, 2))

    field_spec = P('data', 'xs', 'ys', None, None)
    return jax.shard_map(local_layers, mesh=mesh, in_specs=(field_spec, P(), P(), P(), P()), out_specs=field_spec, check_vma=False)
```

```python
import functools
import math

import jax
import jax.numpy as jnp
import ml_dtypes
import numpy as np
from jax import lax
from jax.experimental import pallas as pl
from jax.experimental.pallas import tpu as pltpu
from jax.sharding import PartitionSpec as P

F32 = jnp.float32
BF16 = jnp.bfloat16
VMEM_LIMIT = 64 * 1024 * 1024 - 65536

SUB = 8
X_GROUP = 8
Y_BLOCK = 4
HALF_BLOCK = 2
Z_BLOCK = 8
KZ_CLASS = ((0, 5), (1, 6, 4), (2, 7, 3))
KZ_ORDER = tuple(kz for group in KZ_CLASS for kz in group)
CLASS_ROWS = (0, 64, 160, 256)
FORWARD_UNIT = (2, 10)
FIRST_UNIT = (2, 10)
LAST_UNIT = (1, 10)
ROOT5_4 = math.sqrt(5.0) / 4.0
SIN_1 = math.sin(2.0 * math.pi / 5.0)
SIN_RATIO = math.sin(4.0 * math.pi / 5.0) / SIN_1


def kz_sign(kz):
    return 0 if kz % 5 == 0 else (1 if kz % 5 < 3 else -1)


def kept(modes, size):
    return np.concatenate([np.arange(modes), np.arange(size - modes, size)])


def pieces(table):
    rest = np.asarray(table, np.float32)
    out = []
    for _ in range(3):
        out.append(rest.astype(ml_dtypes.bfloat16))
        rest = rest - out[-1].astype(np.float32)
    return out


def yz_angles(kz, y_pos, ky, grid_y, grid_z):
    z_pos = np.arange(Z_BLOCK)
    turn = (ky[:, None, None] * y_pos[None, :, None] % grid_y) / grid_y + kz * z_pos[None, None, :] / grid_z
    return 2.0 * math.pi * turn


def forward_table(group, y_pos, ky, grid_y, grid_z):
    rows = []
    for kz in group:
        t, s = yz_angles(kz, y_pos, ky, grid_y, grid_z), kz_sign(kz)
        real, imag = [np.cos(t)], [-np.sin(t)]
        if s:
            real.append(-s * SIN_1 * np.sin(t))
            imag.append(-s * SIN_1 * np.cos(t))
        rows += [np.stack(part, 1).reshape(len(ky), -1) for part in (real, imag)]
    return np.concatenate(rows, 0)


def inverse_table(group, y_pos, ky, grid_y, grid_z, points):
    cols = []
    for kz in group:
        t, s = yz_angles(kz, y_pos, ky, grid_y, grid_z).transpose(1, 2, 0), kz_sign(kz)
        w = (0.5 if kz == 0 else 1.0) / points
        real, imag = [w * np.cos(t)], [-w * np.sin(t)]
        if s:
            real.append(s * SIN_1 * w * np.sin(t))
            imag.append(s * SIN_1 * w * np.cos(t))
        cols += [np.stack(part, 0).reshape(-1, len(ky)) for part in (real, imag)]
    return np.concatenate(cols, 1)


def all_tables(blocks, ky, grid_y, grid_z, points):
    fwd, inv = [[], [], []], [[], [], [], [], []]
    for block in range(blocks):
        y_pos = np.arange(Y_BLOCK) + block * Y_BLOCK
        for k, group in enumerate(KZ_CLASS):
            a, b, c = pieces(forward_table(group, y_pos, ky, grid_y, grid_z))
            n = np.zeros_like(a)
            if k == 0:
                fwd[k].append(np.concatenate([a, a, a, b, b, c], 1))
            else:
                fwd[k].append(np.block([[a, a, a, b], [c, b, n, n]]))
            a, b, c = pieces(inverse_table(group, y_pos, ky, grid_y, grid_z, points))
            n = np.zeros_like(a)
            if k == 0:
                inv[0].append(np.block([[a, a, a], [b, b, n], [c, n, n]]))
            else:
                inv[2 * k - 1].append(np.block([[a, a], [b, b]]))
                inv[2 * k].append(np.concatenate([c, a], 1))
    return [np.stack(t) for t in fwd], [np.stack(t) for t in inv]


def split3(v):
    d1 = v.astype(BF16)
    rest = v - d1.astype(F32)
    d2 = rest.astype(BF16)
    return d1, d2, (rest - d2.astype(F32)).astype(BF16)


def dot(a, b):
    return jnp.dot(a, b, preferred_element_type=F32)


def z_forward(v):
    v0, v1, v2, v3, v4 = v
    t1, t2, e1, e2 = v1 + v4, v2 + v3, v1 - v4, v2 - v3
    total = t1 + t2
    mid, dif = v0 - 0.25 * total, ROOT5_4 * (t1 - t2)
    return v0 + total, mid + dif, e1 + SIN_RATIO * e2, mid - dif, SIN_RATIO * e1 - e2


def z_inverse(a0, a1, b1, a2, b2):
    total = a1 + a2
    mid, dif = a0 - 0.25 * total, ROOT5_4 * (a1 - a2)
    p, q = mid + dif, mid - dif
    r, s = b1 + SIN_RATIO * b2, SIN_RATIO * b1 - b2
    return a0 + total, p - r, q - s, q + s, p + r


def split_tiles(u_ref, channels):
    rows, lanes = u_ref.shape[1:]
    out = [[], [], []]
    for k in channels:
        for r in range(0, rows, 2 * SUB):
            cells = [split3(u_ref[k, r:r + 2 * SUB, lane:lane + 128]) for lane in range(0, lanes, 128)]
            for i in range(3):
                out[i].append(jnp.concatenate([cell[i] for cell in cells], -1))
    return [jnp.concatenate(rows, 0) for rows in out]


def add_tiles(o, n, lanes, first=0):
    for r in range(0, n, SUB):
        for lane in range(0, lanes, 128):
            cells = [o[b + r:b + r + SUB, lane:lane + 128] for b in range(0, o.shape[0], n)]
            yield r, lane, functools.reduce(jnp.add, cells)


def forward_stage(u_ref, tables, f_ref, c, pair):
    lanes = f_ref.shape[-1]
    for k, channels in enumerate(((0,), (1, 2), (3, 4))):
        d = split_tiles(u_ref, channels)
        o = dot(tables[k], jnp.concatenate([d[i] for i in ((0, 1, 2, 0) if k else (0, 1, 2, 0, 1, 0))], 0))
        n = CLASS_ROWS[k + 1] - CLASS_ROWS[k]
        for r, lane, v in add_tiles(o, n, pair * lanes):
            at = (c + lane // lanes, slice(CLASS_ROWS[k] + r, CLASS_ROWS[k] + r + SUB), slice(lane % lanes, lane % lanes + 128))
            f_ref[at] += v


def inverse_stage(s_ref, c, pair, tables, u_ref):
    n, lanes = u_ref.shape[1:]

    def part(i, k):
        return jnp.concatenate([s_ref[0, i, c + u, CLASS_ROWS[k]:CLASS_ROWS[k + 1]] for u in range(pair)], -1)
    o = dot(tables[0], jnp.concatenate([part(i, 0) for i in range(3)], 0))
    for r, lane, v in add_tiles(o, n, lanes):
        u_ref[0, r:r + SUB, lane:lane + 128] = v
    for k in (1, 2):
        d1, d2, d3 = (part(i, k) for i in range(3))
        o = jnp.concatenate([dot(tables[2 * k - 1], jnp.concatenate([d1, d2], 0)),
                             dot(tables[2 * k], jnp.concatenate([d1, d3], 0))], 0)
        for r, lane, v in add_tiles(o, 2 * n, lanes):
            u_ref[2 * k - 1 + r // n, r % n:r % n + SUB, lane:lane + 128] = v


def registers(pair, lanes):
    for u in range(pair):
        for y in range(Y_BLOCK):
            for lane in range(0, lanes, 128):
                yield u, y, lane, (slice(y * SUB, (y + 1) * SUB), slice(u * lanes + lane, u * lanes + lane + 128))


def gelu(h):
    k = 2.0 * math.sqrt(2.0 / math.pi)
    return h + h * jnp.tanh(h * (k + (4.0 * 0.044715 * k) * (h * h)))


def field_lanes(x_ref, y, c):
    return jnp.concatenate([x_ref[x, y, c] for x in range(X_GROUP)], -1)


def zero_spectrum(f_ref):
    def clear(c, _):
        f_ref[c] = jnp.zeros(f_ref.shape[1:], F32)
        return 0
    lax.fori_loop(0, f_ref.shape[0], clear, 0)


def forward_kernel(unit, x_ref, t0, t1, t2, f_ref, u_ref):
    f_ref = f_ref.at[0]
    width, lanes = x_ref.shape[2], f_ref.shape[-1]
    pair, per_step = unit
    tables = (t0[0], t1[0], t2[0])

    @pl.when(pl.program_id(1) == 0)
    def _():
        zero_spectrum(f_ref)

    def load(c, slot):
        for u in range(pair):
            for y in range(Y_BLOCK):
                row = field_lanes(x_ref, y, c + u)
                for k, v in enumerate(z_forward([row[SUB * j:SUB * j + SUB] for j in range(5)])):
                    u_ref[slot, k, y * SUB:(y + 1) * SUB, u * lanes:(u + 1) * lanes] = v

    def body(i, _):
        c = i * per_step
        count = per_step // pair
        for n in range(count + 1):
            if n < count:
                load(c + n * pair, n)
            if n:
                forward_stage(u_ref.at[n - 1], tables, f_ref, c + (n - 1) * pair, pair)
        return 0
    lax.fori_loop(0, width // per_step, body, 0)


def channel_product(first, x_ref, w_ref, b_ref, p_ref):
    blocks, width, _, lanes = p_ref.shape

    def z_block(j, _):
        z = pl.ds(pl.multiple_of(j * SUB, SUB), SUB)
        for y in range(blocks):
            if first:
                v = jnp.concatenate([x_ref[x, y, :, z, :] for x in range(X_GROUP)], -1)
            else:
                v = x_ref[0, y, :, z, :]
            p = split_dot((w_ref[0], w_ref[1], w_ref[2]), v.reshape(width * SUB, lanes))
            for c in range(width):
                p_ref[y, c, z, :] = p[c * SUB:(c + 1) * SUB] + b_ref[c]
        return 0
    lax.fori_loop(0, p_ref.shape[2] // SUB, z_block, 0)


def layer_kernel(unit, first, *refs):
    p_ref, s_ref, *tabs = refs
    p_ref = p_ref.at[0]
    width, lanes = p_ref.shape[1], p_ref.shape[-1]
    batch = lanes // X_GROUP
    if first:
        *tabs, v_ref, f_hbm, a_ref, u_ref, f_ref, sem = tabs
        v_ref = v_ref.at[0]

        @pl.when(pl.program_id(1) == 0)
        def _():
            zero_spectrum(f_ref)
    else:
        *tabs, o_ref, a_ref = tabs
    inv, fwd = [t[0] for t in tabs[:5]], [t[0] for t in tabs[5:]]
    pair, per_step = unit

    def activate(c, slot):
        kept_rows = {}
        for u, y, lane, at in registers(pair, lanes):
            new = []
            for j, s in enumerate(z_inverse(*(a_ref[(slot, k) + at] for k in range(5)))):
                g = gelu(s + p_ref[y, c + u, SUB * j:SUB * j + SUB, lane:lane + 128])
                new.append(g)
                if first:
                    v_ref[y, c + u, SUB * j:SUB * j + SUB, lane:lane + 128] = g
                else:
                    kept_rows[j] = kept_rows.get(j, ()) + (g,)
            if first:
                for k, v in enumerate(z_forward(new)):
                    u_ref[(slot, k) + at] = v
            elif lane + 128 == lanes:
                for j, row in kept_rows.items():
                    store_field(o_ref, y, c + u, SUB * j, row, batch)
                kept_rows = {}

    def body(i, _):
        c = i * per_step
        count = per_step // pair
        for n in range(count + 2):
            if n < count:
                inverse_stage(s_ref, c + n * pair, pair, inv, a_ref.at[n])
            if 0 < n <= count:
                activate(c + (n - 1) * pair, n - 1)
            if first and n > 1:
                forward_stage(u_ref.at[n - 2], fwd, f_ref, c + (n - 2) * pair, pair)
        return 0
    lax.fori_loop(0, width // per_step, body, 0)

    if first:
        @pl.when(pl.program_id(1) == pl.num_programs(1) - 1)
        def _():
            copy = pltpu.make_async_copy(f_ref, f_hbm.at[pl.program_id(0)], sem)
            copy.start()
            copy.wait()


def store_field(o_ref, y, c, z, row, batch):
    lane = lax.broadcasted_iota(jnp.int32, row[0].shape, 1)
    for x in range(X_GROUP):
        at, off = divmod(x * batch, 128)
        piece = row[at]
        if off + batch > 128:
            piece = jnp.where(lane < off, row[at + 1], piece)
        if off:
            piece = pltpu.roll(piece, 128 - off, 1)
        o_ref[x, y, c, z:z + SUB, :] = piece[:, :batch]


def split_dot(left, right):
    a, b, c = left
    d1, d2, d3 = split3(right)
    return dot(a, d1) + dot(a, d2) + dot(a, d3) + dot(b, d1) + dot(b, d2) + dot(c, d1)


def x_forward_kernel(m_ref, f_ref, s_ref):
    groups, width, lanes = f_ref.shape[0], f_ref.shape[1], f_ref.shape[-1]
    batch = lanes // X_GROUP
    rows = []
    for g in range(groups):
        for x in range(X_GROUP):
            for p in range(2):
                rows.append(jnp.concatenate([f_ref[g, c, 0, p, 0, :, x * batch:(x + 1) * batch] for c in range(width)], -1))
    out = split_dot((m_ref[0], m_ref[1], m_ref[2]), jnp.concatenate(rows, 0))
    s_ref[:, 0] = out.reshape(s_ref.shape[0], 2, SUB, width * batch)


def x_inverse_kernel(m_ref, t_ref, s_ref):
    groups, width, lanes = s_ref.shape[0], s_ref.shape[2], s_ref.shape[-1]
    batch = lanes // X_GROUP
    n = t_ref.shape[0]
    right = t_ref[:, 0].reshape(n * 16, width * batch)
    out = split_dot((m_ref[0], m_ref[1], m_ref[2]), right).reshape(groups, X_GROUP, 2, SUB, width * batch)
    for g in range(groups):
        for p in range(2):
            for c in range(width):
                row = jnp.concatenate([out[g, x, p, :, c * batch:(c + 1) * batch] for x in range(X_GROUP)], -1)
                for i, d in enumerate(split3(row)):
                    s_ref[g, i, c, 0, p, 0] = d


def mix_kernel(owner, s_ref, r_ref, i_ref, t_ref, rows, re_rows, im_rows, re_s, im_s, re_t, im_t):
    n_ky, width = r_ref.shape[2], r_ref.shape[3]
    slots = s_ref.shape[1]
    lanes = s_ref.shape[-1]
    batch = lanes // width
    modes = slots * n_ky

    for w_ref, out in ((r_ref, re_rows), (i_ref, im_rows)):
        def lay(c, _):
            for ky in range(n_ky):
                rows[ky * SUB:ky * SUB + SUB, 0:width] = w_ref[0, 0, ky, c]
            mat = jnp.concatenate([rows[pl.ds(h * 64 + kz, SUB, stride=SUB), :] for kz in KZ_ORDER for h in range(n_ky // SUB)], 0)
            out[c] = mat.T[0:24]
            return 0
        lax.fori_loop(0, width, lay, 0)
    re_s[...] = s_ref[0, :, 0].reshape(modes, lanes).T
    im_s[...] = s_ref[0, :, 1].reshape(modes, lanes).T

    pair = 2

    def outputs(i, _):
        d = i * pair

        def inner(c, acc):
            at = pl.ds(pl.multiple_of(c * batch, SUB), batch)
            a, b = re_s[at, :], im_s[at, :]
            new = []
            for u in range(pair):
                p = jnp.broadcast_to(re_rows[c, pl.ds(d + u, 1), :], a.shape)
                q = jnp.broadcast_to(im_rows[c, pl.ds(d + u, 1), :], a.shape)
                new += [acc[2 * u] + (a * p - b * q), acc[2 * u + 1] + (a * q + b * p)]
            return tuple(new)
        zero = jnp.zeros((batch, modes), F32)
        acc = lax.fori_loop(0, width, inner, (zero,) * (2 * pair))
        for u in range(pair):
            at = pl.ds(pl.multiple_of((d + u) * batch, SUB), batch)
            re_t[at, :] = acc[2 * u]
            im_t[at, :] = acc[2 * u + 1]
        return 0
    lax.fori_loop(0, width // pair, outputs, 0)
    t_ref[0, :, 0] = re_t[...].T.reshape(slots, n_ky, lanes)
    t_ref[0, :, 1] = im_t[...].T.reshape(slots, n_ky, lanes)


class Place:
    def __init__(self):
        xs, ys = lax.axis_index('xs'), lax.axis_index('ys')
        data = lax.axis_index('data')
        c, x, y = xs % 2, xs // 2, ys
        self.core = (data, ys, 2 * x + 1 - c)
        self.x_chip = (data, ys, 2 * (1 - x) + c)
        self.y_chip = (data, 1 - ys, xs)
        p, q = lambda a, b: 2 * a + b, lambda a, b: 4 + 2 * a + b
        self.mine, self.theirs = SUB * c, SUB * (1 - c)
        self.order = (p(1 - x, 1 - y), q(1 - y, 1 - x), p(1 - x, y), q(1 - y, x),
                      p(x, 1 - y), q(y, 1 - x), p(x, y), q(y, x))

    def enter(self):
        barrier = pltpu.get_barrier_semaphore()
        for device in (self.core, self.x_chip, self.y_chip):
            pl.semaphore_signal(barrier, inc=1, device_id=device, device_id_type=pl.DeviceIdType.MESH)
        pl.semaphore_wait(barrier, 3)


def remote(src, dst, send, recv, device):
    return pltpu.make_async_remote_copy(src_ref=src, dst_ref=dst, send_sem=send, recv_sem=recv, device_id=device,
                                        device_id_type=pl.DeviceIdType.MESH)


def reduce_kernel(first, b_ref, s_hbm, x_ref, w_ref, out_ref, p_ref, acc, r1, r2, r3, local_sem, send1, recv1, send2, recv2, send3, recv3):
    me = Place()
    step, last = pl.program_id(0), pl.num_programs(0) - 1
    local = [pltpu.make_async_copy(s_hbm.at[me.mine + me.order[t]], acc.at[t], local_sem.at[t]) for t in range(SUB)]
    one = [remote(s_hbm.at[me.theirs + me.order[t]], r1.at[t], send1.at[t], recv1.at[t], me.core) for t in range(SUB)]
    two = [remote(acc.at[t], r2.at[t], send2.at[t], recv2.at[t], (me.x_chip, me.y_chip)[t % 2]) for t in range(4)]
    three = [remote(acc.at[4 + t], r3.at[t], send3.at[t], recv3.at[t], (me.y_chip, me.x_chip)[t]) for t in range(2)]

    def add(dst, a, b):
        def row(i, _):
            dst[i] = a[i] + b[i]
            return 0
        lax.fori_loop(0, acc.shape[1], row, 0)

    def from_core(t):
        local[t].wait()
        one[t].wait_recv()
        add(acc.at[t], acc.at[t], r1.at[t])

    def from_chip(t):
        two[t].wait_recv()
        add(acc.at[4 + t], acc.at[4 + t], r2.at[t])

    @pl.when(step == 0)
    def _():
        for copy in local:
            copy.start()
        me.enter()
        for copy in one:
            copy.start()

    @pl.when(step == 1)
    def _():
        for t in range(4):
            from_core(t)
            two[t].start()

    @pl.when(step == 2)
    def _():
        for t in range(4, SUB):
            from_core(t)

    @pl.when(step == last // 2)
    def _():
        for t in range(2):
            from_chip(t)
            three[t].start()

    channel_product(first, x_ref, w_ref, b_ref, p_ref.at[0])

    @pl.when(step == last)
    def _():
        for t in range(2, 4):
            from_chip(t)
        for t in range(2):
            three[t].wait_recv()
            add(out_ref.at[t], acc.at[6 + t], r3.at[t])
        for copy in one + two + three:
            copy.wait_send()


def gather_kernel(first, b_ref, t_ref, x_ref, w_ref, p_in, out, p_ref, local_sem, send, recv):
    me = Place()
    step, last = pl.program_id(0), pl.num_programs(0) - 1
    p3, q3, p2, q2, p1, q1, p0, q0 = (me.mine + o for o in me.order)
    own = (t_ref.at[0], t_ref.at[1])
    local = [pltpu.make_async_copy(own[i], out.at[k], local_sem.at[i]) for i, k in enumerate((p0, q0))]
    plan = [(own[0], p0, me.y_chip), (own[1], q0, me.x_chip), (own[0], p0, me.x_chip), (own[1], q0, me.y_chip),
            (own[0], p0, me.core), (own[1], q0, me.core),
            (out.at[p1], p1, me.x_chip), (out.at[q1], q1, me.y_chip)]
    plan += [(out.at[k], k, me.core) for k in (p1, q1, p2, q2, p3, q3)]
    copies = [remote(src, out.at[k], send.at[n], recv.at[n], device) for n, (src, k, device) in enumerate(plan)]

    @pl.when(step == 0)
    def _():
        for copy in local:
            copy.start()
        me.enter()
        for copy in copies[:6]:
            copy.start()

    @pl.when(step == last // 2)
    def _():
        for n in range(2):
            copies[n].wait_recv()
            copies[6 + n].start()
        for n in range(2):
            copies[SUB + n].start()

    channel_product(first, x_ref, w_ref, b_ref, p_ref.at[0])

    @pl.when(step == last)
    def _():
        for n, arrived in enumerate((2, 3, 6, 7)):
            copies[arrived].wait_recv()
            copies[10 + n].start()
        for n in (4, 5, SUB, 9, 10, 11, 12, 13):
            copies[n].wait_recv()
        for copy in copies:
            copy.wait_send()
        for copy in local:
            copy.wait()


def block(shape, index, **kwargs):
    def index_map(*at):
        return tuple(0 if k == 'o' else at['ij'.index(k)] for k in index)
    return pl.BlockSpec(shape, index_map, **kwargs)


def bf16_addends(table):
    out = []
    for _ in range(3):
        out.append(lax.reduce_precision(table, exponent_bits=SUB, mantissa_bits=7))
        table = table - out[-1]
    return jnp.stack(out).astype(BF16)


def solution(mesh):
    row_devs, col_devs = mesh.shape['ys'], mesh.shape['xs']

    def local_layers(field, spec_real, spec_imag, mix_weight, bias):
        batch, x_loc, y_loc, grid_z, width = field.shape
        modes = spec_real.shape[3]
        grid_x, grid_y = x_loc * col_devs, y_loc * row_devs
        groups, blocks = x_loc // X_GROUP, y_loc // Y_BLOCK
        lanes = X_GROUP * batch
        kx, ky = kept(modes, grid_x), kept(modes, grid_y)
        n_kx, n_ky = len(kx), len(ky)
        x_index, y_index = lax.axis_index('xs'), lax.axis_index('ys')
        fwd_np, inv_np = all_tables(blocks, ky, grid_y, grid_z, grid_x * grid_y * grid_z)
        fwd, inv = [jnp.asarray(t) for t in fwd_np], [jnp.asarray(t) for t in inv_np]

        turn = 2.0 * math.pi * (kx[:, None] * np.arange(grid_x)[None, :] % grid_x) / grid_x
        cos, sin = np.cos(turn), np.sin(turn)
        fwd_x = np.stack([np.stack([cos, sin], -1), np.stack([-sin, cos], -1)], 1)
        inv_x = np.transpose(fwd_x, (2, 3, 0, 1))
        fwd_x = fwd_x.reshape(n_kx, 2, col_devs, x_loc, 2).transpose(2, 0, 1, 3, 4).reshape(col_devs, 2 * n_kx, 2 * x_loc)
        inv_x = inv_x.reshape(col_devs, 2 * x_loc, 2 * n_kx)
        odd = (jnp.arange(16 * x_loc) % 2 * y_index)[:, None]

        def x_table(tables):
            wide = np.kron(tables, np.eye(SUB)).astype(np.float32)
            t = lax.dynamic_index_in_dim(jnp.asarray(wide), x_index, 0, keepdims=False)
            return bf16_addends(jnp.where(odd == 1, -t, t))
        fwd_x, inv_x = x_table(fwd_x), x_table(inv_x)
        eye = jnp.eye(Z_BLOCK, dtype=F32)
        half_w, half_b = 0.5 * mix_weight, 0.5 * bias
        point_w = [bf16_addends((half_w[layer].T[:, None, :, None] * eye[None, :, None, :]).reshape(width * SUB, width * SUB))
                   for layer in range(2)]

        real_w, imag_w = (jnp.transpose(w, (0, 1, 2, 4, 3, 5)) for w in (spec_real, spec_imag))
        v = jnp.transpose(field, (1, 2, 4, 3, 0))
        grid = (groups, blocks)
        params = pltpu.CompilerParams(vmem_limit_bytes=VMEM_LIMIT)
        one = pl.Buffered(1)
        spec_shape = jax.ShapeDtypeStruct((groups, width, 256, lanes), F32)
        in_block = block((X_GROUP, Y_BLOCK, width, grid_z, batch), 'ijooo')
        mid_block = block((1, Y_BLOCK, width, grid_z, lanes), 'ijooo')
        part_block = block((1, 3, width, 256, lanes), 'ioooo', pipeline_mode=one)
        mid_shape = jax.ShapeDtypeStruct((groups, y_loc, width, grid_z, lanes), F32)
        steps = y_loc // HALF_BLOCK
        anywhere, smem = pl.BlockSpec(memory_space=pl.ANY), pl.BlockSpec(memory_space=pltpu.SMEM)

        def stage(unit):
            return pltpu.VMEM((unit[1] // unit[0], 5, Y_BLOCK * SUB, unit[0] * lanes), F32)
        w_block = block((3, width * SUB, width * SUB), 'ooo')

        def half_block(first, half):
            shape = (HALF_BLOCK, width, grid_z)
            if first:
                return pl.BlockSpec((X_GROUP,) + shape + (batch,), lambda j: (half, j, 0, 0, 0))
            return pl.BlockSpec((1,) + shape + (lanes,), lambda j: (half, j, 0, 0, 0))

        def table_specs(tables):
            return [block((1,) + t.shape[1:], 'joo') for t in tables]

        f = pl.pallas_call(
            functools.partial(forward_kernel, FORWARD_UNIT), grid=grid, out_shape=spec_shape,
            in_specs=[in_block] + table_specs(fwd),
            out_specs=block((1, width, 256, lanes), 'iooo'),
            scratch_shapes=[stage(FORWARD_UNIT)], compiler_params=params, name='forward')(v, *fwd)

        own = 2
        core, x_chip = x_index % 2, x_index // 2
        owner = jnp.stack([SUB * core + 2 * x_chip + y_index, SUB * core + 4 + 2 * y_index + x_chip]).astype(jnp.int32)
        full = (n_kx, SUB, 2, n_ky, width * batch)

        def across(f, layer, source):
            s = pl.pallas_call(
                x_forward_kernel, grid=(SUB, n_ky // SUB), out_shape=jax.ShapeDtypeStruct(full, F32),
                in_specs=[block((3, 256, 256), 'ooo'),
                          block((groups, width, 1, 2, 1, SUB, lanes), 'ooiojoo')],
                out_specs=block((n_kx, 1, 2, SUB, width * batch), 'oiojo'),
                compiler_params=params, name='x_forward')(
                    fwd_x, f.reshape(groups, width, SUB, 2, n_ky // SUB, SUB, lanes))
            unit = full[1:]
            first = layer == 0
            own_block = block((own,) + unit, 'ooooo')
            s, p = pl.pallas_call(
                functools.partial(reduce_kernel, first), grid=(steps,),
                out_shape=(jax.ShapeDtypeStruct((own,) + unit, F32), mid_shape),
                in_specs=[smem, anywhere, half_block(first, 0), w_block],
                out_specs=(own_block, half_block(False, 0)),
                scratch_shapes=[pltpu.VMEM((n,) + unit, F32) for n in (SUB, SUB, 4, 2)]
                + [pltpu.SemaphoreType.DMA((n,)) for n in (SUB, SUB, SUB, 4, 4, 2, 2)],
                compiler_params=pltpu.CompilerParams(
                    vmem_limit_bytes=VMEM_LIMIT, collective_id=2 * layer, has_side_effects=True),
                name='reduce')(half_b[layer], s, source, point_w[layer])
            r_spec = pl.BlockSpec((1, 1, n_ky, width, SUB, width), lambda i, o: (layer, o[i], 0, 0, 0, 0))
            s_spec = block((1,) + full[1:], 'ioooo')
            t = pl.pallas_call(
                mix_kernel, out_shape=jax.ShapeDtypeStruct((own,) + full[1:], F32),
                grid_spec=pltpu.PrefetchScalarGridSpec(
                    num_scalar_prefetch=1, grid=(own,), in_specs=[s_spec, r_spec, r_spec], out_specs=s_spec,
                    scratch_shapes=[pltpu.VMEM((n_ky * SUB, 128), F32)] + [pltpu.VMEM((width, 24, 128), F32)] * 2
                    + [pltpu.VMEM((width * batch, SUB * n_ky), F32)] * 4),
                compiler_params=params, name='mix')(owner, s, real_w, imag_w)
            t, p = pl.pallas_call(
                functools.partial(gather_kernel, first), grid=(steps,),
                out_shape=(jax.ShapeDtypeStruct(full, F32), mid_shape),
                in_specs=[smem, own_block, half_block(first, 1), w_block, anywhere],
                out_specs=(anywhere, half_block(False, 1)), input_output_aliases={4: 1},
                scratch_shapes=[pltpu.SemaphoreType.DMA((2,)), pltpu.SemaphoreType.DMA((14,)), pltpu.SemaphoreType.DMA((14,))],
                compiler_params=pltpu.CompilerParams(
                    vmem_limit_bytes=VMEM_LIMIT, collective_id=2 * layer + 1, has_side_effects=True),
                name='gather')(half_b[layer], t, source, point_w[layer], p)
            parts = pl.pallas_call(
                x_inverse_kernel, grid=(SUB, n_ky // SUB),
                out_shape=jax.ShapeDtypeStruct((groups, 3, width, SUB, 2, n_ky // SUB, SUB, lanes), BF16),
                in_specs=[block((3, 256, 256), 'ooo'),
                          block((n_kx, 1, 2, SUB, width * batch), 'oiojo')],
                out_specs=block((groups, 3, width, 1, 2, 1, SUB, lanes), 'oooiojoo'),
                compiler_params=params, name='x_inverse')(inv_x, t)
            return parts.reshape(groups, 3, width, 256, lanes), p

        parts, p = across(f, 0, v)
        v1, f = pl.pallas_call(
            functools.partial(layer_kernel, FIRST_UNIT, True), grid=grid, out_shape=(mid_shape, spec_shape),
            in_specs=[mid_block, part_block] + table_specs(inv) + table_specs(fwd),
            out_specs=(mid_block, anywhere),
            scratch_shapes=[stage(FIRST_UNIT)] * 2 + [pltpu.VMEM((width, 256, lanes), F32), pltpu.SemaphoreType.DMA],
            compiler_params=params, name='layer_first')(p, parts, *inv, *fwd)
        parts, p = across(f, 1, v1)
        out = pl.pallas_call(
            functools.partial(layer_kernel, LAST_UNIT, False), grid=grid,
            out_shape=jax.ShapeDtypeStruct((x_loc, y_loc, width, grid_z, batch), F32),
            in_specs=[mid_block, part_block] + table_specs(inv), out_specs=in_block, scratch_shapes=[stage(LAST_UNIT)],
            compiler_params=params, name='layer_last')(p, parts, *inv)
        return jnp.transpose(out, (4, 0, 1, 3, 2))

    field_spec = P('data', 'xs', 'ys', None, None)
    return jax.shard_map(local_layers, mesh=mesh, in_specs=(field_spec, P(), P(), P(), P()), out_specs=field_spec, check_vma=False)
```

```python
import functools
import math

import jax
import jax.numpy as jnp
import ml_dtypes
import numpy as np
from jax import lax
from jax.experimental import pallas as pl
from jax.experimental.pallas import tpu as pltpu
from jax.sharding import PartitionSpec as P

F32 = jnp.float32
BF16 = jnp.bfloat16
VMEM_LIMIT = 64 * 1024 * 1024 - 65536

SUB = 8
X_GROUP = 8
Y_BLOCK = 4
HALF_BLOCK = 2
Z_BLOCK = 8
KZ_CLASS = ((0, 5), (1, 6, 4), (2, 7, 3))
KZ_ORDER = tuple(kz for group in KZ_CLASS for kz in group)
CLASS_ROWS = (0, 64, 160, 256)
LANES = 128
FORWARD_UNIT = (2, 10)
FIRST_UNIT = (2, 10)
LAST_UNIT = (1, 10)
ROOT5_4 = math.sqrt(5.0) / 4.0
SIN_1 = math.sin(2.0 * math.pi / 5.0)
SIN_RATIO = math.sin(4.0 * math.pi / 5.0) / SIN_1


def kz_sign(kz):
    return 0 if kz % 5 == 0 else (1 if kz % 5 < 3 else -1)


def kept(modes, size):
    return np.concatenate([np.arange(modes), np.arange(size - modes, size)])


def pieces(table):
    rest = np.asarray(table, np.float32)
    out = []
    for _ in range(3):
        out.append(rest.astype(ml_dtypes.bfloat16))
        rest = rest - out[-1].astype(np.float32)
    return out


def yz_angles(kz, y_pos, ky, grid_y, grid_z):
    z_pos = np.arange(Z_BLOCK)
    turn = (ky[:, None, None] * y_pos[None, :, None] % grid_y) / grid_y + kz * z_pos[None, None, :] / grid_z
    return 2.0 * math.pi * turn


def forward_table(group, y_pos, ky, grid_y, grid_z):
    rows = []
    for kz in group:
        t, s = yz_angles(kz, y_pos, ky, grid_y, grid_z), kz_sign(kz)
        real, imag = [np.cos(t)], [-np.sin(t)]
        if s:
            real.append(-s * SIN_1 * np.sin(t))
            imag.append(-s * SIN_1 * np.cos(t))
        rows += [np.stack(part, 1).reshape(len(ky), -1) for part in (real, imag)]
    return np.concatenate(rows, 0)


def inverse_table(group, y_pos, ky, grid_y, grid_z, points):
    cols = []
    for kz in group:
        t, s = yz_angles(kz, y_pos, ky, grid_y, grid_z).transpose(1, 2, 0), kz_sign(kz)
        w = (0.5 if kz == 0 else 1.0) / points
        real, imag = [w * np.cos(t)], [-w * np.sin(t)]
        if s:
            real.append(s * SIN_1 * w * np.sin(t))
            imag.append(s * SIN_1 * w * np.cos(t))
        cols += [np.stack(part, 0).reshape(-1, len(ky)) for part in (real, imag)]
    return np.concatenate(cols, 1)


def all_tables(blocks, ky, grid_y, grid_z, points):
    fwd, inv = [[], [], []], [[], [], [], [], []]
    for block in range(blocks):
        y_pos = np.arange(Y_BLOCK) + block * Y_BLOCK
        for k, group in enumerate(KZ_CLASS):
            a, b, c = pieces(forward_table(group, y_pos, ky, grid_y, grid_z))
            n = np.zeros_like(a)
            if k == 0:
                fwd[k].append(np.concatenate([a, a, a, b, b, c], 1))
            else:
                fwd[k].append(np.block([[a, a, a, b], [c, b, n, n]]))
            a, b, c = pieces(inverse_table(group, y_pos, ky, grid_y, grid_z, points))
            n = np.zeros_like(a)
            if k == 0:
                inv[0].append(np.block([[a, a, a], [b, b, n], [c, n, n]]))
            else:
                inv[2 * k - 1].append(np.block([[a, a], [b, b]]))
                inv[2 * k].append(np.concatenate([c, a], 1))
    return [np.stack(t) for t in fwd], [np.stack(t) for t in inv]


def split3(v):
    d1 = v.astype(BF16)
    rest = v - d1.astype(F32)
    d2 = rest.astype(BF16)
    return d1, d2, (rest - d2.astype(F32)).astype(BF16)


def dot(a, b):
    return jnp.dot(a, b, preferred_element_type=F32)


def z_forward(v):
    v0, v1, v2, v3, v4 = v
    t1, t2, e1, e2 = v1 + v4, v2 + v3, v1 - v4, v2 - v3
    total = t1 + t2
    mid, dif = v0 - 0.25 * total, ROOT5_4 * (t1 - t2)
    return v0 + total, mid + dif, e1 + SIN_RATIO * e2, mid - dif, SIN_RATIO * e1 - e2


def z_inverse(a0, a1, b1, a2, b2):
    total = a1 + a2
    mid, dif = a0 - 0.25 * total, ROOT5_4 * (a1 - a2)
    p, q = mid + dif, mid - dif
    r, s = b1 + SIN_RATIO * b2, SIN_RATIO * b1 - b2
    return a0 + total, p - r, q - s, q + s, p + r


def split_tiles(u_ref, channels):
    rows, lanes = u_ref.shape[1:]
    out = [[], [], []]
    for k in channels:
        for r in range(0, rows, 2 * SUB):
            cells = [split3(u_ref[k, r:r + 2 * SUB, lane:lane + LANES]) for lane in range(0, lanes, LANES)]
            for i in range(3):
                out[i].append(jnp.concatenate([cell[i] for cell in cells], -1))
    return [jnp.concatenate(rows, 0) for rows in out]


def add_tiles(o, n, lanes, first=0):
    for r in range(0, n, SUB):
        for lane in range(0, lanes, LANES):
            cells = [o[b + r:b + r + SUB, lane:lane + LANES] for b in range(0, o.shape[0], n)]
            yield r, lane, functools.reduce(jnp.add, cells)


def forward_stage(u_ref, tables, f_ref, c, pair):
    lanes = f_ref.shape[-1]
    for k, channels in enumerate(((0,), (1, 2), (3, 4))):
        d = split_tiles(u_ref, channels)
        o = dot(tables[k], jnp.concatenate([d[i] for i in ((0, 1, 2, 0) if k else (0, 1, 2, 0, 1, 0))], 0))
        n = CLASS_ROWS[k + 1] - CLASS_ROWS[k]
        for r, lane, v in add_tiles(o, n, pair * lanes):
            at = (c + lane // lanes, slice(CLASS_ROWS[k] + r, CLASS_ROWS[k] + r + SUB), slice(lane % lanes, lane % lanes + LANES))
            f_ref[at] += v


def inverse_stage(s_ref, c, pair, tables, u_ref):
    n, lanes = u_ref.shape[1:]

    def part(i, k):
        return jnp.concatenate([s_ref[0, i, c + u, CLASS_ROWS[k]:CLASS_ROWS[k + 1]] for u in range(pair)], -1)
    o = dot(tables[0], jnp.concatenate([part(i, 0) for i in range(3)], 0))
    for r, lane, v in add_tiles(o, n, lanes):
        u_ref[0, r:r + SUB, lane:lane + LANES] = v
    for k in (1, 2):
        d1, d2, d3 = (part(i, k) for i in range(3))
        o = jnp.concatenate([dot(tables[2 * k - 1], jnp.concatenate([d1, d2], 0)),
                             dot(tables[2 * k], jnp.concatenate([d1, d3], 0))], 0)
        for r, lane, v in add_tiles(o, 2 * n, lanes):
            u_ref[2 * k - 1 + r // n, r % n:r % n + SUB, lane:lane + LANES] = v


def registers(pair, lanes):
    for u in range(pair):
        for y in range(Y_BLOCK):
            for lane in range(0, lanes, LANES):
                yield u, y, lane, (slice(y * SUB, (y + 1) * SUB), slice(u * lanes + lane, u * lanes + lane + LANES))


def gelu(h):
    k = 2.0 * math.sqrt(2.0 / math.pi)
    return h + h * jnp.tanh(h * (k + (4.0 * 0.044715 * k) * (h * h)))


def field_lanes(x_ref, y, c):
    return jnp.concatenate([x_ref[x, y, c] for x in range(X_GROUP)], -1)


def zero_spectrum(f_ref):
    def clear(c, _):
        f_ref[c] = jnp.zeros(f_ref.shape[1:], F32)
        return 0
    lax.fori_loop(0, f_ref.shape[0], clear, 0)


def forward_kernel(unit, x_ref, t0, t1, t2, f_ref, u_ref):
    f_ref = f_ref.at[0]
    width, lanes = x_ref.shape[2], f_ref.shape[-1]
    pair, per_step = unit
    tables = (t0[0], t1[0], t2[0])

    @pl.when(pl.program_id(1) == 0)
    def _():
        zero_spectrum(f_ref)

    def load(c, slot):
        for u in range(pair):
            for y in range(Y_BLOCK):
                row = field_lanes(x_ref, y, c + u)
                for k, v in enumerate(z_forward([row[SUB * j:SUB * j + SUB] for j in range(5)])):
                    u_ref[slot, k, y * SUB:(y + 1) * SUB, u * lanes:(u + 1) * lanes] = v

    def body(i, _):
        c = i * per_step
        count = per_step // pair
        for n in range(count + 1):
            if n < count:
                load(c + n * pair, n)
            if n:
                forward_stage(u_ref.at[n - 1], tables, f_ref, c + (n - 1) * pair, pair)
        return 0
    lax.fori_loop(0, width // per_step, body, 0)


def channel_product(first, x_ref, w_ref, p_ref):
    blocks, width, depth, lanes = p_ref.shape
    rows = width * SUB
    ones = jnp.ones((w_ref.shape[2] - rows, lanes), BF16)
    full, (a, b, c) = w_ref[0], (w_ref[i, :, :rows] for i in range(3))

    def z_block(j, _):
        z = pl.ds(pl.multiple_of(j * SUB, SUB), SUB)
        for y in range(blocks):
            if first:
                v = jnp.concatenate([x_ref[x, y, :, z, :] for x in range(X_GROUP)], -1)
            else:
                v = x_ref[0, y, :, z, :]
            d1, d2, d3 = split3(v.reshape(rows, lanes))
            p = dot(full, jnp.concatenate([d1, ones], 0)) + dot(a, d2) + dot(a, d3) + dot(b, d1) + dot(b, d2) + dot(c, d1)
            p_ref[y, :, z, :] = p.reshape(width, SUB, lanes)
        return 0
    lax.fori_loop(0, depth // SUB, z_block, 0)


def layer_kernel(unit, first, *refs):
    p_ref, s_ref, *tabs = refs
    p_ref = p_ref.at[0]
    width, lanes = p_ref.shape[1], p_ref.shape[-1]
    batch = lanes // X_GROUP
    if first:
        *tabs, v_ref, f_hbm, a_ref, u_ref, f_ref, sem = tabs
        v_ref = v_ref.at[0]

        @pl.when(pl.program_id(1) == 0)
        def _():
            zero_spectrum(f_ref)
    else:
        *tabs, o_ref, a_ref = tabs
    inv, fwd = [t[0] for t in tabs[:5]], [t[0] for t in tabs[5:]]
    pair, per_step = unit

    def activate(c, slot):
        kept_rows = {}
        for u, y, lane, at in registers(pair, lanes):
            new = []
            for j, s in enumerate(z_inverse(*(a_ref[(slot, k) + at] for k in range(5)))):
                g = gelu(s + p_ref[y, c + u, SUB * j:SUB * j + SUB, lane:lane + LANES])
                new.append(g)
                if first:
                    v_ref[y, c + u, SUB * j:SUB * j + SUB, lane:lane + LANES] = g
                else:
                    kept_rows[j] = kept_rows.get(j, ()) + (g,)
            if first:
                for k, v in enumerate(z_forward(new)):
                    u_ref[(slot, k) + at] = v
            elif lane + LANES == lanes:
                for j, row in kept_rows.items():
                    store_field(o_ref, y, c + u, SUB * j, row, batch)
                kept_rows = {}

    def body(i, _):
        c = i * per_step
        count = per_step // pair
        for n in range(count + 2):
            if n < count:
                inverse_stage(s_ref, c + n * pair, pair, inv, a_ref.at[n])
            if 0 < n <= count:
                activate(c + (n - 1) * pair, n - 1)
            if first and n > 1:
                forward_stage(u_ref.at[n - 2], fwd, f_ref, c + (n - 2) * pair, pair)
        return 0
    lax.fori_loop(0, width // per_step, body, 0)

    if first:
        @pl.when(pl.program_id(1) == pl.num_programs(1) - 1)
        def _():
            copy = pltpu.make_async_copy(f_ref, f_hbm.at[pl.program_id(0)], sem)
            copy.start()
            copy.wait()


def store_field(o_ref, y, c, z, row, batch):
    lane = lax.broadcasted_iota(jnp.int32, row[0].shape, 1)
    for x in range(X_GROUP):
        at, off = divmod(x * batch, LANES)
        piece = row[at]
        if off + batch > LANES:
            piece = jnp.where(lane < off, row[at + 1], piece)
        if off:
            piece = pltpu.roll(piece, LANES - off, 1)
        o_ref[x, y, c, z:z + SUB, :] = piece[:, :batch]


def split_dot(left, right):
    a, b, c = left
    d1, d2, d3 = split3(right)
    return dot(a, d1) + dot(a, d2) + dot(a, d3) + dot(b, d1) + dot(b, d2) + dot(c, d1)


def x_forward(m_ref, f_ref, s_ref, slot):
    groups, width, lanes = f_ref.shape[0], f_ref.shape[1], f_ref.shape[-1]
    batch = lanes // X_GROUP
    halves = range(f_ref.shape[4])
    rights = []
    for h in halves:
        rows = []
        for g in range(groups):
            for x in range(X_GROUP):
                for p in range(2):
                    rows.append(jnp.concatenate([f_ref[g, c, 0, p, h, :, x * batch:(x + 1) * batch] for c in range(width)], -1))
        rights.append(jnp.concatenate(rows, 0))
    for h in halves:
        out = split_dot((m_ref[0], m_ref[1], m_ref[2]), rights[h])
        s_ref[:, slot, :, h * SUB:(h + 1) * SUB, :] = out.reshape(s_ref.shape[0], 2, SUB, width * batch)


def x_inverse(m_ref, t_ref, slot, s_ref):
    groups, width, lanes = s_ref.shape[0], s_ref.shape[2], s_ref.shape[-1]
    batch = lanes // X_GROUP
    halves = range(s_ref.shape[5])
    outs = []
    for h in halves:
        right = t_ref[:, slot, :, h * SUB:(h + 1) * SUB, :].reshape(t_ref.shape[0] * 2 * SUB, width * batch)
        outs.append(split_dot((m_ref[0], m_ref[1], m_ref[2]), right).reshape(groups, X_GROUP, 2, SUB, width * batch))
    for h in halves:
        for g in range(groups):
            for p in range(2):
                for c in range(width):
                    row = jnp.concatenate([outs[h][g, x, p, :, c * batch:(c + 1) * batch] for x in range(X_GROUP)], -1)
                    for i, d in enumerate(split3(row)):
                        s_ref[g, i, c, 0, p, h] = d


def mix(s_ref, re_w, im_w, t_ref, to, half, rows, re_rows, im_rows, re_s, im_s, re_t, im_t):
    own, slots, _, n_ky, lanes = s_ref.shape
    width = re_w.shape[2]
    batch = lanes // width
    some = slots // 2
    part_modes = some * n_ky
    pick = slice(half * some, (half + 1) * some)

    for w_ref, out in ((re_w, re_rows), (im_w, im_rows)):
        def lay(c, _):
            for k in range(own):
                for ky in range(n_ky):
                    at = (k * n_ky + ky) * SUB
                    rows[at:at + SUB, 0:width] = w_ref[k, ky, c]
            mat = jnp.concatenate([rows[pl.ds((k * n_ky + h * SUB) * SUB + kz, SUB, stride=SUB), :]
                                   for k in range(own) for kz in KZ_ORDER[pick] for h in range(n_ky // SUB)], 0)
            out[c] = mat.T[0:out.shape[1]]
            return 0
        lax.fori_loop(0, width, lay, 0)
    for p, out in enumerate((re_s, im_s)):
        out[...] = jnp.concatenate([s_ref[k, pick, p].reshape(part_modes, lanes) for k in range(own)], 0).T
    pair = 2

    def outputs(i, _):
        d = i * pair

        def inner(c, acc):
            at = pl.ds(pl.multiple_of(c * batch, SUB), batch)
            a, b = re_s[at, :], im_s[at, :]
            new = []
            for u in range(pair):
                p = jnp.broadcast_to(re_rows[c, pl.ds(d + u, 1), :], a.shape)
                q = jnp.broadcast_to(im_rows[c, pl.ds(d + u, 1), :], a.shape)
                new += [acc[2 * u] + (a * p - b * q), acc[2 * u + 1] + (a * q + b * p)]
            return tuple(new)
        zero = jnp.zeros((batch, own * part_modes), F32)
        acc = lax.fori_loop(0, width, inner, (zero,) * (2 * pair))
        for u in range(pair):
            at = pl.ds(pl.multiple_of((d + u) * batch, SUB), batch)
            re_t[at, :] = acc[2 * u]
            im_t[at, :] = acc[2 * u + 1]
        return 0
    lax.fori_loop(0, width // pair, outputs, 0)
    for p, got in enumerate((re_t, im_t)):
        back = got[...].T
        for k in range(own):
            t_ref[to[k], pick, p] = back[k * part_modes:(k + 1) * part_modes].reshape(some, n_ky, lanes)


class Place:
    def __init__(self):
        xs, ys = lax.axis_index('xs'), lax.axis_index('ys')
        data = lax.axis_index('data')
        c, x, y = xs % 2, xs // 2, ys
        self.core = (data, ys, 2 * x + 1 - c)
        self.x_chip = (data, ys, 2 * (1 - x) + c)
        self.y_chip = (data, 1 - ys, xs)
        p, q = lambda a, b: 2 * a + b, lambda a, b: 4 + 2 * a + b
        self.mine = SUB * c
        self.order = (p(1 - x, 1 - y), q(1 - y, 1 - x), p(1 - x, y), q(1 - y, x),
                      p(x, 1 - y), q(y, 1 - x), p(x, y), q(y, x))

    def enter(self):
        barrier = pltpu.get_barrier_semaphore()
        for device in (self.core, self.x_chip, self.y_chip):
            pl.semaphore_signal(barrier, inc=1, device_id=device, device_id_type=pl.DeviceIdType.MESH)
        pl.semaphore_wait(barrier, 3)


def remote(src, dst, send, recv, device):
    return pltpu.make_async_remote_copy(src_ref=src, dst_ref=dst, send_sem=send, recv_sem=recv, device_id=device,
                                        device_id_type=pl.DeviceIdType.MESH)


def half_slots(ref, k, half):
    some = ref.shape[1] // 2
    return ref.at[k, pl.ds(half * some, some)]


def reduce_kernel(first, m_ref, f_ref, x_ref, w_ref, out_ref, p_ref, s_ref, r1, r2, r3,
                  send1, recv1, send2, recv2, send3, recv3):
    me = Place()
    step, last = pl.program_id(0), pl.num_programs(0) - 1
    one, two, three = [], [], []
    for h in range(2):
        mine = [half_slots(s_ref, k, h) for k in me.order]
        one.append([remote(half_slots(s_ref, SUB + me.order[t], h), half_slots(r1, t, h), send1.at[h, t], recv1.at[h, t], me.core)
                    for t in range(SUB)])
        two.append([remote(mine[t], half_slots(r2, t, h), send2.at[h, t], recv2.at[h, t], (me.x_chip, me.y_chip)[t % 2])
                    for t in range(4)])
        three.append([remote(mine[4 + t], half_slots(r3, t, h), send3.at[h, t], recv3.at[h, t], (me.y_chip, me.x_chip)[t])
                      for t in range(2)])

    def add(dst, a, b):
        def row(i, _):
            dst[i] = a[i] + b[i]
            return 0
        lax.fori_loop(0, dst.shape[0], row, 0)

    def from_core(h):
        for t in range(SUB):
            one[h][t].wait_recv()
            to = half_slots(s_ref, me.order[t], h)
            add(to, to, half_slots(r1, t, h))
            if t < 4:
                two[h][t].start()

    def from_chip(h, these):
        for t in these:
            two[h][t].wait_recv()
            to = half_slots(s_ref, me.order[4 + t], h)
            add(to, to, half_slots(r2, t, h))
            if t < 2:
                three[h][t].start()

    def finish(h):
        from_chip(h, (2, 3))
        for t in range(2):
            three[h][t].wait_recv()
            add(half_slots(out_ref, t, h), half_slots(s_ref, me.order[6 + t], h), half_slots(r3, t, h))

    def send_core(h):
        for copy in one[h]:
            copy.start()

    slots = s_ref.shape[1]
    events = ((0, me.enter), (slots // 2, lambda: send_core(0)), (slots // 2 + 1, lambda: from_core(0)),
              (slots - 1, lambda: from_chip(0, (0, 1))), (slots, lambda: send_core(1)), (slots + 2, lambda: from_core(1)),
              (slots + 4, lambda: finish(0)), (slots + 6, lambda: from_chip(1, (0, 1))))
    for at, event in events:
        pl.when(step == at)(event)

    @pl.when(step < slots)
    def _():
        x_forward(m_ref, f_ref, s_ref, step)

    @pl.when(step >= slots // 2)
    def _():
        channel_product(first, x_ref, w_ref, p_ref.at[0])

    @pl.when(step == last)
    def _():
        finish(1)
        for h in range(2):
            for copy in one[h] + two[h] + three[h]:
                copy.wait_send()


def gather_kernel(first, layer, m_ref, s_ref, re_hbm, im_hbm, x_ref, w_ref, p_in, parts_ref, p_ref, t_ref,
                  re_w, im_w, rows, re_rows, im_rows, re_s, im_s, re_t, im_t, w_sem, send, recv):
    me = Place()
    step, last = pl.program_id(0), pl.num_programs(0) - 1
    p3, q3, p2, q2, p1, q1, p0, q0 = me.order
    plan = [(p0, me.y_chip, 0), (q0, me.x_chip, 0), (p0, me.x_chip, 0), (q0, me.y_chip, 0), (p0, me.core, SUB), (q0, me.core, SUB),
            (p1, me.x_chip, 0), (q1, me.y_chip, 0)] + [(k, me.core, SUB) for k in (p1, q1, p2, q2, p3, q3)]
    copies = [[remote(half_slots(t_ref, k, h), half_slots(t_ref, k + up, h), send.at[h, n], recv.at[h, n], device)
               for n, (k, device, up) in enumerate(plan)] for h in range(2)]
    weights = [pltpu.make_async_copy(hbm.at[layer, me.mine + k], to.at[i], w_sem.at[n, i])
               for n, (hbm, to) in enumerate(((re_hbm, re_w), (im_hbm, im_w))) for i, k in enumerate((p0, q0))]

    def mix_half(h):
        mix(s_ref, re_w, im_w, t_ref, (p0, q0), h, rows, re_rows, im_rows, re_s, im_s, re_t, im_t)
        for copy in copies[h][:6]:
            copy.start()

    def begin():
        for copy in weights:
            copy.start()
        me.enter()
        for copy in weights:
            copy.wait()
        mix_half(0)

    def pass_on(h):
        for n in range(2):
            copies[h][n].wait_recv()
            copies[h][6 + n].start()
        for n in range(2):
            copies[h][SUB + n].start()

    def finish(h):
        for n, arrived in enumerate((2, 3, 6, 7)):
            copies[h][arrived].wait_recv()
            copies[h][10 + n].start()
        for n in (4, 5, *range(SUB, len(plan))):
            copies[h][n].wait_recv()

    slots = t_ref.shape[1]
    x_from = last + 1 - slots
    for at, event in ((0, begin), (1, lambda: mix_half(1)), (3, lambda: pass_on(0)), (x_from - 2, lambda: pass_on(1)),
                      (x_from, lambda: finish(0)), (x_from + slots // 2, lambda: finish(1))):
        pl.when(step == at)(event)

    @pl.when(step >= 2)
    def _():
        channel_product(first, x_ref, w_ref, p_ref.at[0])

    @pl.when(step >= x_from)
    def _():
        x_inverse(m_ref, t_ref, step - x_from, parts_ref)

    @pl.when(step == last)
    def _():
        for h in range(2):
            for copy in copies[h]:
                copy.wait_send()


def block(shape, index, slot=None, **kwargs):
    def index_map(*at):
        return tuple(0 if k == 'o' else slot(at[0]) if k == 's' else at['ij'.index(k)] for k in index)
    return pl.BlockSpec(shape, index_map, **kwargs)


def bf16_addends(table):
    out = []
    for _ in range(3):
        out.append(lax.reduce_precision(table, exponent_bits=SUB, mantissa_bits=7))
        table = table - out[-1]
    return jnp.stack(out).astype(BF16)


def solution(mesh):
    row_devs, col_devs = mesh.shape['ys'], mesh.shape['xs']

    def local_layers(field, spec_real, spec_imag, mix_weight, bias):
        batch, x_loc, y_loc, grid_z, width = field.shape
        modes = spec_real.shape[3]
        grid_x, grid_y = x_loc * col_devs, y_loc * row_devs
        groups, blocks = x_loc // X_GROUP, y_loc // Y_BLOCK
        lanes = X_GROUP * batch
        kx, ky = kept(modes, grid_x), kept(modes, grid_y)
        n_kx, n_ky = len(kx), len(ky)
        x_index, y_index = lax.axis_index('xs'), lax.axis_index('ys')
        fwd_np, inv_np = all_tables(blocks, ky, grid_y, grid_z, grid_x * grid_y * grid_z)
        fwd, inv = [jnp.asarray(t) for t in fwd_np], [jnp.asarray(t) for t in inv_np]

        turn = 2.0 * math.pi * (kx[:, None] * np.arange(grid_x)[None, :] % grid_x) / grid_x
        cos, sin = np.cos(turn), np.sin(turn)
        fwd_x = np.stack([np.stack([cos, sin], -1), np.stack([-sin, cos], -1)], 1)
        inv_x = np.transpose(fwd_x, (2, 3, 0, 1))
        fwd_x = fwd_x.reshape(n_kx, 2, col_devs, x_loc, 2).transpose(2, 0, 1, 3, 4).reshape(col_devs, 2 * n_kx, 2 * x_loc)
        inv_x = inv_x.reshape(col_devs, 2 * x_loc, 2 * n_kx)
        odd = (jnp.arange(16 * x_loc) % 2 * y_index)[:, None]

        core, x_chip = x_index % 2, x_index // 2

        def x_table(tables, axis):
            wide = np.kron(tables, np.eye(SUB)).astype(np.float32)
            t = lax.dynamic_index_in_dim(jnp.asarray(wide), x_index, 0, keepdims=False)
            t = jnp.where(core == 1, jnp.roll(t, SUB * n_kx, axis), t)
            return bf16_addends(jnp.where(odd == 1, -t, t))
        fwd_x, inv_x = x_table(fwd_x, 0), x_table(inv_x, 1)
        eye = jnp.eye(Z_BLOCK, dtype=F32)
        def point_table(layer):
            w = bf16_addends((0.5 * mix_weight[layer].T[:, None, :, None] * eye[None, :, None, :]).reshape(width * SUB, width * SUB))
            b = bf16_addends(jnp.broadcast_to(0.5 * bias[layer][:, None], (width, SUB)).reshape(width * SUB))
            b = jnp.pad(jnp.stack([b.T, 0 * b.T, 0 * b.T]), ((0, 0), (0, 0), (0, 2 * SUB - 3)))
            return jnp.concatenate([w, b], -1)
        point_w = [point_table(layer) for layer in range(2)]

        real_w, imag_w = (jnp.swapaxes(w, 3, 4) for w in (spec_real, spec_imag))
        v = jnp.swapaxes(jnp.moveaxis(field, 0, -1), 2, 3)
        grid = (groups, blocks)
        params = pltpu.CompilerParams(vmem_limit_bytes=VMEM_LIMIT)
        one = pl.Buffered(1)
        spec_shape = jax.ShapeDtypeStruct((groups, width, 256, lanes), F32)
        in_block = block((X_GROUP, Y_BLOCK, width, grid_z, batch), 'ijooo')
        mid_block = block((1, Y_BLOCK, width, grid_z, lanes), 'ijooo')
        part_block = block((1, 3, width, 256, lanes), 'ioooo', pipeline_mode=one)
        mid_shape = jax.ShapeDtypeStruct((groups, y_loc, width, grid_z, lanes), F32)
        anywhere = pl.BlockSpec(memory_space=pl.ANY)

        def stage(unit):
            return pltpu.VMEM((unit[1] // unit[0], 5, Y_BLOCK * SUB, unit[0] * lanes), F32)
        w_block = block((3, width * SUB, width * SUB + 2 * SUB), 'ooo')

        units = y_loc // HALF_BLOCK

        def half_block(first, half, start):
            shape = (HALF_BLOCK, width, grid_z) + ((batch,) if first else (lanes,))
            return pl.BlockSpec((X_GROUP if first else 1,) + shape,
                                lambda j: (half, jnp.clip(j - start, 0, units - 1), 0, 0, 0))

        def table_specs(tables):
            return [block((1,) + t.shape[1:], 'joo') for t in tables]

        f = pl.pallas_call(
            functools.partial(forward_kernel, FORWARD_UNIT), grid=grid, out_shape=spec_shape,
            in_specs=[in_block] + table_specs(fwd),
            out_specs=block((1, width, 256, lanes), 'iooo'),
            scratch_shapes=[stage(FORWARD_UNIT)], compiler_params=params, name='forward')(v, *fwd)

        own, slots, halves = 2, SUB, n_ky // SUB
        unit = (slots, 2, n_ky, width * batch)
        own_block = block((own,) + unit, 'ooooo')
        x_block = block((3, 16 * x_loc, 16 * x_loc), 'ooo')
        dma = pltpu.SemaphoreType.DMA

        def exchange(number):
            return pltpu.CompilerParams(vmem_limit_bytes=VMEM_LIMIT, collective_id=number, has_side_effects=True)

        def across(f, layer, source):
            first = layer == 0
            s, p = pl.pallas_call(
                functools.partial(reduce_kernel, first), grid=(slots // 2 + units,),
                out_shape=(jax.ShapeDtypeStruct((own,) + unit, F32), mid_shape),
                in_specs=[x_block,
                          block((groups, width, 1, 2, halves, SUB, lanes), 'oosoooo', lambda j: jnp.minimum(j, slots - 1)),
                          half_block(first, 0, slots // 2), w_block],
                out_specs=(own_block, half_block(False, 0, slots // 2)),
                scratch_shapes=[pltpu.VMEM((n,) + unit, F32) for n in (n_kx, SUB, 4, 2)]
                + [dma((2, n)) for n in (SUB, SUB, 4, 4, 2, 2)],
                compiler_params=exchange(2 * layer), name='reduce')(
                    fwd_x, f.reshape(groups, width, slots, 2, halves, SUB, lanes), source, point_w[layer])
            x_from = units + 2 - slots
            parts, p = pl.pallas_call(
                functools.partial(gather_kernel, first, layer), grid=(units + 2,),
                out_shape=(jax.ShapeDtypeStruct((groups, 3, width, slots, 2, halves, SUB, lanes), BF16), mid_shape),
                in_specs=[x_block, own_block, anywhere, anywhere, half_block(first, 1, 2), w_block, anywhere],
                out_specs=(block((groups, 3, width, 1, 2, halves, SUB, lanes), 'ooosoooo', lambda j: jnp.maximum(j - x_from, 0)),
                           half_block(False, 1, 2)),
                input_output_aliases={6: 1},
                scratch_shapes=[pltpu.VMEM((n_kx,) + unit, F32)]
                + [pltpu.VMEM((own, n_ky, width, SUB, width), F32)] * 2
                + [pltpu.VMEM((own * n_ky * SUB, LANES), F32)] + [pltpu.VMEM((width, 24, LANES), F32)] * 2
                + [pltpu.VMEM((width * batch, own * slots * n_ky // 2), F32)] * 4
                + [dma((2, 2)), dma((2, 14)), dma((2, 14))],
                compiler_params=exchange(2 * layer + 1), name='gather')(
                    inv_x, s, real_w, imag_w, source, point_w[layer], p)
            return parts.reshape(groups, 3, width, CLASS_ROWS[-1], lanes), p

        parts, p = across(f, 0, v)
        v1, f = pl.pallas_call(
            functools.partial(layer_kernel, FIRST_UNIT, True), grid=grid, out_shape=(mid_shape, spec_shape),
            in_specs=[mid_block, part_block] + table_specs(inv) + table_specs(fwd),
            out_specs=(mid_block, anywhere),
            scratch_shapes=[stage(FIRST_UNIT)] * 2 + [pltpu.VMEM((width, 256, lanes), F32), pltpu.SemaphoreType.DMA],
            compiler_params=params, name='layer_first')(p, parts, *inv, *fwd)
        parts, p = across(f, 1, v1)
        out = pl.pallas_call(
            functools.partial(layer_kernel, LAST_UNIT, False), grid=grid,
            out_shape=jax.ShapeDtypeStruct((x_loc, y_loc, width, grid_z, batch), F32),
            in_specs=[mid_block, part_block] + table_specs(inv), out_specs=in_block, scratch_shapes=[stage(LAST_UNIT)],
            compiler_params=params, name='layer_last')(p, parts, *inv)
        return jnp.moveaxis(jnp.swapaxes(out, 2, 3), -1, 0)

    field_spec = P('data', 'xs', 'ys', None, None)
    return jax.shard_map(local_layers, mesh=mesh, in_specs=(field_spec, P(), P(), P(), P()), out_specs=field_spec, check_vma=False)
```

```python
import functools
import math

import jax
import jax.numpy as jnp
import ml_dtypes
import numpy as np
from jax import lax
from jax.experimental import pallas as pl
from jax.experimental.pallas import tpu as pltpu
from jax.sharding import PartitionSpec as P

F32 = jnp.float32
BF16 = jnp.bfloat16
VMEM_LIMIT = 64 * 1024 * 1024 - 65536

SUB = 8
X_GROUP = 8
Y_BLOCK = 4
HALF_BLOCK = 2
Z_BLOCK = 8
KZ_CLASS = ((0, 5), (1, 6, 4), (2, 7, 3))
KZ_ORDER = tuple(kz for group in KZ_CLASS for kz in group)
CLASS_ROWS = (0, 64, 160, 256)
LANES = 128
ADDENDS = 3
FORWARD_UNIT = (2, 10)
FIRST_UNIT = (2, 10)
LAST_UNIT = (1, 10)
ROOT5_4 = math.sqrt(5.0) / 4.0
SIN_1 = math.sin(2.0 * math.pi / 5.0)
SIN_RATIO = math.sin(4.0 * math.pi / 5.0) / SIN_1


def kz_sign(kz):
    return 0 if kz % 5 == 0 else (1 if kz % 5 < 3 else -1)


def kept(modes, size):
    return np.concatenate([np.arange(modes), np.arange(size - modes, size)])


def pieces(table):
    rest = np.asarray(table, np.float32)
    out = []
    for _ in range(ADDENDS):
        out.append(rest.astype(ml_dtypes.bfloat16))
        rest = rest - out[-1].astype(np.float32)
    return out


def yz_angles(kz, y_pos, ky, grid_y, grid_z):
    z_pos = np.arange(Z_BLOCK)
    turn = (ky[:, None, None] * y_pos[None, :, None] % grid_y) / grid_y + kz * z_pos[None, None, :] / grid_z
    return 2.0 * math.pi * turn


def forward_table(group, y_pos, ky, grid_y, grid_z):
    rows = []
    for kz in group:
        t, s = yz_angles(kz, y_pos, ky, grid_y, grid_z), kz_sign(kz)
        real, imag = [np.cos(t)], [-np.sin(t)]
        if s:
            real.append(-s * SIN_1 * np.sin(t))
            imag.append(-s * SIN_1 * np.cos(t))
        rows += [np.stack(part, 1).reshape(len(ky), -1) for part in (real, imag)]
    return np.concatenate(rows, 0)


def inverse_table(group, y_pos, ky, grid_y, grid_z, points):
    cols = []
    for kz in group:
        t, s = yz_angles(kz, y_pos, ky, grid_y, grid_z).transpose(1, 2, 0), kz_sign(kz)
        w = (0.5 if kz == 0 else 1.0) / points
        real, imag = [w * np.cos(t)], [-w * np.sin(t)]
        if s:
            real.append(s * SIN_1 * w * np.sin(t))
            imag.append(s * SIN_1 * w * np.cos(t))
        cols += [np.stack(part, 0).reshape(-1, len(ky)) for part in (real, imag)]
    return np.concatenate(cols, 1)


def all_tables(blocks, ky, grid_y, grid_z, points):
    fwd, inv = [[], [], []], [[], [], [], [], []]
    for block in range(blocks):
        y_pos = np.arange(Y_BLOCK) + block * Y_BLOCK
        for k, group in enumerate(KZ_CLASS):
            a, b, c = pieces(forward_table(group, y_pos, ky, grid_y, grid_z))
            n = np.zeros_like(a)
            if k == 0:
                fwd[k].append(np.concatenate([a, a, a, b, b, c], 1))
            else:
                fwd[k].append(np.block([[a, a, a, b], [c, b, n, n]]))
            a, b, c = pieces(inverse_table(group, y_pos, ky, grid_y, grid_z, points))
            n = np.zeros_like(a)
            if k == 0:
                inv[0].append(np.block([[a, a, a], [b, b, n], [c, n, n]]))
            else:
                inv[2 * k - 1].append(np.block([[a, a], [b, b]]))
                inv[2 * k].append(np.concatenate([c, a], 1))
    return [np.stack(t) for t in fwd], [np.stack(t) for t in inv]


def split3(v):
    d1 = v.astype(BF16)
    rest = v - d1.astype(F32)
    d2 = rest.astype(BF16)
    return d1, d2, (rest - d2.astype(F32)).astype(BF16)


def dot(a, b):
    return jnp.dot(a, b, preferred_element_type=F32)


def z_forward(v):
    v0, v1, v2, v3, v4 = v
    t1, t2, e1, e2 = v1 + v4, v2 + v3, v1 - v4, v2 - v3
    total = t1 + t2
    mid, dif = v0 - 0.25 * total, ROOT5_4 * (t1 - t2)
    return v0 + total, mid + dif, e1 + SIN_RATIO * e2, mid - dif, SIN_RATIO * e1 - e2


def z_inverse(a0, a1, b1, a2, b2):
    total = a1 + a2
    mid, dif = a0 - 0.25 * total, ROOT5_4 * (a1 - a2)
    p, q = mid + dif, mid - dif
    r, s = b1 + SIN_RATIO * b2, SIN_RATIO * b1 - b2
    return a0 + total, p - r, q - s, q + s, p + r


def split_tiles(u_ref, channels):
    rows, lanes = u_ref.shape[1:]
    out = [[], [], []]
    for k in channels:
        for r in range(0, rows, 2 * SUB):
            cells = [split3(u_ref[k, r:r + 2 * SUB, lane:lane + LANES]) for lane in range(0, lanes, LANES)]
            for i in range(ADDENDS):
                out[i].append(jnp.concatenate([cell[i] for cell in cells], -1))
    return [jnp.concatenate(rows, 0) for rows in out]


def add_tiles(o, n, lanes, first=0):
    for r in range(0, n, SUB):
        for lane in range(0, lanes, LANES):
            cells = [o[b + r:b + r + SUB, lane:lane + LANES] for b in range(0, o.shape[0], n)]
            yield r, lane, functools.reduce(jnp.add, cells)


def forward_stage(u_ref, tables, f_ref, c, pair):
    lanes = f_ref.shape[-1]
    for k, channels in enumerate(((0,), (1, 2), (3, 4))):
        d = split_tiles(u_ref, channels)
        o = dot(tables[k], jnp.concatenate([d[i] for i in ((0, 1, 2, 0) if k else (0, 1, 2, 0, 1, 0))], 0))
        n = CLASS_ROWS[k + 1] - CLASS_ROWS[k]
        for r, lane, v in add_tiles(o, n, pair * lanes):
            at = (c + lane // lanes, slice(CLASS_ROWS[k] + r, CLASS_ROWS[k] + r + SUB), slice(lane % lanes, lane % lanes + LANES))
            f_ref[at] += v


def inverse_stage(s_ref, c, pair, tables, u_ref):
    n, lanes = u_ref.shape[1:]

    def part(i, k):
        return jnp.concatenate([s_ref[0, i, c + u, CLASS_ROWS[k]:CLASS_ROWS[k + 1]] for u in range(pair)], -1)
    o = dot(tables[0], jnp.concatenate([part(i, 0) for i in range(ADDENDS)], 0))
    for r, lane, v in add_tiles(o, n, lanes):
        u_ref[0, r:r + SUB, lane:lane + LANES] = v
    for k in (1, 2):
        d1, d2, d3 = (part(i, k) for i in range(ADDENDS))
        o = jnp.concatenate([dot(tables[2 * k - 1], jnp.concatenate([d1, d2], 0)),
                             dot(tables[2 * k], jnp.concatenate([d1, d3], 0))], 0)
        for r, lane, v in add_tiles(o, 2 * n, lanes):
            u_ref[2 * k - 1 + r // n, r % n:r % n + SUB, lane:lane + LANES] = v


def registers(pair, lanes):
    for u in range(pair):
        for y in range(Y_BLOCK):
            for lane in range(0, lanes, LANES):
                yield u, y, lane, (slice(y * SUB, (y + 1) * SUB), slice(u * lanes + lane, u * lanes + lane + LANES))


def gelu(h):
    k = 2.0 * math.sqrt(2.0 / math.pi)
    return h + h * jnp.tanh(h * (k + (4.0 * 0.044715 * k) * (h * h)))


def field_lanes(x_ref, y, c):
    return jnp.concatenate([x_ref[x, y, c] for x in range(X_GROUP)], -1)


def zero_spectrum(f_ref):
    def clear(c, _):
        f_ref[c] = jnp.zeros(f_ref.shape[1:], F32)
        return 0
    lax.fori_loop(0, f_ref.shape[0], clear, 0)


def forward_kernel(unit, x_ref, t0, t1, t2, f_ref, u_ref):
    f_ref = f_ref.at[0]
    width, lanes = x_ref.shape[2], f_ref.shape[-1]
    pair, per_step = unit
    tables = (t0[0], t1[0], t2[0])

    @pl.when(pl.program_id(1) == 0)
    def _():
        zero_spectrum(f_ref)

    def load(c, slot):
        for u in range(pair):
            for y in range(Y_BLOCK):
                row = field_lanes(x_ref, y, c + u)
                for k, v in enumerate(z_forward([row[SUB * j:SUB * j + SUB] for j in range(5)])):
                    u_ref[slot, k, y * SUB:(y + 1) * SUB, u * lanes:(u + 1) * lanes] = v

    def body(i, _):
        c = i * per_step
        count = per_step // pair
        for n in range(count + 1):
            if n < count:
                load(c + n * pair, n)
            if n:
                forward_stage(u_ref.at[n - 1], tables, f_ref, c + (n - 1) * pair, pair)
        return 0
    lax.fori_loop(0, width // per_step, body, 0)


def channel_product(first, x_ref, w_ref, p_ref, d_ref):
    blocks, width, depth, lanes = p_ref.shape
    rows = width * SUB
    ones = jnp.ones((w_ref.shape[2] - rows, blocks * lanes), BF16)
    full, (a, b, c) = w_ref[0], (w_ref[i, :, :rows] for i in range(ADDENDS))

    def load(j):
        z = slice(j * SUB, (j + 1) * SUB)
        if first:
            v = [x_ref[x, y, :, z, :] for y in range(blocks) for x in range(X_GROUP)]
        else:
            v = [x_ref[0, y, :, z, :] for y in range(blocks)]
        d_ref[j % 2] = jnp.concatenate(v, -1).reshape(rows, blocks * lanes)

    def product(j):
        d1, d2, d3 = split3(d_ref[j % 2])
        p = dot(full, jnp.concatenate([d1, ones], 0)) + dot(a, d2) + dot(a, d3) + dot(b, d1) + dot(b, d2) + dot(c, d1)
        for y in range(blocks):
            p_ref[y, :, j * SUB:(j + 1) * SUB, :] = p[:, y * lanes:(y + 1) * lanes].reshape(width, SUB, lanes)
    count = depth // SUB
    for j in range(count + 1):
        if j < count:
            load(j)
        if j:
            product(j - 1)


def layer_kernel(unit, first, *refs):
    p_ref, s_ref, *tabs = refs
    p_ref = p_ref.at[0]
    width, lanes = p_ref.shape[1], p_ref.shape[-1]
    batch = lanes // X_GROUP
    if first:
        *tabs, v_ref, f_hbm, a_ref, u_ref, f_ref, sem = tabs
        v_ref = v_ref.at[0]

        @pl.when(pl.program_id(1) == 0)
        def _():
            zero_spectrum(f_ref)
    else:
        *tabs, o_ref, a_ref = tabs
    inv, fwd = [t[0] for t in tabs[:5]], [t[0] for t in tabs[5:]]
    pair, per_step = unit

    def activate(c, slot):
        kept_rows = {}
        for u, y, lane, at in registers(pair, lanes):
            new = []
            for j, s in enumerate(z_inverse(*(a_ref[(slot, k) + at] for k in range(5)))):
                g = gelu(s + p_ref[y, c + u, SUB * j:SUB * j + SUB, lane:lane + LANES])
                new.append(g)
                if first:
                    v_ref[y, c + u, SUB * j:SUB * j + SUB, lane:lane + LANES] = g
                else:
                    kept_rows[j] = kept_rows.get(j, ()) + (g,)
            if first:
                for k, v in enumerate(z_forward(new)):
                    u_ref[(slot, k) + at] = v
            elif lane + LANES == lanes:
                for j, row in kept_rows.items():
                    store_field(o_ref, y, c + u, SUB * j, row, batch)
                kept_rows = {}

    def body(i, _):
        c = i * per_step
        count = per_step // pair
        for n in range(count + 2):
            if n < count:
                inverse_stage(s_ref, c + n * pair, pair, inv, a_ref.at[n])
            if 0 < n <= count:
                activate(c + (n - 1) * pair, n - 1)
            if first and n > 1:
                forward_stage(u_ref.at[n - 2], fwd, f_ref, c + (n - 2) * pair, pair)
        return 0
    lax.fori_loop(0, width // per_step, body, 0)

    if first:
        @pl.when(pl.program_id(1) == pl.num_programs(1) - 1)
        def _():
            copy = pltpu.make_async_copy(f_ref, f_hbm.at[pl.program_id(0)], sem)
            copy.start()
            copy.wait()


def store_field(o_ref, y, c, z, row, batch):
    lane = lax.broadcasted_iota(jnp.int32, row[0].shape, 1)
    for x in range(X_GROUP):
        at, off = divmod(x * batch, LANES)
        piece = row[at]
        if off + batch > LANES:
            piece = jnp.where(lane < off, row[at + 1], piece)
        if off:
            piece = pltpu.roll(piece, LANES - off, 1)
        o_ref[x, y, c, z:z + SUB, :] = piece[:, :batch]


def split_dot(left, right):
    a, b, c = left
    d1, d2, d3 = split3(right)
    return dot(a, d1) + dot(a, d2) + dot(a, d3) + dot(b, d1) + dot(b, d2) + dot(c, d1)


def x_forward(m_ref, f_ref, s_ref, slot):
    groups, width, lanes = f_ref.shape[0], f_ref.shape[1], f_ref.shape[-1]
    batch = lanes // X_GROUP
    halves = range(f_ref.shape[4])
    rights = []
    for h in halves:
        rows = []
        for g in range(groups):
            for x in range(X_GROUP):
                for p in range(2):
                    rows.append(jnp.concatenate([f_ref[g, c, 0, p, h, :, x * batch:(x + 1) * batch] for c in range(width)], -1))
        rights.append(jnp.concatenate(rows, 0))
    for h in halves:
        out = split_dot((m_ref[0], m_ref[1], m_ref[2]), rights[h])
        s_ref[:, slot, :, h * SUB:(h + 1) * SUB, :] = out.reshape(s_ref.shape[0], 2, SUB, width * batch)


def x_inverse(m_ref, t_ref, slot, s_ref):
    groups, width, lanes = s_ref.shape[0], s_ref.shape[2], s_ref.shape[-1]
    batch = lanes // X_GROUP
    halves = range(s_ref.shape[5])
    outs = []
    for h in halves:
        right = t_ref[:, slot, :, h * SUB:(h + 1) * SUB, :].reshape(t_ref.shape[0] * 2 * SUB, width * batch)
        outs.append(split_dot((m_ref[0], m_ref[1], m_ref[2]), right).reshape(groups, X_GROUP, 2, SUB, width * batch))
    for h in halves:
        for g in range(groups):
            for p in range(2):
                for c in range(width):
                    row = jnp.concatenate([outs[h][g, x, p, :, c * batch:(c + 1) * batch] for x in range(X_GROUP)], -1)
                    for i, d in enumerate(split3(row)):
                        s_ref[g, i, c, 0, p, h] = d


def mix(s_ref, re_w, im_w, t_ref, to, half, rows, re_rows, im_rows, re_s, im_s, re_t, im_t):
    own, slots, _, n_ky, lanes = s_ref.shape
    width = re_w.shape[2]
    batch = lanes // width
    some = slots // 2
    part_modes = some * n_ky
    pick = slice(half * some, (half + 1) * some)

    for w_ref, out in ((re_w, re_rows), (im_w, im_rows)):
        def lay(c, _):
            for k in range(own):
                for ky in range(n_ky):
                    at = (k * n_ky + ky) * SUB
                    rows[at:at + SUB, 0:width] = w_ref[k, ky, c]
            mat = jnp.concatenate([rows[pl.ds((k * n_ky + h * SUB) * SUB + kz, SUB, stride=SUB), :]
                                   for k in range(own) for kz in KZ_ORDER[pick] for h in range(n_ky // SUB)], 0)
            out[c] = mat.T[0:out.shape[1]]
            return 0
        lax.fori_loop(0, width, lay, 0)
    for p, out in enumerate((re_s, im_s)):
        out[...] = jnp.concatenate([s_ref[k, pick, p].reshape(part_modes, lanes) for k in range(own)], 0).T
    pair = 2

    def outputs(i, _):
        d = i * pair

        def inner(c, acc):
            at = pl.ds(pl.multiple_of(c * batch, SUB), batch)
            a, b = re_s[at, :], im_s[at, :]
            new = []
            for u in range(pair):
                p = jnp.broadcast_to(re_rows[c, pl.ds(d + u, 1), :], a.shape)
                q = jnp.broadcast_to(im_rows[c, pl.ds(d + u, 1), :], a.shape)
                new += [acc[2 * u] + (a * p - b * q), acc[2 * u + 1] + (a * q + b * p)]
            return tuple(new)
        zero = jnp.zeros((batch, own * part_modes), F32)
        acc = lax.fori_loop(0, width, inner, (zero,) * (2 * pair))
        for u in range(pair):
            at = pl.ds(pl.multiple_of((d + u) * batch, SUB), batch)
            re_t[at, :] = acc[2 * u]
            im_t[at, :] = acc[2 * u + 1]
        return 0
    lax.fori_loop(0, width // pair, outputs, 0)
    for p, got in enumerate((re_t, im_t)):
        back = got[...].T
        for k in range(own):
            t_ref[to[k], pick, p] = back[k * part_modes:(k + 1) * part_modes].reshape(some, n_ky, lanes)


class Place:
    def __init__(self):
        xs, ys = lax.axis_index('xs'), lax.axis_index('ys')
        data = lax.axis_index('data')
        c, x, y = xs % 2, xs // 2, ys
        self.core = (data, ys, 2 * x + 1 - c)
        self.x_chip = (data, ys, 2 * (1 - x) + c)
        self.y_chip = (data, 1 - ys, xs)
        p, q = lambda a, b: 2 * a + b, lambda a, b: 4 + 2 * a + b
        self.mine = SUB * c
        self.order = (p(1 - x, 1 - y), q(1 - y, 1 - x), p(1 - x, y), q(1 - y, x),
                      p(x, 1 - y), q(y, 1 - x), p(x, y), q(y, x))

    def enter(self):
        barrier = pltpu.get_barrier_semaphore()
        for device in (self.core, self.x_chip, self.y_chip):
            pl.semaphore_signal(barrier, inc=1, device_id=device, device_id_type=pl.DeviceIdType.MESH)
        pl.semaphore_wait(barrier, 3)


def remote(src, dst, send, recv, device):
    return pltpu.make_async_remote_copy(src_ref=src, dst_ref=dst, send_sem=send, recv_sem=recv, device_id=device,
                                        device_id_type=pl.DeviceIdType.MESH)


def half_slots(ref, k, half):
    some = ref.shape[1] // 2
    return ref.at[k, pl.ds(half * some, some)]


def reduce_kernel(first, m_ref, f_ref, x_ref, w_ref, out_ref, p_ref, d_ref, s_ref, r1, r2, r3,
                  send1, recv1, send2, recv2, send3, recv3):
    me = Place()
    step, last = pl.program_id(0), pl.num_programs(0) - 1
    slots = s_ref.shape[1]
    two, three = [], []

    def to_core(slot):
        return [remote(s_ref.at[SUB + me.order[t], slot], r1.at[t, slot], send1.at[slot, t], recv1.at[slot, t], me.core)
                for t in range(SUB)]
    for h in range(2):
        mine = [half_slots(s_ref, k, h) for k in me.order]
        two.append([remote(mine[t], half_slots(r2, t, h), send2.at[h, t], recv2.at[h, t], (me.x_chip, me.y_chip)[t % 2])
                    for t in range(4)])
        three.append([remote(mine[4 + t], half_slots(r3, t, h), send3.at[h, t], recv3.at[h, t], (me.y_chip, me.x_chip)[t])
                      for t in range(2)])

    def add(dst, a, b):
        def row(i, _):
            dst[i] = a[i] + b[i]
            return 0
        lax.fori_loop(0, dst.shape[0], row, 0)

    def from_core(h):
        arriving = [to_core(slot) for slot in range(h * slots // 2, (h + 1) * slots // 2)]
        for t in range(SUB):
            for copies in arriving:
                copies[t].wait_recv()
            to = half_slots(s_ref, me.order[t], h)
            add(to, to, half_slots(r1, t, h))
            if t < 4:
                two[h][t].start()

    def from_chip(h, these):
        for t in these:
            two[h][t].wait_recv()
            to = half_slots(s_ref, me.order[4 + t], h)
            add(to, to, half_slots(r2, t, h))
            if t < 2:
                three[h][t].start()

    def finish(h):
        from_chip(h, (2, 3))
        for t in range(2):
            three[h][t].wait_recv()
            add(half_slots(out_ref, t, h), half_slots(s_ref, me.order[6 + t], h), half_slots(r3, t, h))

    events = ((0, me.enter), (slots // 2, lambda: from_core(0)), (slots - 1, lambda: from_chip(0, (0, 1))),
              (slots + 1, lambda: from_core(1)), (slots + 3, lambda: finish(0)), (slots + 5, lambda: from_chip(1, (0, 1))))
    for at, event in events:
        pl.when(step == at)(event)

    @pl.when(step < slots)
    def _():
        x_forward(m_ref, f_ref, s_ref, step)
        for copy in to_core(step):
            copy.start()

    @pl.when(step >= slots // 2)
    def _():
        channel_product(first, x_ref, w_ref, p_ref.at[0], d_ref)

    @pl.when(step == last)
    def _():
        finish(1)
        for copies in [to_core(slot) for slot in range(slots)] + two + three:
            for copy in copies:
                copy.wait_send()


def gather_steps(units, half):
    return 2 + units // 2, 2 + units


def gather_kernel(first, layer, m_ref, s_ref, re_hbm, im_hbm, x_ref, w_ref, p_in, parts_ref, p_ref, d_ref, t_ref,
                  re_w, im_w, rows, re_rows, im_rows, re_s, im_s, re_t, im_t, w_sem, send, recv):
    me = Place()
    step, last = pl.program_id(0), pl.num_programs(0) - 1
    p3, q3, p2, q2, p1, q1, p0, q0 = me.order
    plan = [(p0, me.y_chip, 0), (q0, me.x_chip, 0), (p0, me.x_chip, 0), (q0, me.y_chip, 0), (p0, me.core, SUB), (q0, me.core, SUB),
            (p1, me.x_chip, 0), (q1, me.y_chip, 0)] + [(k, me.core, SUB) for k in (p1, q1, p2, q2, p3, q3)]
    copies = [[remote(half_slots(t_ref, k, h), half_slots(t_ref, k + up, h), send.at[h, n], recv.at[h, n], device)
               for n, (k, device, up) in enumerate(plan)] for h in range(2)]
    weights = [pltpu.make_async_copy(hbm.at[layer, me.mine + k], to.at[i], w_sem.at[n, i])
               for n, (hbm, to) in enumerate(((re_hbm, re_w), (im_hbm, im_w))) for i, k in enumerate((p0, q0))]

    def mix_half(h):
        mix(s_ref, re_w, im_w, t_ref, (p0, q0), h, rows, re_rows, im_rows, re_s, im_s, re_t, im_t)
        if h:
            pass_on(0)
        for copy in copies[h][:6]:
            copy.start()

    def begin():
        for copy in weights:
            copy.start()
        me.enter()
        for copy in weights:
            copy.wait()
        mix_half(0)

    def pass_on(h):
        for n in range(2):
            copies[h][n].wait_recv()
            copies[h][6 + n].start()
        for n in range(2):
            copies[h][SUB + n].start()

    def finish(h):
        for n, arrived in enumerate((2, 3, 6, 7)):
            copies[h][arrived].wait_recv()
            copies[h][10 + n].start()
        for n in (4, 5, *range(SUB, len(plan))):
            copies[h][n].wait_recv()

    half = t_ref.shape[1] // 2
    x_from, x_then = gather_steps(last + 1 - 2 - half, half)
    for at, event in ((0, begin), (1, lambda: mix_half(1)), (x_from, lambda: finish(0)), (x_from + 2, lambda: pass_on(1)),
                      (x_then, lambda: finish(1))):
        pl.when(step == at)(event)

    @pl.when((step >= 2) & (step < x_then))
    def _():
        channel_product(first, x_ref, w_ref, p_ref.at[0], d_ref)

    @pl.when((step >= x_from) & (step < x_from + half))
    def _():
        x_inverse(m_ref, t_ref, step - x_from, parts_ref)

    @pl.when(step >= x_then)
    def _():
        x_inverse(m_ref, t_ref, step - x_then + half, parts_ref)

    @pl.when(step == last)
    def _():
        for h in range(2):
            for copy in copies[h]:
                copy.wait_send()


def block(shape, index, slot=None, **kwargs):
    def index_map(*at):
        return tuple(0 if k == 'o' else slot(at[0]) if k == 's' else at['ij'.index(k)] for k in index)
    return pl.BlockSpec(shape, index_map, **kwargs)


def bf16_addends(table):
    out = []
    for _ in range(ADDENDS):
        out.append(lax.reduce_precision(table, exponent_bits=SUB, mantissa_bits=7))
        table = table - out[-1]
    return jnp.stack(out).astype(BF16)


def solution(mesh):
    row_devs, col_devs = mesh.shape['ys'], mesh.shape['xs']

    def local_layers(field, spec_real, spec_imag, mix_weight, bias):
        batch, x_loc, y_loc, grid_z, width = field.shape
        modes = spec_real.shape[3]
        grid_x, grid_y = x_loc * col_devs, y_loc * row_devs
        groups, blocks = x_loc // X_GROUP, y_loc // Y_BLOCK
        lanes = X_GROUP * batch
        kx, ky = kept(modes, grid_x), kept(modes, grid_y)
        n_kx, n_ky = len(kx), len(ky)
        x_index, y_index = lax.axis_index('xs'), lax.axis_index('ys')
        fwd_np, inv_np = all_tables(blocks, ky, grid_y, grid_z, grid_x * grid_y * grid_z)
        fwd, inv = [jnp.asarray(t) for t in fwd_np], [jnp.asarray(t) for t in inv_np]

        turn = 2.0 * math.pi * (kx[:, None] * np.arange(grid_x)[None, :] % grid_x) / grid_x
        cos, sin = np.cos(turn), np.sin(turn)
        fwd_x = np.stack([np.stack([cos, sin], -1), np.stack([-sin, cos], -1)], 1)
        inv_x = np.transpose(fwd_x, (2, 3, 0, 1))
        fwd_x = fwd_x.reshape(n_kx, 2, col_devs, x_loc, 2).transpose(2, 0, 1, 3, 4).reshape(col_devs, 2 * n_kx, 2 * x_loc)
        inv_x = inv_x.reshape(col_devs, 2 * x_loc, 2 * n_kx)
        odd = (jnp.arange(16 * x_loc) % 2 * y_index)[:, None]

        core, x_chip = x_index % 2, x_index // 2

        def x_table(tables, axis):
            wide = np.kron(tables, np.eye(SUB)).astype(np.float32)
            t = lax.dynamic_index_in_dim(jnp.asarray(wide), x_index, 0, keepdims=False)
            t = jnp.where(core == 1, jnp.roll(t, SUB * n_kx, axis), t)
            return bf16_addends(jnp.where(odd == 1, -t, t))
        fwd_x, inv_x = x_table(fwd_x, 0), x_table(inv_x, 1)
        eye = jnp.eye(Z_BLOCK, dtype=F32)
        def point_table(layer):
            w = bf16_addends((0.5 * mix_weight[layer].T[:, None, :, None] * eye[None, :, None, :]).reshape(width * SUB, width * SUB))
            b = bf16_addends(jnp.broadcast_to(0.5 * bias[layer][:, None], (width, SUB)).reshape(width * SUB))
            b = jnp.pad(jnp.stack([b.T, 0 * b.T, 0 * b.T]), ((0, 0), (0, 0), (0, 2 * SUB - 3)))
            return jnp.concatenate([w, b], -1)
        point_w = [point_table(layer) for layer in range(2)]

        real_w, imag_w = (jnp.swapaxes(w, 3, 4) for w in (spec_real, spec_imag))
        v = jnp.swapaxes(jnp.moveaxis(field, 0, -1), 2, 3)
        grid = (groups, blocks)
        params = pltpu.CompilerParams(vmem_limit_bytes=VMEM_LIMIT)
        spec_shape = jax.ShapeDtypeStruct((groups, width, 256, lanes), F32)
        in_block = block((X_GROUP, Y_BLOCK, width, grid_z, batch), 'ijooo')
        mid_block = block((1, Y_BLOCK, width, grid_z, lanes), 'ijooo')
        part_block = block((1, ADDENDS, width, CLASS_ROWS[-1], lanes), 'ioooo')
        mid_shape = jax.ShapeDtypeStruct((groups, y_loc, width, grid_z, lanes), F32)
        anywhere = pl.BlockSpec(memory_space=pl.ANY)

        def stage(unit):
            return pltpu.VMEM((unit[1] // unit[0], 5, Y_BLOCK * SUB, unit[0] * lanes), F32)
        w_block = block((ADDENDS, width * SUB, width * SUB + 2 * SUB), 'ooo')

        units = y_loc // HALF_BLOCK

        def half_block(first, half, start):
            shape = (HALF_BLOCK, width, grid_z) + ((batch,) if first else (lanes,))
            return pl.BlockSpec((X_GROUP if first else 1,) + shape,
                                lambda j: (half, jnp.clip(j - start, 0, units - 1), 0, 0, 0))

        def table_specs(tables):
            return [block((1,) + t.shape[1:], 'joo') for t in tables]

        f = pl.pallas_call(
            functools.partial(forward_kernel, FORWARD_UNIT), grid=grid, out_shape=spec_shape,
            in_specs=[in_block] + table_specs(fwd),
            out_specs=block((1, width, 256, lanes), 'iooo'),
            scratch_shapes=[stage(FORWARD_UNIT)], compiler_params=params, name='forward')(v, *fwd)

        own, slots, halves = 2, SUB, n_ky // SUB
        unit = (slots, 2, n_ky, width * batch)
        own_block = block((own,) + unit, 'ooooo')
        x_block = block((ADDENDS, 16 * x_loc, 16 * x_loc), 'ooo')
        dma = pltpu.SemaphoreType.DMA
        half_rows = pltpu.VMEM((2, width * SUB, HALF_BLOCK * lanes), F32)

        def exchange(number):
            return pltpu.CompilerParams(vmem_limit_bytes=VMEM_LIMIT, collective_id=number, has_side_effects=True)

        def across(f, layer, source):
            first = layer == 0
            s, p = pl.pallas_call(
                functools.partial(reduce_kernel, first), grid=(slots // 2 + units,),
                out_shape=(jax.ShapeDtypeStruct((own,) + unit, F32), mid_shape),
                in_specs=[x_block,
                          block((groups, width, 1, 2, halves, SUB, lanes), 'oosoooo', lambda j: jnp.minimum(j, slots - 1)),
                          half_block(first, 0, slots // 2), w_block],
                out_specs=(own_block, half_block(False, 0, slots // 2)),
                scratch_shapes=[half_rows] + [pltpu.VMEM((n,) + unit, F32) for n in (n_kx, SUB, 4, 2)]
                + [dma((slots, SUB))] * 2 + [dma((2, n)) for n in (4, 4, 2, 2)],
                compiler_params=exchange(2 * layer), name='reduce')(
                    fwd_x, f.reshape(groups, width, slots, 2, halves, SUB, lanes), source, point_w[layer])
            x_from, x_then = gather_steps(units, slots // 2)

            def inverse_slot(j):
                return jnp.where(j < x_then, jnp.clip(j - x_from, 0, slots // 2 - 1), j - x_then + slots // 2)
            parts, p = pl.pallas_call(
                functools.partial(gather_kernel, first, layer), grid=(units + 2 + slots // 2,),
                out_shape=(jax.ShapeDtypeStruct((groups, ADDENDS, width, slots, 2, halves, SUB, lanes), BF16), mid_shape),
                in_specs=[x_block, own_block, anywhere, anywhere, half_block(first, 1, 2), w_block, anywhere],
                out_specs=(block((groups, ADDENDS, width, 1, 2, halves, SUB, lanes), 'ooosoooo', inverse_slot),
                           half_block(False, 1, 2)),
                input_output_aliases={6: 1},
                scratch_shapes=[half_rows, pltpu.VMEM((n_kx,) + unit, F32)]
                + [pltpu.VMEM((own, n_ky, width, SUB, width), F32)] * 2
                + [pltpu.VMEM((own * n_ky * SUB, LANES), F32)] + [pltpu.VMEM((width, 24, LANES), F32)] * 2
                + [pltpu.VMEM((width * batch, own * slots * n_ky // 2), F32)] * 4
                + [dma((2, 2)), dma((2, 14)), dma((2, 14))],
                compiler_params=exchange(2 * layer + 1), name='gather')(
                    inv_x, s, real_w, imag_w, source, point_w[layer], p)
            return parts.reshape(groups, ADDENDS, width, CLASS_ROWS[-1], lanes), p

        parts, p = across(f, 0, v)
        v1, f = pl.pallas_call(
            functools.partial(layer_kernel, FIRST_UNIT, True), grid=grid, out_shape=(mid_shape, spec_shape),
            in_specs=[mid_block, part_block] + table_specs(inv) + table_specs(fwd),
            out_specs=(mid_block, anywhere),
            scratch_shapes=[stage(FIRST_UNIT)] * 2 + [pltpu.VMEM((width, 256, lanes), F32), pltpu.SemaphoreType.DMA],
            compiler_params=params, name='layer_first')(p, parts, *inv, *fwd)
        parts, p = across(f, 1, v1)
        out = pl.pallas_call(
            functools.partial(layer_kernel, LAST_UNIT, False), grid=grid,
            out_shape=jax.ShapeDtypeStruct((x_loc, y_loc, width, grid_z, batch), F32),
            in_specs=[mid_block, part_block] + table_specs(inv), out_specs=in_block, scratch_shapes=[stage(LAST_UNIT)],
            compiler_params=params, name='layer_last')(p, parts, *inv)
        return jnp.moveaxis(jnp.swapaxes(out, 2, 3), -1, 0)

    field_spec = P('data', 'xs', 'ys', None, None)
    return jax.shard_map(local_layers, mesh=mesh, in_specs=(field_spec, P(), P(), P(), P()), out_specs=field_spec, check_vma=False)
```

```python
import functools
import math

import jax
import jax.numpy as jnp
import ml_dtypes
import numpy as np
from jax import lax
from jax.experimental import pallas as pl
from jax.experimental.pallas import tpu as pltpu
from jax.sharding import PartitionSpec as P

F32 = jnp.float32
BF16 = jnp.bfloat16
VMEM_LIMIT = 64 * 1024 * 1024 - 65536

SUB = 8
X_GROUP = 8
Y_BLOCK = 4
HALF_BLOCK = 2
Z_BLOCK = 8
KZ_CLASS = ((0, 5), (1, 6, 4), (2, 7, 3))
KZ_ORDER = tuple(kz for group in KZ_CLASS for kz in group)
CLASS_ROWS = (0, 64, 160, 256)
LANES = 128
ADDENDS = 3
CHUNKS = ((0, 2), (2, 6), (6, 8))
FORWARD_UNIT = (2, 10)
FIRST_UNIT = (2, 10)
LAST_UNIT = (1, 10)
ROOT5_4 = math.sqrt(5.0) / 4.0
SIN_1 = math.sin(2.0 * math.pi / 5.0)
SIN_RATIO = math.sin(4.0 * math.pi / 5.0) / SIN_1


def kz_sign(kz):
    return 0 if kz % 5 == 0 else (1 if kz % 5 < 3 else -1)


def kept(modes, size):
    return np.concatenate([np.arange(modes), np.arange(size - modes, size)])


def pieces(table):
    rest = np.asarray(table, np.float32)
    out = []
    for _ in range(ADDENDS):
        out.append(rest.astype(ml_dtypes.bfloat16))
        rest = rest - out[-1].astype(np.float32)
    return out


def yz_angles(kz, y_pos, ky, grid_y, grid_z):
    z_pos = np.arange(Z_BLOCK)
    turn = (ky[:, None, None] * y_pos[None, :, None] % grid_y) / grid_y + kz * z_pos[None, None, :] / grid_z
    return 2.0 * math.pi * turn


def forward_table(group, y_pos, ky, grid_y, grid_z):
    rows = []
    for kz in group:
        t, s = yz_angles(kz, y_pos, ky, grid_y, grid_z), kz_sign(kz)
        real, imag = [np.cos(t)], [-np.sin(t)]
        if s:
            real.append(-s * SIN_1 * np.sin(t))
            imag.append(-s * SIN_1 * np.cos(t))
        rows += [np.stack(part, 1).reshape(len(ky), -1) for part in (real, imag)]
    return np.concatenate(rows, 0)


def inverse_table(group, y_pos, ky, grid_y, grid_z, points):
    cols = []
    for kz in group:
        t, s = yz_angles(kz, y_pos, ky, grid_y, grid_z).transpose(1, 2, 0), kz_sign(kz)
        w = (0.5 if kz == 0 else 1.0) / points
        real, imag = [w * np.cos(t)], [-w * np.sin(t)]
        if s:
            real.append(s * SIN_1 * w * np.sin(t))
            imag.append(s * SIN_1 * w * np.cos(t))
        cols += [np.stack(part, 0).reshape(-1, len(ky)) for part in (real, imag)]
    return np.concatenate(cols, 1)


def all_tables(blocks, ky, grid_y, grid_z, points):
    fwd, inv = [[], [], []], [[], [], [], [], []]
    for block in range(blocks):
        y_pos = np.arange(Y_BLOCK) + block * Y_BLOCK
        for k, group in enumerate(KZ_CLASS):
            a, b, c = pieces(forward_table(group, y_pos, ky, grid_y, grid_z))
            n = np.zeros_like(a)
            if k == 0:
                fwd[k].append(np.concatenate([a, a, a, b, b, c], 1))
            else:
                fwd[k].append(np.block([[a, a, a, b], [c, b, n, n]]))
            a, b, c = pieces(inverse_table(group, y_pos, ky, grid_y, grid_z, points))
            n = np.zeros_like(a)
            if k == 0:
                inv[0].append(np.block([[a, a, a], [b, b, n], [c, n, n]]))
            else:
                inv[2 * k - 1].append(np.block([[a, a], [b, b]]))
                inv[2 * k].append(np.concatenate([c, a], 1))
    return [np.stack(t) for t in fwd], [np.stack(t) for t in inv]


def split3(v):
    d1 = v.astype(BF16)
    rest = v - d1.astype(F32)
    d2 = rest.astype(BF16)
    return d1, d2, (rest - d2.astype(F32)).astype(BF16)


def dot(a, b):
    return jnp.dot(a, b, preferred_element_type=F32)


def z_forward(v):
    v0, v1, v2, v3, v4 = v
    t1, t2, e1, e2 = v1 + v4, v2 + v3, v1 - v4, v2 - v3
    total = t1 + t2
    mid, dif = v0 - 0.25 * total, ROOT5_4 * (t1 - t2)
    return v0 + total, mid + dif, e1 + SIN_RATIO * e2, mid - dif, SIN_RATIO * e1 - e2


def z_inverse(a0, a1, b1, a2, b2):
    total = a1 + a2
    mid, dif = a0 - 0.25 * total, ROOT5_4 * (a1 - a2)
    p, q = mid + dif, mid - dif
    r, s = b1 + SIN_RATIO * b2, SIN_RATIO * b1 - b2
    return a0 + total, p - r, q - s, q + s, p + r


def split_tiles(u_ref, channels):
    rows, lanes = u_ref.shape[1:]
    out = [[], [], []]
    for k in channels:
        for r in range(0, rows, 2 * SUB):
            cells = [split3(u_ref[k, r:r + 2 * SUB, lane:lane + LANES]) for lane in range(0, lanes, LANES)]
            for i in range(ADDENDS):
                out[i].append(jnp.concatenate([cell[i] for cell in cells], -1))
    return [jnp.concatenate(rows, 0) for rows in out]


def add_tiles(o, n, lanes, first=0):
    for r in range(0, n, SUB):
        for lane in range(0, lanes, LANES):
            cells = [o[b + r:b + r + SUB, lane:lane + LANES] for b in range(0, o.shape[0], n)]
            yield r, lane, functools.reduce(jnp.add, cells)


def forward_stage(u_ref, tables, f_ref, c, pair):
    lanes = f_ref.shape[-1]
    for k, channels in enumerate(((0,), (1, 2), (3, 4))):
        d = split_tiles(u_ref, channels)
        o = dot(tables[k], jnp.concatenate([d[i] for i in ((0, 1, 2, 0) if k else (0, 1, 2, 0, 1, 0))], 0))
        n = CLASS_ROWS[k + 1] - CLASS_ROWS[k]
        for r, lane, v in add_tiles(o, n, pair * lanes):
            at = (c + lane // lanes, slice(CLASS_ROWS[k] + r, CLASS_ROWS[k] + r + SUB), slice(lane % lanes, lane % lanes + LANES))
            f_ref[at] += v


def inverse_stage(s_ref, c, pair, tables, u_ref):
    n, lanes = u_ref.shape[1:]

    def part(i, k):
        return jnp.concatenate([s_ref[0, i, c + u, CLASS_ROWS[k]:CLASS_ROWS[k + 1]] for u in range(pair)], -1)
    o = dot(tables[0], jnp.concatenate([part(i, 0) for i in range(ADDENDS)], 0))
    for r, lane, v in add_tiles(o, n, lanes):
        u_ref[0, r:r + SUB, lane:lane + LANES] = v
    for k in (1, 2):
        d1, d2, d3 = (part(i, k) for i in range(ADDENDS))
        o = jnp.concatenate([dot(tables[2 * k - 1], jnp.concatenate([d1, d2], 0)),
                             dot(tables[2 * k], jnp.concatenate([d1, d3], 0))], 0)
        for r, lane, v in add_tiles(o, 2 * n, lanes):
            u_ref[2 * k - 1 + r // n, r % n:r % n + SUB, lane:lane + LANES] = v


def registers(pair, lanes):
    for u in range(pair):
        for y in range(Y_BLOCK):
            for lane in range(0, lanes, LANES):
                yield u, y, lane, (slice(y * SUB, (y + 1) * SUB), slice(u * lanes + lane, u * lanes + lane + LANES))


def gelu(h):
    k = 2.0 * math.sqrt(2.0 / math.pi)
    return h + h * jnp.tanh(h * (k + (4.0 * 0.044715 * k) * (h * h)))


def field_lanes(x_ref, y, c):
    return jnp.concatenate([x_ref[x, y, c] for x in range(X_GROUP)], -1)


def zero_spectrum(f_ref):
    def clear(c, _):
        f_ref[c] = jnp.zeros(f_ref.shape[1:], F32)
        return 0
    lax.fori_loop(0, f_ref.shape[0], clear, 0)


def forward_kernel(unit, x_ref, t0, t1, t2, f_ref, u_ref):
    f_ref = f_ref.at[0]
    width, lanes = x_ref.shape[2], f_ref.shape[-1]
    pair, per_step = unit
    tables = (t0[0], t1[0], t2[0])
    start = pl.program_id(2) * width

    @pl.when((pl.program_id(1) == 0) & (start == 0))
    def _():
        zero_spectrum(f_ref)

    def load(c, slot):
        for u in range(pair):
            for y in range(Y_BLOCK):
                row = field_lanes(x_ref, y, c + u)
                for k, v in enumerate(z_forward([row[SUB * j:SUB * j + SUB] for j in range(5)])):
                    u_ref[slot, k, y * SUB:(y + 1) * SUB, u * lanes:(u + 1) * lanes] = v

    def body(i, _):
        c = i * per_step
        count = per_step // pair
        for n in range(count + 1):
            if n < count:
                load(c + n * pair, n)
            if n:
                forward_stage(u_ref.at[n - 1], tables, f_ref, start + c + (n - 1) * pair, pair)
        return 0
    lax.fori_loop(0, width // per_step, body, 0)


def channel_product(first, x_ref, w_ref, p_ref, d_ref):
    blocks, width, depth, lanes = p_ref.shape
    rows = width * SUB
    ones = jnp.ones((w_ref.shape[2] - rows, blocks * lanes), BF16)
    full, (a, b, c) = w_ref[0], (w_ref[i, :, :rows] for i in range(ADDENDS))

    def load(j):
        z = slice(j * SUB, (j + 1) * SUB)
        if first:
            v = [x_ref[x, y, :, z, :] for y in range(blocks) for x in range(X_GROUP)]
        else:
            v = [x_ref[0, y, :, z, :] for y in range(blocks)]
        d_ref[j % 2] = jnp.concatenate(v, -1).reshape(rows, blocks * lanes)

    def product(j):
        d1, d2, d3 = split3(d_ref[j % 2])
        p = dot(full, jnp.concatenate([d1, ones], 0)) + dot(a, d2) + dot(a, d3) + dot(b, d1) + dot(b, d2) + dot(c, d1)
        for y in range(blocks):
            p_ref[y, :, j * SUB:(j + 1) * SUB, :] = p[:, y * lanes:(y + 1) * lanes].reshape(width, SUB, lanes)
    count = depth // SUB
    for j in range(count + 1):
        if j < count:
            load(j)
        if j:
            product(j - 1)


def layer_kernel(unit, first, *refs):
    p_ref, s_ref, *tabs = refs
    p_ref = p_ref.at[0]
    width, lanes = p_ref.shape[1], p_ref.shape[-1]
    batch = lanes // X_GROUP
    start = pl.program_id(2) * width
    if first:
        *tabs, v_ref, f_hbm, a_ref, u_ref, f_ref, sem = tabs
        v_ref = v_ref.at[0]

        @pl.when((pl.program_id(1) == 0) & (start == 0))
        def _():
            zero_spectrum(f_ref)
    else:
        *tabs, o_ref, a_ref = tabs
    inv, fwd = [t[0] for t in tabs[:5]], [t[0] for t in tabs[5:]]
    pair, per_step = unit

    def activate(c, slot):
        kept_rows = {}
        for u, y, lane, at in registers(pair, lanes):
            new = []
            for j, s in enumerate(z_inverse(*(a_ref[(slot, k) + at] for k in range(5)))):
                g = gelu(s + p_ref[y, c + u, SUB * j:SUB * j + SUB, lane:lane + LANES])
                new.append(g)
                if first:
                    v_ref[y, c + u, SUB * j:SUB * j + SUB, lane:lane + LANES] = g
                else:
                    kept_rows[j] = kept_rows.get(j, ()) + (g,)
            if first:
                for k, v in enumerate(z_forward(new)):
                    u_ref[(slot, k) + at] = v
            elif lane + LANES == lanes:
                for j, row in kept_rows.items():
                    store_field(o_ref, y, c + u, SUB * j, row, batch)
                kept_rows = {}

    def body(i, _):
        c = i * per_step
        count = per_step // pair
        for n in range(count + 2):
            if n < count:
                inverse_stage(s_ref, start + c + n * pair, pair, inv, a_ref.at[n])
            if 0 < n <= count:
                activate(c + (n - 1) * pair, n - 1)
            if first and n > 1:
                forward_stage(u_ref.at[n - 2], fwd, f_ref, start + c + (n - 2) * pair, pair)
        return 0
    lax.fori_loop(0, width // per_step, body, 0)

    if first:
        @pl.when((pl.program_id(1) == pl.num_programs(1) - 1) & (start > 0))
        def _():
            copy = pltpu.make_async_copy(f_ref, f_hbm.at[pl.program_id(0)], sem)
            copy.start()
            copy.wait()


def store_field(o_ref, y, c, z, row, batch):
    lane = lax.broadcasted_iota(jnp.int32, row[0].shape, 1)
    for x in range(X_GROUP):
        at, off = divmod(x * batch, LANES)
        piece = row[at]
        if off + batch > LANES:
            piece = jnp.where(lane < off, row[at + 1], piece)
        if off:
            piece = pltpu.roll(piece, LANES - off, 1)
        o_ref[x, y, c, z:z + SUB, :] = piece[:, :batch]


def split_dot(left, right):
    a, b, c = left
    d1, d2, d3 = split3(right)
    return dot(a, d1) + dot(a, d2) + dot(a, d3) + dot(b, d1) + dot(b, d2) + dot(c, d1)


def x_forward(m_ref, f_ref, s_ref, slot):
    groups, width, lanes = f_ref.shape[0], f_ref.shape[1], f_ref.shape[-1]
    batch = lanes // X_GROUP
    halves = range(f_ref.shape[4])
    rights = []
    for h in halves:
        rows = []
        for g in range(groups):
            for x in range(X_GROUP):
                for p in range(2):
                    rows.append(jnp.concatenate([f_ref[g, c, 0, p, h, :, x * batch:(x + 1) * batch] for c in range(width)], -1))
        rights.append(jnp.concatenate(rows, 0))
    for h in halves:
        out = split_dot((m_ref[0], m_ref[1], m_ref[2]), rights[h])
        s_ref[:, slot, :, h * SUB:(h + 1) * SUB, :] = out.reshape(s_ref.shape[0], 2, SUB, width * batch)


def x_inverse(m_ref, t_ref, slot, s_ref):
    groups, width, lanes = s_ref.shape[0], s_ref.shape[2], s_ref.shape[-1]
    batch = lanes // X_GROUP
    halves = range(s_ref.shape[5])
    outs = []
    for h in halves:
        right = t_ref[:, slot, :, h * SUB:(h + 1) * SUB, :].reshape(t_ref.shape[0] * 2 * SUB, width * batch)
        outs.append(split_dot((m_ref[0], m_ref[1], m_ref[2]), right).reshape(groups, X_GROUP, 2, SUB, width * batch))
    for h in halves:
        for g in range(groups):
            for p in range(2):
                for c in range(width):
                    row = jnp.concatenate([outs[h][g, x, p, :, c * batch:(c + 1) * batch] for x in range(X_GROUP)], -1)
                    for i, d in enumerate(split3(row)):
                        s_ref[g, i, c, 0, p, h] = d


def mix(s_ref, re_w, im_w, t_ref, to, chunk, rows, re_rows, im_rows, re_s, im_s, re_t, im_t):
    own, _, _, n_ky, lanes = s_ref.shape
    width = re_w.shape[2]
    batch = lanes // width
    some = chunk[1] - chunk[0]
    part_modes = some * n_ky
    pick, modes = slice(*chunk), slice(0, own * part_modes)

    for w_ref, out in ((re_w, re_rows), (im_w, im_rows)):
        def lay(c, _):
            for k in range(own):
                for ky in range(n_ky):
                    at = (k * n_ky + ky) * SUB
                    rows[at:at + SUB, 0:width] = w_ref[k, ky, c]
            mat = jnp.concatenate([rows[pl.ds((k * n_ky + h * SUB) * SUB + kz, SUB, stride=SUB), :]
                                   for k in range(own) for kz in KZ_ORDER[pick] for h in range(n_ky // SUB)], 0)
            out[c, :, modes] = mat.T[0:out.shape[1]]
            return 0
        lax.fori_loop(0, width, lay, 0)
    for p, out in enumerate((re_s, im_s)):
        out[:, modes] = jnp.concatenate([s_ref[k, pick, p].reshape(part_modes, lanes) for k in range(own)], 0).T
    pair = 2

    def outputs(i, _):
        d = i * pair

        def inner(c, acc):
            at = pl.ds(pl.multiple_of(c * batch, SUB), batch)
            a, b = re_s[at, modes], im_s[at, modes]
            new = []
            for u in range(pair):
                p = jnp.broadcast_to(re_rows[c, pl.ds(d + u, 1), modes], a.shape)
                q = jnp.broadcast_to(im_rows[c, pl.ds(d + u, 1), modes], a.shape)
                new += [acc[2 * u] + (a * p - b * q), acc[2 * u + 1] + (a * q + b * p)]
            return tuple(new)
        zero = jnp.zeros((batch, own * part_modes), F32)
        acc = lax.fori_loop(0, width, inner, (zero,) * (2 * pair))
        for u in range(pair):
            at = pl.ds(pl.multiple_of((d + u) * batch, SUB), batch)
            re_t[at, modes] = acc[2 * u]
            im_t[at, modes] = acc[2 * u + 1]
        return 0
    lax.fori_loop(0, width // pair, outputs, 0)
    for p, got in enumerate((re_t, im_t)):
        back = got[:, modes].T
        for k in range(own):
            t_ref[to[k], pick, p] = back[k * part_modes:(k + 1) * part_modes].reshape(some, n_ky, lanes)


class Place:
    def __init__(self):
        xs, ys = lax.axis_index('xs'), lax.axis_index('ys')
        data = lax.axis_index('data')
        c, x, y = xs % 2, xs // 2, ys
        self.core = (data, ys, 2 * x + 1 - c)
        self.x_chip = (data, ys, 2 * (1 - x) + c)
        self.y_chip = (data, 1 - ys, xs)
        p, q = lambda a, b: 2 * a + b, lambda a, b: 4 + 2 * a + b
        self.mine = SUB * c
        self.order = (p(1 - x, 1 - y), q(1 - y, 1 - x), p(1 - x, y), q(1 - y, x),
                      p(x, 1 - y), q(y, 1 - x), p(x, y), q(y, x))

    def enter(self):
        barrier = pltpu.get_barrier_semaphore()
        for device in (self.core, self.x_chip, self.y_chip):
            pl.semaphore_signal(barrier, inc=1, device_id=device, device_id_type=pl.DeviceIdType.MESH)
        pl.semaphore_wait(barrier, 3)


def remote(src, dst, send, recv, device):
    return pltpu.make_async_remote_copy(src_ref=src, dst_ref=dst, send_sem=send, recv_sem=recv, device_id=device,
                                        device_id_type=pl.DeviceIdType.MESH)


def chunk_of(ref, k, n):
    low, high = CHUNKS[n]
    return ref.at[k, pl.ds(low, high - low)]


def reduce_kernel(first, m_ref, f_ref, x_ref, w_ref, out_ref, p_ref, d_ref, s_ref, r1, r2, r3,
                  send1, recv1, send2, recv2, send3, recv3):
    me = Place()
    step, last = pl.program_id(0), pl.num_programs(0) - 1
    slots = s_ref.shape[1]
    two, three = [], []

    def to_core(slot):
        return [remote(s_ref.at[SUB + me.order[t], slot], r1.at[t, slot], send1.at[slot, t], recv1.at[slot, t], me.core)
                for t in range(SUB)]
    for h in range(len(CHUNKS)):
        mine = [chunk_of(s_ref, k, h) for k in me.order]
        two.append([remote(mine[t], chunk_of(r2, t, h), send2.at[h, t], recv2.at[h, t], (me.x_chip, me.y_chip)[t % 2])
                    for t in range(4)])
        three.append([remote(mine[4 + t], chunk_of(r3, t, h), send3.at[h, t], recv3.at[h, t], (me.y_chip, me.x_chip)[t])
                      for t in range(2)])

    def add(dst, a, b):
        def row(i, _):
            dst[i] = a[i] + b[i]
            return 0
        lax.fori_loop(0, dst.shape[0], row, 0)

    def from_core(h):
        arriving = [to_core(slot) for slot in range(*CHUNKS[h])]
        for t in range(SUB):
            for copies in arriving:
                copies[t].wait_recv()
            to = chunk_of(s_ref, me.order[t], h)
            add(to, to, chunk_of(r1, t, h))
            if t < 4:
                two[h][t].start()

    def from_chip(h, these):
        for t in these:
            two[h][t].wait_recv()
            to = chunk_of(s_ref, me.order[4 + t], h)
            add(to, to, chunk_of(r2, t, h))
            if t < 2:
                three[h][t].start()

    def finish(h):
        from_chip(h, (2, 3))
        for t in range(2):
            three[h][t].wait_recv()
            add(chunk_of(out_ref, t, h), chunk_of(s_ref, me.order[6 + t], h), chunk_of(r3, t, h))

    events = ((0, me.enter), (2, lambda: from_core(0)), (slots - 3, lambda: from_chip(0, (0, 1))), (slots - 2, lambda: from_core(1)),
              (slots, lambda: from_core(2)), (slots + 3, lambda: finish(0)), (slots + 5, lambda: from_chip(1, (0, 1))),
              (slots + 12, lambda: from_chip(2, (0, 1))))
    for at, event in events:
        pl.when(step == at)(event)

    @pl.when(step < slots)
    def _():
        x_forward(m_ref, f_ref, s_ref, step)
        for copy in to_core(step):
            copy.start()

    @pl.when(step >= slots)
    def _():
        channel_product(first, x_ref, w_ref, p_ref.at[0], d_ref)

    @pl.when(step == last)
    def _():
        finish(1)
        finish(2)
        for copies in [to_core(slot) for slot in range(slots)] + two + three:
            for copy in copies:
                copy.wait_send()


def inverse_slot(step):
    return jnp.where(step < SUB, jnp.clip(step - 6, 0, 1), jnp.clip(step - 14, 1, SUB - 1))


def gather_kernel(first, layer, m_ref, s_ref, re_hbm, im_hbm, x_ref, w_ref, p_in, parts_ref, p_ref, d_ref, t_ref,
                  re_w, im_w, rows, re_rows, im_rows, re_s, im_s, re_t, im_t, w_sem, send_sem, recv_sem):
    me = Place()
    step, last = pl.program_id(0), pl.num_programs(0) - 1
    p3, q3, p2, q2, p1, q1, p0, q0 = me.order
    plan = [(p0, me.y_chip, 0), (q0, me.x_chip, 0), (p0, me.x_chip, 0), (q0, me.y_chip, 0), (p0, me.core, SUB), (q0, me.core, SUB),
            (p1, me.x_chip, 0), (q1, me.y_chip, 0)] + [(k, me.core, SUB) for k in (p1, q1, p2, q2, p3, q3)]
    copies = [[remote(chunk_of(t_ref, k, h), chunk_of(t_ref, k + up, h), send_sem.at[h, n], recv_sem.at[h, n], device)
               for n, (k, device, up) in enumerate(plan)] for h in range(len(CHUNKS))]
    weights = [pltpu.make_async_copy(hbm.at[layer, me.mine + k], to.at[i], w_sem.at[n, i])
               for n, (hbm, to) in enumerate(((re_hbm, re_w), (im_hbm, im_w))) for i, k in enumerate((p0, q0))]

    def mixed(h):
        mix(s_ref, re_w, im_w, t_ref, (p0, q0), CHUNKS[h], rows, re_rows, im_rows, re_s, im_s, re_t, im_t)

    def send(h):
        for copy in copies[h][:6]:
            copy.start()

    def begin():
        for copy in weights:
            copy.start()
        me.enter()
        for copy in weights:
            copy.wait()
        mixed(0)
        send(0)

    def follow(h):
        pass_on(h)
        send(h + 1)

    def pass_on(h):
        for n in range(2):
            copies[h][n].wait_recv()
            copies[h][6 + n].start()
        for n in range(2):
            copies[h][SUB + n].start()

    def finish(h):
        for n, arrived in enumerate((2, 3, 6, 7)):
            copies[h][arrived].wait_recv()
            copies[h][10 + n].start()
        for n in (4, 5, *range(SUB, len(plan))):
            copies[h][n].wait_recv()

    def second():
        mixed(1)
        follow(0)

    for at, event in ((0, begin), (1, second), (2, lambda: mixed(2)), (6, lambda: finish(0)), (SUB, lambda: follow(1)),
                      (16, lambda: finish(1)), (18, lambda: pass_on(2)), (20, lambda: finish(2))):
        pl.when(step == at)(event)

    @pl.when((step >= 3) & (step <= last - 3))
    def _():
        channel_product(first, x_ref, w_ref, p_ref.at[0], d_ref)

    @pl.when((step == 6) | (step == 7) | (step >= 16))
    def _():
        x_inverse(m_ref, t_ref, inverse_slot(step), parts_ref)

    @pl.when(step == last)
    def _():
        for some in copies:
            for copy in some:
                copy.wait_send()


def block(shape, index, slot=None, **kwargs):
    def index_map(*at):
        return tuple(0 if k == 'o' else slot(at[0]) if k == 's' else at['ijk'.index(k)] for k in index)
    return pl.BlockSpec(shape, index_map, **kwargs)


def bf16_addends(table):
    out = []
    for _ in range(ADDENDS):
        out.append(lax.reduce_precision(table, exponent_bits=SUB, mantissa_bits=7))
        table = table - out[-1]
    return jnp.stack(out).astype(BF16)


def solution(mesh):
    row_devs, col_devs = mesh.shape['ys'], mesh.shape['xs']

    def local_layers(field, spec_real, spec_imag, mix_weight, bias):
        batch, x_loc, y_loc, grid_z, width = field.shape
        modes = spec_real.shape[3]
        grid_x, grid_y = x_loc * col_devs, y_loc * row_devs
        groups, blocks = x_loc // X_GROUP, y_loc // Y_BLOCK
        lanes = X_GROUP * batch
        kx, ky = kept(modes, grid_x), kept(modes, grid_y)
        n_kx, n_ky = len(kx), len(ky)
        x_index, y_index = lax.axis_index('xs'), lax.axis_index('ys')
        fwd_np, inv_np = all_tables(blocks, ky, grid_y, grid_z, grid_x * grid_y * grid_z)
        fwd, inv = [jnp.asarray(t) for t in fwd_np], [jnp.asarray(t) for t in inv_np]

        turn = 2.0 * math.pi * (kx[:, None] * np.arange(grid_x)[None, :] % grid_x) / grid_x
        cos, sin = np.cos(turn), np.sin(turn)
        fwd_x = np.stack([np.stack([cos, sin], -1), np.stack([-sin, cos], -1)], 1)
        inv_x = np.transpose(fwd_x, (2, 3, 0, 1))
        fwd_x = fwd_x.reshape(n_kx, 2, col_devs, x_loc, 2).transpose(2, 0, 1, 3, 4).reshape(col_devs, 2 * n_kx, 2 * x_loc)
        inv_x = inv_x.reshape(col_devs, 2 * x_loc, 2 * n_kx)
        odd = (jnp.arange(16 * x_loc) % 2 * y_index)[:, None]

        core, x_chip = x_index % 2, x_index // 2

        def x_table(tables, axis):
            wide = np.kron(tables, np.eye(SUB)).astype(np.float32)
            t = lax.dynamic_index_in_dim(jnp.asarray(wide), x_index, 0, keepdims=False)
            t = jnp.where(core == 1, jnp.roll(t, SUB * n_kx, axis), t)
            return bf16_addends(jnp.where(odd == 1, -t, t))
        fwd_x, inv_x = x_table(fwd_x, 0), x_table(inv_x, 1)
        eye = jnp.eye(Z_BLOCK, dtype=F32)
        def point_table(layer):
            w = bf16_addends((0.5 * mix_weight[layer].T[:, None, :, None] * eye[None, :, None, :]).reshape(width * SUB, width * SUB))
            b = bf16_addends(jnp.broadcast_to(0.5 * bias[layer][:, None], (width, SUB)).reshape(width * SUB))
            b = jnp.pad(jnp.stack([b.T, 0 * b.T, 0 * b.T]), ((0, 0), (0, 0), (0, 2 * SUB - 3)))
            return jnp.concatenate([w, b], -1)
        point_w = [point_table(layer) for layer in range(2)]

        real_w, imag_w = (jnp.swapaxes(w, 3, 4) for w in (spec_real, spec_imag))
        v = jnp.swapaxes(jnp.moveaxis(field, 0, -1), 2, 3)
        grid = (groups, blocks, 2)
        part_width = width // 2
        params = pltpu.CompilerParams(vmem_limit_bytes=VMEM_LIMIT)
        spec_shape = jax.ShapeDtypeStruct((groups, width, 256, lanes), F32)
        in_block = block((X_GROUP, Y_BLOCK, part_width, grid_z, batch), 'ijkoo')
        mid_block = block((1, Y_BLOCK, part_width, grid_z, lanes), 'ijkoo')
        part_block = block((1, ADDENDS, width, CLASS_ROWS[-1], lanes), 'ioooo')
        mid_shape = jax.ShapeDtypeStruct((groups, y_loc, width, grid_z, lanes), F32)
        anywhere = pl.BlockSpec(memory_space=pl.ANY)

        def stage(unit):
            return pltpu.VMEM((unit[1] // unit[0], 5, Y_BLOCK * SUB, unit[0] * lanes), F32)
        w_block = block((ADDENDS, width * SUB, width * SUB + 2 * SUB), 'ooo')

        units = y_loc // HALF_BLOCK

        def half_block(first, half, start):
            shape = (HALF_BLOCK, width, grid_z) + ((batch,) if first else (lanes,))
            return pl.BlockSpec((X_GROUP if first else 1,) + shape,
                                lambda j: (half, jnp.clip(j - start, 0, units - 1), 0, 0, 0))

        def table_specs(tables):
            return [block((1,) + t.shape[1:], 'joo') for t in tables]

        f = pl.pallas_call(
            functools.partial(forward_kernel, FORWARD_UNIT), grid=grid, out_shape=spec_shape,
            in_specs=[in_block] + table_specs(fwd),
            out_specs=block((1, width, 256, lanes), 'iooo'),
            scratch_shapes=[stage(FORWARD_UNIT)], compiler_params=params, name='forward')(v, *fwd)

        own, slots, halves = 2, SUB, n_ky // SUB
        unit = (slots, 2, n_ky, width * batch)
        own_block = block((own,) + unit, 'ooooo')
        x_block = block((ADDENDS, 16 * x_loc, 16 * x_loc), 'ooo')
        dma = pltpu.SemaphoreType.DMA
        half_rows = pltpu.VMEM((2, width * SUB, HALF_BLOCK * lanes), F32)

        def exchange(number):
            return pltpu.CompilerParams(vmem_limit_bytes=VMEM_LIMIT, collective_id=number, has_side_effects=True)

        def across(f, layer, source):
            first = layer == 0
            s, p = pl.pallas_call(
                functools.partial(reduce_kernel, first), grid=(slots + units,),
                out_shape=(jax.ShapeDtypeStruct((own,) + unit, F32), mid_shape),
                in_specs=[x_block,
                          block((groups, width, 1, 2, halves, SUB, lanes), 'oosoooo', lambda j: jnp.minimum(j, slots - 1)),
                          half_block(first, 0, slots), w_block],
                out_specs=(own_block, half_block(False, 0, slots)),
                scratch_shapes=[half_rows] + [pltpu.VMEM((n,) + unit, F32) for n in (n_kx, SUB, 4, 2)]
                + [dma((slots, SUB))] * 2 + [dma((len(CHUNKS), n)) for n in (4, 4, 2, 2)],
                compiler_params=exchange(2 * layer), name='reduce')(
                    fwd_x, f.reshape(groups, width, slots, 2, halves, SUB, lanes), source, point_w[layer])
            parts, p = pl.pallas_call(
                functools.partial(gather_kernel, first, layer), grid=(units + 6,),
                out_shape=(jax.ShapeDtypeStruct((groups, ADDENDS, width, slots, 2, halves, SUB, lanes), BF16), mid_shape),
                in_specs=[x_block, own_block, anywhere, anywhere, half_block(first, 1, 3), w_block, anywhere],
                out_specs=(block((groups, ADDENDS, width, 1, 2, halves, SUB, lanes), 'ooosoooo', inverse_slot),
                           half_block(False, 1, 3)),
                input_output_aliases={6: 1},
                scratch_shapes=[half_rows, pltpu.VMEM((n_kx,) + unit, F32)]
                + [pltpu.VMEM((own, n_ky, width, SUB, width), F32)] * 2
                + [pltpu.VMEM((own * n_ky * SUB, LANES), F32)] + [pltpu.VMEM((width, 24, LANES), F32)] * 2
                + [pltpu.VMEM((width * batch, LANES), F32)] * 4
                + [dma((2, 2))] + [dma((len(CHUNKS), 14))] * 2,
                compiler_params=exchange(2 * layer + 1), name='gather')(
                    inv_x, s, real_w, imag_w, source, point_w[layer], p)
            return parts.reshape(groups, ADDENDS, width, CLASS_ROWS[-1], lanes), p

        parts, p = across(f, 0, v)
        v1, f = pl.pallas_call(
            functools.partial(layer_kernel, FIRST_UNIT, True), grid=grid, out_shape=(mid_shape, spec_shape),
            in_specs=[mid_block, part_block] + table_specs(inv) + table_specs(fwd),
            out_specs=(mid_block, anywhere),
            scratch_shapes=[stage(FIRST_UNIT)] * 2 + [pltpu.VMEM((width, 256, lanes), F32), pltpu.SemaphoreType.DMA],
            compiler_params=params, name='layer_first')(p, parts, *inv, *fwd)
        parts, p = across(f, 1, v1)
        out = pl.pallas_call(
            functools.partial(layer_kernel, LAST_UNIT, False), grid=grid,
            out_shape=jax.ShapeDtypeStruct((x_loc, y_loc, width, grid_z, batch), F32),
            in_specs=[mid_block, part_block] + table_specs(inv), out_specs=in_block, scratch_shapes=[stage(LAST_UNIT)],
            compiler_params=params, name='layer_last')(p, parts, *inv)
        return jnp.moveaxis(jnp.swapaxes(out, 2, 3), -1, 0)

    field_spec = P('data', 'xs', 'ys', None, None)
    return jax.shard_map(local_layers, mesh=mesh, in_specs=(field_spec, P(), P(), P(), P()), out_specs=field_spec, check_vma=False)
```

```python
import functools
import math

import jax
import jax.numpy as jnp
import ml_dtypes
import numpy as np
from jax import lax
from jax.experimental import pallas as pl
from jax.experimental.pallas import tpu as pltpu
from jax.sharding import PartitionSpec as P

F32 = jnp.float32
BF16 = jnp.bfloat16
VMEM_LIMIT = 64 * 1024 * 1024 - 65536

SUB = 8
X_GROUP = 8
Y_BLOCK = 4
HALF_BLOCK = 2
Z_BLOCK = 8
KZ_CLASS = ((0, 5), (1, 6, 4), (2, 7, 3))
KZ_ORDER = tuple(kz for group in KZ_CLASS for kz in group)
CLASS_ROWS = (0, 64, 160, 256)
LANES = 128
ADDENDS = 3
REDUCE_CHUNKS = ((0, 2), (2, 6), (6, 8))
GATHER_CHUNKS = ((0, 4), (4, 6), (6, 8))
MIX_CHUNKS = ((0, 4), (4, 8))
FORWARD_UNIT = (2, 10)
FIRST_UNIT = (2, 10)
LAST_UNIT = (1, 10)
ROOT5_4 = math.sqrt(5.0) / 4.0
SIN_1 = math.sin(2.0 * math.pi / 5.0)
SIN_RATIO = math.sin(4.0 * math.pi / 5.0) / SIN_1


def kz_sign(kz):
    return 0 if kz % 5 == 0 else (1 if kz % 5 < 3 else -1)


def kept(modes, size):
    return np.concatenate([np.arange(modes), np.arange(size - modes, size)])


def pieces(table):
    rest = np.asarray(table, np.float32)
    out = []
    for _ in range(ADDENDS):
        out.append(rest.astype(ml_dtypes.bfloat16))
        rest = rest - out[-1].astype(np.float32)
    return out


def yz_angles(kz, y_pos, ky, grid_y, grid_z):
    z_pos = np.arange(Z_BLOCK)
    turn = (ky[:, None, None] * y_pos[None, :, None] % grid_y) / grid_y + kz * z_pos[None, None, :] / grid_z
    return 2.0 * math.pi * turn


def forward_table(group, y_pos, ky, grid_y, grid_z):
    rows = []
    for kz in group:
        t, s = yz_angles(kz, y_pos, ky, grid_y, grid_z), kz_sign(kz)
        real, imag = [np.cos(t)], [-np.sin(t)]
        if s:
            real.append(-s * SIN_1 * np.sin(t))
            imag.append(-s * SIN_1 * np.cos(t))
        rows += [np.stack(part, 1).reshape(len(ky), -1) for part in (real, imag)]
    return np.concatenate(rows, 0)


def inverse_table(group, y_pos, ky, grid_y, grid_z, points):
    cols = []
    for kz in group:
        t, s = yz_angles(kz, y_pos, ky, grid_y, grid_z).transpose(1, 2, 0), kz_sign(kz)
        w = (0.5 if kz == 0 else 1.0) / points
        real, imag = [w * np.cos(t)], [-w * np.sin(t)]
        if s:
            real.append(s * SIN_1 * w * np.sin(t))
            imag.append(s * SIN_1 * w * np.cos(t))
        cols += [np.stack(part, 0).reshape(-1, len(ky)) for part in (real, imag)]
    return np.concatenate(cols, 1)


def all_tables(blocks, ky, grid_y, grid_z, points):
    fwd, inv = [[], [], []], [[], [], [], [], []]
    for block in range(blocks):
        y_pos = np.arange(Y_BLOCK) + block * Y_BLOCK
        for k, group in enumerate(KZ_CLASS):
            a, b, c = pieces(forward_table(group, y_pos, ky, grid_y, grid_z))
            n = np.zeros_like(a)
            if k == 0:
                fwd[k].append(np.concatenate([a, a, a, b, b, c], 1))
            else:
                fwd[k].append(np.block([[a, a, a, b], [c, b, n, n]]))
            a, b, c = pieces(inverse_table(group, y_pos, ky, grid_y, grid_z, points))
            n = np.zeros_like(a)
            if k == 0:
                inv[0].append(np.block([[a, a, a], [b, b, n], [c, n, n]]))
            else:
                inv[2 * k - 1].append(np.block([[a, a], [b, b]]))
                inv[2 * k].append(np.concatenate([c, a], 1))
    return [np.stack(t) for t in fwd], [np.stack(t) for t in inv]


def split3(v):
    d1 = v.astype(BF16)
    rest = v - d1.astype(F32)
    d2 = rest.astype(BF16)
    return d1, d2, (rest - d2.astype(F32)).astype(BF16)


def dot(a, b):
    return jnp.dot(a, b, preferred_element_type=F32)


def z_forward(v):
    v0, v1, v2, v3, v4 = v
    t1, t2, e1, e2 = v1 + v4, v2 + v3, v1 - v4, v2 - v3
    total = t1 + t2
    mid, dif = v0 - 0.25 * total, ROOT5_4 * (t1 - t2)
    return v0 + total, mid + dif, e1 + SIN_RATIO * e2, mid - dif, SIN_RATIO * e1 - e2


def z_inverse(a0, a1, b1, a2, b2):
    total = a1 + a2
    mid, dif = a0 - 0.25 * total, ROOT5_4 * (a1 - a2)
    p, q = mid + dif, mid - dif
    r, s = b1 + SIN_RATIO * b2, SIN_RATIO * b1 - b2
    return a0 + total, p - r, q - s, q + s, p + r


def split_tiles(u_ref, channels):
    rows, lanes = u_ref.shape[1:]
    out = [[], [], []]
    for k in channels:
        for r in range(0, rows, 2 * SUB):
            cells = [split3(u_ref[k, r:r + 2 * SUB, lane:lane + LANES]) for lane in range(0, lanes, LANES)]
            for i in range(ADDENDS):
                out[i].append(jnp.concatenate([cell[i] for cell in cells], -1))
    return [jnp.concatenate(rows, 0) for rows in out]


def add_tiles(o, n, lanes, first=0):
    for r in range(0, n, SUB):
        for lane in range(0, lanes, LANES):
            cells = [o[b + r:b + r + SUB, lane:lane + LANES] for b in range(0, o.shape[0], n)]
            yield r, lane, functools.reduce(jnp.add, cells)


def forward_stage(u_ref, tables, f_ref, c, pair):
    lanes = f_ref.shape[-1]
    for k, channels in enumerate(((0,), (1, 2), (3, 4))):
        d = split_tiles(u_ref, channels)
        o = dot(tables[k], jnp.concatenate([d[i] for i in ((0, 1, 2, 0) if k else (0, 1, 2, 0, 1, 0))], 0))
        n = CLASS_ROWS[k + 1] - CLASS_ROWS[k]
        for r, lane, v in add_tiles(o, n, pair * lanes):
            at = (c + lane // lanes, slice(CLASS_ROWS[k] + r, CLASS_ROWS[k] + r + SUB), slice(lane % lanes, lane % lanes + LANES))
            f_ref[at] += v


def inverse_stage(s_ref, c, pair, tables, u_ref):
    n, lanes = u_ref.shape[1:]

    def part(i, k):
        return jnp.concatenate([s_ref[0, i, c + u, CLASS_ROWS[k]:CLASS_ROWS[k + 1]] for u in range(pair)], -1)
    o = dot(tables[0], jnp.concatenate([part(i, 0) for i in range(ADDENDS)], 0))
    for r, lane, v in add_tiles(o, n, lanes):
        u_ref[0, r:r + SUB, lane:lane + LANES] = v
    for k in (1, 2):
        d1, d2, d3 = (part(i, k) for i in range(ADDENDS))
        o = jnp.concatenate([dot(tables[2 * k - 1], jnp.concatenate([d1, d2], 0)),
                             dot(tables[2 * k], jnp.concatenate([d1, d3], 0))], 0)
        for r, lane, v in add_tiles(o, 2 * n, lanes):
            u_ref[2 * k - 1 + r // n, r % n:r % n + SUB, lane:lane + LANES] = v


def registers(pair, lanes):
    for u in range(pair):
        for y in range(Y_BLOCK):
            for lane in range(0, lanes, LANES):
                yield u, y, lane, (slice(y * SUB, (y + 1) * SUB), slice(u * lanes + lane, u * lanes + lane + LANES))


def gelu(h):
    k = 2.0 * math.sqrt(2.0 / math.pi)
    return h + h * jnp.tanh(h * (k + (4.0 * 0.044715 * k) * (h * h)))


def field_lanes(x_ref, y, c):
    return jnp.concatenate([x_ref[x, y, c] for x in range(X_GROUP)], -1)


def zero_spectrum(f_ref):
    def clear(c, _):
        f_ref[c] = jnp.zeros(f_ref.shape[1:], F32)
        return 0
    lax.fori_loop(0, f_ref.shape[0], clear, 0)


def forward_kernel(unit, x_ref, t0, t1, t2, f_ref, u_ref):
    f_ref = f_ref.at[0]
    width, lanes = x_ref.shape[2], f_ref.shape[-1]
    pair, per_step = unit
    tables = (t0[0], t1[0], t2[0])

    @pl.when(pl.program_id(1) == 0)
    def _():
        zero_spectrum(f_ref)

    def load(c, slot):
        for u in range(pair):
            for y in range(Y_BLOCK):
                row = field_lanes(x_ref, y, c + u)
                for k, v in enumerate(z_forward([row[SUB * j:SUB * j + SUB] for j in range(5)])):
                    u_ref[slot, k, y * SUB:(y + 1) * SUB, u * lanes:(u + 1) * lanes] = v

    def body(i, _):
        c = i * per_step
        count = per_step // pair
        for n in range(count + 1):
            if n < count:
                load(c + n * pair, n)
            if n:
                forward_stage(u_ref.at[n - 1], tables, f_ref, c + (n - 1) * pair, pair)
        return 0
    lax.fori_loop(0, width // per_step, body, 0)


def channel_product(first, x_ref, w_ref, p_ref, d_ref):
    blocks, width, depth, lanes = p_ref.shape
    rows = width * SUB
    ones = jnp.ones((w_ref.shape[-1] - rows, blocks * lanes), BF16)
    full, (a, b, c) = w_ref[0, 0], (w_ref[0, i, :, :rows] for i in range(ADDENDS))

    def load(j):
        z = slice(j * SUB, (j + 1) * SUB)
        if first:
            v = [x_ref[x, y, :, z, :] for y in range(blocks) for x in range(X_GROUP)]
        else:
            v = [x_ref[0, y, :, z, :] for y in range(blocks)]
        d_ref[j % 2] = jnp.concatenate(v, -1).reshape(rows, blocks * lanes)

    def product(j):
        d1, d2, d3 = split3(d_ref[j % 2])
        p = dot(full, jnp.concatenate([d1, ones], 0)) + dot(a, d2) + dot(a, d3) + dot(b, d1) + dot(b, d2) + dot(c, d1)
        for y in range(blocks):
            p_ref[y, :, j * SUB:(j + 1) * SUB, :] = p[:, y * lanes:(y + 1) * lanes].reshape(width, SUB, lanes)
    count = depth // SUB
    for j in range(count + 1):
        if j < count:
            load(j)
        if j:
            product(j - 1)


def layer_kernel(unit, first, *refs):
    p_ref, s_ref, *tabs = refs
    p_ref = p_ref.at[0]
    width, lanes = p_ref.shape[1], p_ref.shape[-1]
    batch = lanes // X_GROUP
    start = pl.program_id(2) * width
    if first:
        *tabs, v_ref, f_hbm, a_ref, u_ref, f_ref, sem = tabs
        v_ref = v_ref.at[0]

        @pl.when((pl.program_id(1) == 0) & (start == 0))
        def _():
            zero_spectrum(f_ref)
    else:
        *tabs, o_ref, a_ref = tabs
    inv, fwd = [t[0] for t in tabs[:5]], [t[0] for t in tabs[5:]]
    pair, per_step = unit

    def activate(c, slot):
        kept_rows = {}
        for u, y, lane, at in registers(pair, lanes):
            new = []
            for j, s in enumerate(z_inverse(*(a_ref[(slot, k) + at] for k in range(5)))):
                g = gelu(s + p_ref[y, c + u, SUB * j:SUB * j + SUB, lane:lane + LANES])
                new.append(g)
                if first:
                    v_ref[y, c + u, SUB * j:SUB * j + SUB, lane:lane + LANES] = g
                else:
                    kept_rows[j] = kept_rows.get(j, ()) + (g,)
            if first:
                for k, v in enumerate(z_forward(new)):
                    u_ref[(slot, k) + at] = v
            elif lane + LANES == lanes:
                for j, row in kept_rows.items():
                    store_field(o_ref, y, c + u, SUB * j, row, batch)
                kept_rows = {}

    def body(i, _):
        c = i * per_step
        count = per_step // pair
        for n in range(count + 2):
            if n < count:
                inverse_stage(s_ref, start + c + n * pair, pair, inv, a_ref.at[n])
            if 0 < n <= count:
                activate(c + (n - 1) * pair, n - 1)
            if first and n > 1:
                forward_stage(u_ref.at[n - 2], fwd, f_ref, start + c + (n - 2) * pair, pair)
        return 0
    lax.fori_loop(0, width // per_step, body, 0)

    if first:
        @pl.when((pl.program_id(1) == pl.num_programs(1) - 1) & (start > 0))
        def _():
            copy = pltpu.make_async_copy(f_ref, f_hbm.at[pl.program_id(0)], sem)
            copy.start()
            copy.wait()


def store_field(o_ref, y, c, z, row, batch):
    lane = lax.broadcasted_iota(jnp.int32, row[0].shape, 1)
    for x in range(X_GROUP):
        at, off = divmod(x * batch, LANES)
        piece = row[at]
        if off + batch > LANES:
            piece = jnp.where(lane < off, row[at + 1], piece)
        if off:
            piece = pltpu.roll(piece, LANES - off, 1)
        o_ref[x, y, c, z:z + SUB, :] = piece[:, :batch]


def split_dot(left, right):
    a, b, c = left
    d1, d2, d3 = split3(right)
    return dot(a, d1) + dot(a, d2) + dot(a, d3) + dot(b, d1) + dot(b, d2) + dot(c, d1)


def x_forward(m_ref, f_ref, s_ref, slot):
    groups, width, lanes = f_ref.shape[0], f_ref.shape[1], f_ref.shape[-1]
    batch = lanes // X_GROUP
    halves = range(f_ref.shape[4])
    rights = []
    for h in halves:
        rows = []
        for g in range(groups):
            for x in range(X_GROUP):
                for p in range(2):
                    rows.append(jnp.concatenate([f_ref[g, c, 0, p, h, :, x * batch:(x + 1) * batch] for c in range(width)], -1))
        rights.append(jnp.concatenate(rows, 0))
    for h in halves:
        out = split_dot((m_ref[0], m_ref[1], m_ref[2]), rights[h])
        s_ref[:, slot, :, h * SUB:(h + 1) * SUB, :] = out.reshape(s_ref.shape[0], 2, SUB, width * batch)


def x_inverse(m_ref, t_ref, slot, s_ref):
    groups, width, lanes = s_ref.shape[0], s_ref.shape[2], s_ref.shape[-1]
    batch = lanes // X_GROUP
    halves = range(s_ref.shape[5])
    outs = []
    for h in halves:
        right = t_ref[:, slot, :, h * SUB:(h + 1) * SUB, :].reshape(t_ref.shape[0] * 2 * SUB, width * batch)
        outs.append(split_dot((m_ref[0], m_ref[1], m_ref[2]), right).reshape(groups, X_GROUP, 2, SUB, width * batch))
    for h in halves:
        for g in range(groups):
            for p in range(2):
                for c in range(width):
                    row = jnp.concatenate([outs[h][g, x, p, :, c * batch:(c + 1) * batch] for x in range(X_GROUP)], -1)
                    for i, d in enumerate(split3(row)):
                        s_ref[g, i, c, 0, p, h] = d


def mix(s_ref, re_w, im_w, t_ref, to, chunk, rows, re_rows, im_rows, re_s, im_s, re_t, im_t):
    own, _, _, n_ky, lanes = s_ref.shape
    width = re_w.shape[2]
    batch = lanes // width
    some = chunk[1] - chunk[0]
    part_modes = some * n_ky
    pick, modes = slice(*chunk), slice(0, own * part_modes)

    for w_ref, out in ((re_w, re_rows), (im_w, im_rows)):
        def lay(c, _):
            for k in range(own):
                for ky in range(n_ky):
                    at = (k * n_ky + ky) * SUB
                    rows[at:at + SUB, 0:width] = w_ref[k, ky, c]
            mat = jnp.concatenate([rows[pl.ds((k * n_ky + h * SUB) * SUB + kz, SUB, stride=SUB), :]
                                   for k in range(own) for kz in KZ_ORDER[pick] for h in range(n_ky // SUB)], 0)
            out[c, :, modes] = mat.T[0:out.shape[1]]
            return 0
        lax.fori_loop(0, width, lay, 0)
    for p, out in enumerate((re_s, im_s)):
        out[:, modes] = jnp.concatenate([s_ref[k, pick, p].reshape(part_modes, lanes) for k in range(own)], 0).T
    pair = 1

    def outputs(i, _):
        d = i * pair

        def inner(c, acc):
            at = pl.ds(pl.multiple_of(c * batch, SUB), batch)
            a, b = re_s[at, modes], im_s[at, modes]
            new = []
            for u in range(pair):
                p = jnp.broadcast_to(re_rows[c, pl.ds(d + u, 1), modes], a.shape)
                q = jnp.broadcast_to(im_rows[c, pl.ds(d + u, 1), modes], a.shape)
                new += [acc[2 * u] + (a * p - b * q), acc[2 * u + 1] + (a * q + b * p)]
            return tuple(new)
        zero = jnp.zeros((batch, own * part_modes), F32)
        acc = lax.fori_loop(0, width, inner, (zero,) * (2 * pair), unroll=True)
        for u in range(pair):
            at = pl.ds(pl.multiple_of((d + u) * batch, SUB), batch)
            re_t[at, modes] = acc[2 * u]
            im_t[at, modes] = acc[2 * u + 1]
        return 0
    lax.fori_loop(0, width // pair, outputs, 0)
    for p, got in enumerate((re_t, im_t)):
        back = got[:, modes].T
        for k in range(own):
            t_ref[to[k], pick, p] = back[k * part_modes:(k + 1) * part_modes].reshape(some, n_ky, lanes)


class Place:
    def __init__(self):
        xs, ys = lax.axis_index('xs'), lax.axis_index('ys')
        data = lax.axis_index('data')
        c, x, y = xs % 2, xs // 2, ys
        self.core = (data, ys, 2 * x + 1 - c)
        self.x_chip = (data, ys, 2 * (1 - x) + c)
        self.y_chip = (data, 1 - ys, xs)
        p, q = lambda a, b: 2 * a + b, lambda a, b: 4 + 2 * a + b
        self.mine = SUB * c
        self.table = 2 * xs + ys
        self.order = (p(1 - x, 1 - y), q(1 - y, 1 - x), p(1 - x, y), q(1 - y, x),
                      p(x, 1 - y), q(y, 1 - x), p(x, y), q(y, x))

    def enter(self):
        barrier = pltpu.get_barrier_semaphore()
        for device in (self.core, self.x_chip, self.y_chip):
            pl.semaphore_signal(barrier, inc=1, device_id=device, device_id_type=pl.DeviceIdType.MESH)
        pl.semaphore_wait(barrier, 3)


def remote(src, dst, send, recv, device):
    return pltpu.make_async_remote_copy(src_ref=src, dst_ref=dst, send_sem=send, recv_sem=recv, device_id=device,
                                        device_id_type=pl.DeviceIdType.MESH)


def step_and_last():
    return pl.program_id(0), pl.num_programs(0) - 1


def chunk_of(ref, k, chunk):
    low, high = chunk
    return ref.at[k, pl.ds(low, high - low)]


def reduce_kernel(first, m_hbm, f_ref, x_ref, w_ref, out_ref, p_ref, m_ref, m_sem, d_ref, s_ref, r1, r2, r3,
                  send1, recv1, send2, recv2, send3, recv3):
    me = Place()
    step, last = step_and_last()
    slots = s_ref.shape[1]
    two, three = [], []

    def to_core(slot):
        return [remote(s_ref.at[SUB + me.order[t], slot], r1.at[t, slot], send1.at[slot, t], recv1.at[slot, t], me.core)
                for t in range(SUB)]
    for h, chunk in enumerate(REDUCE_CHUNKS):
        mine = [chunk_of(s_ref, k, chunk) for k in me.order]
        two.append([remote(mine[t], chunk_of(r2, t, chunk), send2.at[h, t], recv2.at[h, t], (me.x_chip, me.y_chip)[t % 2])
                    for t in range(4)])
        three.append([remote(mine[4 + t], chunk_of(r3, t, chunk), send3.at[h, t], recv3.at[h, t], (me.y_chip, me.x_chip)[t])
                      for t in range(2)])

    def add(dst, a, b):
        def row(i, _):
            dst[i] = a[i] + b[i]
            return 0
        lax.fori_loop(0, dst.shape[0], row, 0)

    def from_core(h):
        arriving = [to_core(slot) for slot in range(*REDUCE_CHUNKS[h])]
        for t in range(SUB):
            for copies in arriving:
                copies[t].wait_recv()
            to = chunk_of(s_ref, me.order[t], REDUCE_CHUNKS[h])
            add(to, to, chunk_of(r1, t, REDUCE_CHUNKS[h]))
            if t < 4:
                two[h][t].start()

    def from_chip(h, these=(0, 1)):
        for t in these:
            two[h][t].wait_recv()
            to = chunk_of(s_ref, me.order[4 + t], REDUCE_CHUNKS[h])
            add(to, to, chunk_of(r2, t, REDUCE_CHUNKS[h]))
            if t < 2:
                three[h][t].start()

    def finish(h):
        from_chip(h, (2, 3))
        for t in range(2):
            three[h][t].wait_recv()
            add(*(chunk_of(ref, k, REDUCE_CHUNKS[h]) for ref, k in ((out_ref, t), (s_ref, me.order[6 + t]), (r3, t))))

    def begin():
        table = pltpu.make_async_copy(m_hbm.at[me.table], m_ref, m_sem)
        table.start()
        me.enter()
        table.wait()

    events = ((0, begin), (2, lambda: from_core(0)), (slots - 3, lambda: from_chip(0)), (slots - 2, lambda: from_core(1)),
              (slots, lambda: from_core(2)), (slots + 3, lambda: finish(0)), (slots + 5, lambda: from_chip(1)),
              (slots + 12, lambda: from_chip(2)))
    for at, event in events:
        pl.when(step == at)(event)

    @pl.when(step < slots)
    def _():
        x_forward(m_ref, f_ref, s_ref, step)
        for copy in to_core(step):
            copy.start()

    @pl.when(step >= slots)
    def _():
        channel_product(first, x_ref, w_ref, p_ref.at[0], d_ref)

    @pl.when(step == last)
    def _():
        finish(1)
        finish(2)
        for copies in [to_core(slot) for slot in range(slots)] + two + three:
            for copy in copies:
                copy.wait_send()


def gather_kernel(first, layer, m_hbm, s_ref, re_hbm, im_hbm, x_ref, w_ref, p_in, parts_ref, p_ref, m_ref, m_sem, d_ref, t_ref,
                  re_w, im_w, rows, re_rows, im_rows, re_s, im_s, re_t, im_t, w_sem, send_sem, recv_sem):
    me = Place()
    step, last = step_and_last()
    p3, q3, p2, q2, p1, q1, p0, q0 = me.order
    plan = [(p0, me.y_chip, 0), (q0, me.x_chip, 0), (p0, me.x_chip, 0), (q0, me.y_chip, 0), (p0, me.core, SUB), (q0, me.core, SUB),
            (p1, me.x_chip, 0), (q1, me.y_chip, 0)] + [(k, me.core, SUB) for k in (p1, q1, p2, q2, p3, q3)]
    copies = [[remote(chunk_of(t_ref, k, chunk), chunk_of(t_ref, k + up, chunk), send_sem.at[h, n], recv_sem.at[h, n], device)
               for n, (k, device, up) in enumerate(plan)] for h, chunk in enumerate(GATHER_CHUNKS)]
    weights = [pltpu.make_async_copy(hbm.at[layer, me.mine + k], to.at[i], w_sem.at[n, i])
               for n, (hbm, to) in enumerate(((re_hbm, re_w), (im_hbm, im_w))) for i, k in enumerate((p0, q0))]
    weights.append(pltpu.make_async_copy(m_hbm.at[me.table], m_ref, m_sem))

    def mixed(h):
        mix(s_ref, re_w, im_w, t_ref, (p0, q0), MIX_CHUNKS[h], rows, re_rows, im_rows, re_s, im_s, re_t, im_t)

    def send(h):
        for copy in copies[h][:6]:
            copy.start()

    def begin():
        for copy in weights:
            copy.start()
        me.enter()
        for copy in weights:
            copy.wait()
        mixed(0)
        send(0)

    def follow(h):
        pass_on(h)
        send(h + 1)

    def pass_on(h):
        for n in range(2):
            copies[h][n].wait_recv()
            copies[h][6 + n].start()
            copies[h][SUB + n].start()

    def finish(h):
        for n, arrived in enumerate((2, 3, 6, 7)):
            copies[h][arrived].wait_recv()
            copies[h][10 + n].start()
        for n in (4, 5, *range(SUB, len(plan))):
            copies[h][n].wait_recv()

    x_from = last + 1 - t_ref.shape[1]
    for at, event in ((0, begin), (1, lambda: mixed(1)), (5, lambda: follow(0)), (x_from, lambda: finish(0)),
                      (x_from + 1, lambda: follow(1)), (x_from + 4, lambda: finish(1)), (x_from + 5, lambda: pass_on(2)),
                      (x_from + 6, lambda: finish(2))):
        pl.when(step == at)(event)

    @pl.when((step >= 2) & (step < x_from + 4))
    def _():
        channel_product(first, x_ref, w_ref, p_ref.at[0], d_ref)

    @pl.when(step >= x_from)
    def _():
        x_inverse(m_ref, t_ref, step - x_from, parts_ref)

    @pl.when(step == last)
    def _():
        for some in copies:
            for copy in some:
                copy.wait_send()


def block(shape, index, slot=None, **kwargs):
    def index_map(*at):
        return tuple(0 if k == 'o' else slot(at[0]) if k == 's' else at['ijk'.index(k)] for k in index)
    return pl.BlockSpec(shape, index_map, **kwargs)


def point_table_kernel(w_ref, b_ref, out_ref):
    layers, width = b_ref.shape
    rows = width * SUB

    def spread(shape, axis):
        at = [lax.broadcasted_iota(jnp.int32, shape, k) for k in range(2)]
        return jnp.where(at[axis] // SUB == at[1 - axis], 1.0, 0.0).astype(BF16)
    down, across = spread((rows, width), 0), spread((width, rows), 1)
    at = [lax.broadcasted_iota(jnp.int32, (rows, rows), k) % SUB for k in range(2)]
    column = lax.broadcasted_iota(jnp.int32, (rows, 2 * SUB), 1)
    for layer in range(layers):
        weights, biases = split3(0.5 * w_ref[layer].T), split3(0.5 * b_ref[layer:layer + 1])
        shift = sum(jnp.where(column == i, jnp.sum(down.astype(F32) * b.astype(F32), 1, keepdims=True), 0.0)
                    for i, b in enumerate(biases))
        for i, w in enumerate(weights):
            wide = dot(dot(down, w).astype(BF16), across)
            wide = jnp.where(at[0] == at[1], wide, 0.0)
            out_ref[layer, i] = jnp.concatenate([wide, shift if i == 0 else jnp.zeros_like(shift)], 1).astype(BF16)


def solution(mesh):
    row_devs, col_devs = mesh.shape['ys'], mesh.shape['xs']

    def local_layers(field, spec_real, spec_imag, mix_weight, bias):
        batch, x_loc, y_loc, grid_z, width = field.shape
        modes = spec_real.shape[3]
        grid_x, grid_y = x_loc * col_devs, y_loc * row_devs
        groups, blocks = x_loc // X_GROUP, y_loc // Y_BLOCK
        lanes = X_GROUP * batch
        kx, ky = kept(modes, grid_x), kept(modes, grid_y)
        n_kx, n_ky = len(kx), len(ky)
        fwd_np, inv_np = all_tables(blocks, ky, grid_y, grid_z, grid_x * grid_y * grid_z)
        fwd, inv = [jnp.asarray(t) for t in fwd_np], [jnp.asarray(t) for t in inv_np]

        turn = 2.0 * math.pi * (kx[:, None] * np.arange(grid_x)[None, :] % grid_x) / grid_x
        cos, sin = np.cos(turn), np.sin(turn)
        fwd_x = np.stack([np.stack([cos, sin], -1), np.stack([-sin, cos], -1)], 1)
        inv_x = np.transpose(fwd_x, (2, 3, 0, 1))
        fwd_x = fwd_x.reshape(n_kx, 2, col_devs, x_loc, 2).transpose(2, 0, 1, 3, 4).reshape(col_devs, 2 * n_kx, 2 * x_loc)
        inv_x = inv_x.reshape(col_devs, 2 * x_loc, 2 * n_kx)
        odd_rows = np.where(np.arange(2 * SUB * x_loc) % 2, -1.0, 1.0)[:, None]

        def x_tables(tables, axis):
            out = []
            for xs in range(col_devs):
                t = np.roll(np.kron(tables[xs], np.eye(SUB)), SUB * n_kx * (xs % 2), axis)
                out += [np.stack(pieces(t * sign)) for sign in (1.0, odd_rows)]
            return jnp.asarray(np.stack(out))
        fwd_x, inv_x = x_tables(fwd_x, 0), x_tables(inv_x, 1)
        params = pltpu.CompilerParams(vmem_limit_bytes=VMEM_LIMIT)
        point_w = pl.pallas_call(
            point_table_kernel, out_shape=jax.ShapeDtypeStruct((2, ADDENDS, width * SUB, width * SUB + 2 * SUB), BF16),
            compiler_params=params, name='point_table')(mix_weight, bias)

        real_w, imag_w = (jnp.swapaxes(w, 3, 4) for w in (spec_real, spec_imag))
        v = jnp.swapaxes(jnp.moveaxis(field, 0, -1), 2, 3)
        grid = (groups, blocks, 2)
        part_width = width // 2
        spec_shape = jax.ShapeDtypeStruct((groups, width, 256, lanes), F32)
        in_block = block((X_GROUP, Y_BLOCK, part_width, grid_z, batch), 'ijkoo')
        mid_block = block((1, Y_BLOCK, part_width, grid_z, lanes), 'ijkoo')
        part_block = block((1, ADDENDS, width, CLASS_ROWS[-1], lanes), 'ioooo')
        mid_shape = jax.ShapeDtypeStruct((groups, y_loc, width, grid_z, lanes), F32)
        anywhere = pl.BlockSpec(memory_space=pl.ANY)

        def stage(unit):
            return pltpu.VMEM((unit[1] // unit[0], 5, Y_BLOCK * SUB, unit[0] * lanes), F32)

        units = y_loc // HALF_BLOCK

        def half_block(first, half, start):
            shape = (HALF_BLOCK, width, grid_z) + ((batch,) if first else (lanes,))
            return pl.BlockSpec((X_GROUP if first else 1,) + shape,
                                lambda j: (half, jnp.clip(j - start, 0, units - 1), 0, 0, 0))

        def table_specs(tables):
            return [block((1,) + t.shape[1:], 'joo') for t in tables]

        f = pl.pallas_call(
            functools.partial(forward_kernel, FORWARD_UNIT), grid=grid[:2], out_shape=spec_shape,
            in_specs=[block((X_GROUP, Y_BLOCK, width, grid_z, batch), 'ijooo')] + table_specs(fwd),
            out_specs=block((1, width, 256, lanes), 'iooo'),
            scratch_shapes=[stage(FORWARD_UNIT)], compiler_params=params, name='forward')(v, *fwd)

        own, slots, halves = 2, SUB, n_ky // SUB
        unit = (slots, 2, n_ky, width * batch)
        own_block = block((own,) + unit, 'ooooo')

        def w_block(layer):
            return block((1,) + point_w.shape[1:], 'sooo', lambda j: layer)
        dma = pltpu.SemaphoreType.DMA
        x_scratch = [pltpu.VMEM(fwd_x.shape[1:], BF16), dma]
        half_rows = pltpu.VMEM((2, width * SUB, HALF_BLOCK * lanes), F32)

        def exchange(number):
            return pltpu.CompilerParams(vmem_limit_bytes=VMEM_LIMIT, collective_id=number, has_side_effects=True)

        def across(f, layer, source):
            first = layer == 0
            s, p = pl.pallas_call(
                functools.partial(reduce_kernel, first), grid=(slots + units,),
                out_shape=(jax.ShapeDtypeStruct((own,) + unit, F32), mid_shape),
                in_specs=[anywhere,
                          block((groups, width, 1, 2, halves, SUB, lanes), 'oosoooo', lambda j: jnp.minimum(j, slots - 1)),
                          half_block(first, 0, slots), w_block(layer)],
                out_specs=(own_block, half_block(False, 0, slots)),
                scratch_shapes=x_scratch + [half_rows] + [pltpu.VMEM((n,) + unit, F32) for n in (n_kx, SUB, 4, 2)]
                + [dma((slots, SUB))] * 2 + [dma((len(REDUCE_CHUNKS), n)) for n in (4, 4, 2, 2)],
                compiler_params=exchange(2 * layer), name='reduce')(
                    fwd_x, f.reshape(groups, width, slots, 2, halves, SUB, lanes), source, point_w)
            parts, p = pl.pallas_call(
                functools.partial(gather_kernel, first, layer), grid=(units + 6,),
                out_shape=(jax.ShapeDtypeStruct((groups, ADDENDS, width, slots, 2, halves, SUB, lanes), BF16), mid_shape),
                in_specs=[anywhere, own_block, anywhere, anywhere, half_block(first, 1, 2), w_block(layer), anywhere],
                out_specs=(block((groups, ADDENDS, width, 1, 2, halves, SUB, lanes), 'ooosoooo', lambda j: jnp.maximum(j - units + 2, 0)),
                           half_block(False, 1, 2)),
                input_output_aliases={6: 1},
                scratch_shapes=x_scratch + [half_rows, pltpu.VMEM((n_kx,) + unit, F32)]
                + [pltpu.VMEM((own, n_ky, width, SUB, width), F32)] * 2
                + [pltpu.VMEM((own * n_ky * SUB, LANES), F32)] + [pltpu.VMEM((width, 24, LANES), F32)] * 2
                + [pltpu.VMEM((width * batch, LANES), F32)] * 4
                + [dma((2, 2))] + [dma((len(GATHER_CHUNKS), 14))] * 2,
                compiler_params=exchange(2 * layer + 1), name='gather')(
                    inv_x, s, real_w, imag_w, source, point_w, p)
            return parts.reshape(groups, ADDENDS, width, CLASS_ROWS[-1], lanes), p

        parts, p = across(f, 0, v)
        v1, f = pl.pallas_call(
            functools.partial(layer_kernel, FIRST_UNIT, True), grid=grid, out_shape=(mid_shape, spec_shape),
            in_specs=[mid_block, part_block] + table_specs(inv) + table_specs(fwd),
            out_specs=(mid_block, anywhere),
            scratch_shapes=[stage(FIRST_UNIT)] * 2 + [pltpu.VMEM((width, 256, lanes), F32), pltpu.SemaphoreType.DMA],
            compiler_params=params, name='layer_first')(p, parts, *inv, *fwd)
        parts, p = across(f, 1, v1)
        out = pl.pallas_call(
            functools.partial(layer_kernel, LAST_UNIT, False), grid=grid,
            out_shape=jax.ShapeDtypeStruct((x_loc, y_loc, width, grid_z, batch), F32),
            in_specs=[mid_block, part_block] + table_specs(inv), out_specs=in_block, scratch_shapes=[stage(LAST_UNIT)],
            compiler_params=params, name='layer_last')(p, parts, *inv)
        return jnp.moveaxis(jnp.swapaxes(out, 2, 3), -1, 0)

    field_spec = P('data', 'xs', 'ys', None, None)
    return jax.shard_map(local_layers, mesh=mesh, in_specs=(field_spec, P(), P(), P(), P()), out_specs=field_spec, check_vma=False)
```

```python
import functools
import math

import jax
import jax.numpy as jnp
import ml_dtypes
import numpy as np
from jax import lax
from jax.experimental import pallas as pl
from jax.experimental.pallas import tpu as pltpu
from jax.sharding import PartitionSpec as P

F32 = jnp.float32
BF16 = jnp.bfloat16
VMEM_LIMIT = 64 * 1024 * 1024 - 65536

SUB = 8
X_GROUP = 8
Y_BLOCK = 4
HALF_BLOCK = 2
Z_BLOCK = 8
KZ_CLASS = ((0, 5), (1, 6, 4), (2, 7, 3))
KZ_ORDER = tuple(kz for group in KZ_CLASS for kz in group)
CLASS_ROWS = (0, 64, 160, 256)
LANES = 128
ADDENDS = 3
CUT = 96
HALF = 0.5
REDUCE_UNITS = (20, 22)
REDUCE_CHUNKS = ((0, 2), (2, 6), (6, 8))
GATHER_CHUNKS = ((0, 4), (4, 6), (6, 8))
MIX_CHUNKS = ((0, 4), (4, 8))
FORWARD_UNIT = (2, 10)
FIRST_UNIT = (2, 10)
LAST_UNIT = (1, 10)
ROOT5_4 = math.sqrt(5.0) / 4.0
SIN_1 = math.sin(2.0 * math.pi / 5.0)
SIN_RATIO = math.sin(4.0 * math.pi / 5.0) / SIN_1


def kz_sign(kz):
    return 0 if kz % 5 == 0 else (1 if kz % 5 < 3 else -1)


def kept(modes, size):
    return np.concatenate([np.arange(modes), np.arange(size - modes, size)])


def pieces(table):
    rest = np.asarray(table, np.float32)
    out = []
    for _ in range(ADDENDS):
        out.append(rest.astype(ml_dtypes.bfloat16))
        rest = rest - out[-1].astype(np.float32)
    return out


def yz_angles(kz, y_pos, ky, grid_y, grid_z):
    z_pos = np.arange(Z_BLOCK)
    turn = (ky[:, None, None] * y_pos[None, :, None] % grid_y) / grid_y + kz * z_pos[None, None, :] / grid_z
    return 2.0 * math.pi * turn


def forward_table(group, y_pos, ky, grid_y, grid_z):
    rows = []
    for kz in group:
        t, s = yz_angles(kz, y_pos, ky, grid_y, grid_z), kz_sign(kz)
        real, imag = [np.cos(t)], [-np.sin(t)]
        if s:
            real.append(-s * SIN_1 * np.sin(t))
            imag.append(-s * SIN_1 * np.cos(t))
        rows += [np.stack(part, 1).reshape(len(ky), -1) for part in (real, imag)]
    return np.concatenate(rows, 0)


def inverse_table(group, y_pos, ky, grid_y, grid_z, points):
    cols = []
    for kz in group:
        t, s = yz_angles(kz, y_pos, ky, grid_y, grid_z).transpose(1, 2, 0), kz_sign(kz)
        w = (HALF if kz == 0 else 1.0) / points
        real, imag = [w * np.cos(t)], [-w * np.sin(t)]
        if s:
            real.append(s * SIN_1 * w * np.sin(t))
            imag.append(s * SIN_1 * w * np.cos(t))
        cols += [np.stack(part, 0).reshape(-1, len(ky)) for part in (real, imag)]
    return np.concatenate(cols, 1)


def all_tables(blocks, ky, grid_y, grid_z, points):
    fwd, inv = [[], [], []], [[], [], [], [], []]
    for block in range(blocks):
        y_pos = np.arange(Y_BLOCK) + block * Y_BLOCK
        for k, group in enumerate(KZ_CLASS):
            a, b, c = pieces(forward_table(group, y_pos, ky, grid_y, grid_z))
            n = np.zeros_like(a)
            if k == 0:
                fwd[k].append(np.concatenate([a, a, a, b, b, c], 1))
            else:
                fwd[k].append(np.block([[a, a, a, b], [c, b, n, n]]))
            a, b, c = pieces(inverse_table(group, y_pos, ky, grid_y, grid_z, points))
            n = np.zeros_like(a)
            if k == 0:
                inv[0].append(np.block([[a, a, a], [b, b, n], [c, n, n]]))
            else:
                inv[2 * k - 1].append(np.block([[a, a], [b, b]]))
                inv[2 * k].append(np.concatenate([c, a], 1))
    return [np.stack(t) for t in fwd], [np.stack(t) for t in inv]


def split3(v):
    d1 = v.astype(BF16)
    rest = v - d1.astype(F32)
    d2 = rest.astype(BF16)
    return d1, d2, (rest - d2.astype(F32)).astype(BF16)


def dot(a, b):
    return jnp.dot(a, b, preferred_element_type=F32)


def z_forward(v):
    v0, v1, v2, v3, v4 = v
    t1, t2, e1, e2 = v1 + v4, v2 + v3, v1 - v4, v2 - v3
    total = t1 + t2
    mid, dif = v0 - 0.25 * total, ROOT5_4 * (t1 - t2)
    return v0 + total, mid + dif, e1 + SIN_RATIO * e2, mid - dif, SIN_RATIO * e1 - e2


def z_inverse(a0, a1, b1, a2, b2):
    total = a1 + a2
    mid, dif = a0 - 0.25 * total, ROOT5_4 * (a1 - a2)
    p, q = mid + dif, mid - dif
    r, s = b1 + SIN_RATIO * b2, SIN_RATIO * b1 - b2
    return a0 + total, p - r, q - s, q + s, p + r


def split_tiles(u_ref, channels):
    rows, lanes = u_ref.shape[1:]
    out = [[], [], []]
    for k in channels:
        for r in range(0, rows, 2 * SUB):
            cells = [split3(u_ref[k, r:r + 2 * SUB, lane:lane + LANES]) for lane in range(0, lanes, LANES)]
            for i in range(ADDENDS):
                out[i].append(jnp.concatenate([cell[i] for cell in cells], -1))
    return [jnp.concatenate(rows, 0) for rows in out]


def add_tiles(o, n, lanes, first=0):
    for r in range(0, n, SUB):
        for lane in range(0, lanes, LANES):
            cells = [o[b + r:b + r + SUB, lane:lane + LANES] for b in range(0, o.shape[0], n)]
            yield r, lane, functools.reduce(jnp.add, cells)


def forward_stage(u_ref, tables, f_ref, c, pair):
    lanes = f_ref.shape[-1]
    for k, channels in enumerate(((0,), (1, 2), (3, 4))):
        d = split_tiles(u_ref, channels)
        o = dot(tables[k], jnp.concatenate([d[i] for i in ((0, 1, 2, 0) if k else (0, 1, 2, 0, 1, 0))], 0))
        n = CLASS_ROWS[k + 1] - CLASS_ROWS[k]
        for r, lane, v in add_tiles(o, n, pair * lanes):
            at = (c + lane // lanes, slice(CLASS_ROWS[k] + r, CLASS_ROWS[k] + r + SUB), slice(lane % lanes, lane % lanes + LANES))
            f_ref[at] += v


def inverse_stage(s_ref, c, pair, tables, u_ref):
    n, lanes = u_ref.shape[1:]

    def part(i, k):
        return jnp.concatenate([s_ref[0, i, c + u, CLASS_ROWS[k]:CLASS_ROWS[k + 1]] for u in range(pair)], -1)
    o = dot(tables[0], jnp.concatenate([part(i, 0) for i in range(ADDENDS)], 0))
    for r, lane, v in add_tiles(o, n, lanes):
        u_ref[0, r:r + SUB, lane:lane + LANES] = v
    for k in (1, 2):
        d1, d2, d3 = (part(i, k) for i in range(ADDENDS))
        o = jnp.concatenate([dot(tables[2 * k - 1], jnp.concatenate([d1, d2], 0)),
                             dot(tables[2 * k], jnp.concatenate([d1, d3], 0))], 0)
        for r, lane, v in add_tiles(o, 2 * n, lanes):
            u_ref[2 * k - 1 + r // n, r % n:r % n + SUB, lane:lane + LANES] = v


def registers(pair, lanes):
    for u in range(pair):
        for y in range(Y_BLOCK):
            for lane in range(0, lanes, LANES):
                yield u, y, lane, (slice(y * SUB, (y + 1) * SUB), slice(u * lanes + lane, u * lanes + lane + LANES))


def gelu(h):
    k = 2.0 * math.sqrt(2.0 / math.pi)
    return h + h * jnp.tanh(h * (k + (4.0 * 0.044715 * k) * (h * h)))


def field_lanes(x_ref, y, c):
    return jnp.concatenate([x_ref[x, y, c] for x in range(X_GROUP)], -1)


def zero_spectrum(f_ref):
    def clear(c, _):
        f_ref[c] = jnp.zeros(f_ref.shape[1:], F32)
        return 0
    lax.fori_loop(0, f_ref.shape[0], clear, 0)


def forward_kernel(unit, x_ref, t0, t1, t2, f_ref, u_ref):
    f_ref = f_ref.at[0]
    width, lanes = x_ref.shape[2], f_ref.shape[-1]
    pair, per_step = unit
    tables = (t0[0], t1[0], t2[0])

    @pl.when(pl.program_id(1) == 0)
    def _():
        zero_spectrum(f_ref)

    def load(c, slot):
        for u in range(pair):
            for y in range(Y_BLOCK):
                row = field_lanes(x_ref, y, c + u)
                for k, v in enumerate(z_forward([row[SUB * j:SUB * j + SUB] for j in range(5)])):
                    u_ref[slot, k, y * SUB:(y + 1) * SUB, u * lanes:(u + 1) * lanes] = v

    def body(i, _):
        c = i * per_step
        count = per_step // pair
        for n in range(count + 1):
            if n < count:
                load(c + n * pair, n)
            if n:
                forward_stage(u_ref.at[n - 1], tables, f_ref, c + (n - 1) * pair, pair)
        return 0
    lax.fori_loop(0, width // per_step, body, 0)


def channel_product(first, x_ref, w_ref, p_ref, d_ref):
    blocks, width, depth, lanes = p_ref.shape
    rows = width * SUB
    ones = jnp.ones((w_ref.shape[-1] + CUT - 2 * rows, blocks * lanes), BF16)
    left = [w_ref[0, i] for i in range(w_ref.shape[1])]

    def load(j):
        z = slice(j * SUB, (j + 1) * SUB)
        if first:
            v = [x_ref[x, y, :, z, :] for y in range(blocks) for x in range(X_GROUP)]
        else:
            v = [x_ref[0, y, :, z, :] for y in range(blocks)]
        d_ref[j % 2] = jnp.concatenate(v, -1).reshape(rows, blocks * lanes)

    def product(j):
        d1, d2, d3 = split3(d_ref[j % 2])
        low, high = jnp.concatenate([d1, d2[:CUT]], 0), jnp.concatenate([d2[CUT:], d3, ones], 0)
        p = functools.reduce(jnp.add, [dot(w, low if i < ADDENDS else high) for i, w in enumerate(left)])
        for y in range(blocks):
            p_ref[y, :, j * SUB:(j + 1) * SUB, :] = p[:, y * lanes:(y + 1) * lanes].reshape(width, SUB, lanes)
    count = depth // SUB
    for j in range(count + 1):
        if j < count:
            load(j)
        if j:
            product(j - 1)


def layer_kernel(unit, first, *refs):
    p_ref, s_ref, *tabs = refs
    p_ref = p_ref.at[0]
    width, lanes = p_ref.shape[1], p_ref.shape[-1]
    batch = lanes // X_GROUP
    start = pl.program_id(2) * width
    if first:
        *tabs, v_ref, f_hbm, a_ref, u_ref, f_all, f_sem = tabs
        v_ref = v_ref.at[0]
        group = pl.program_id(0)
        f_ref = f_all.at[group]

        @pl.when((pl.program_id(1) == 0) & (start == 0))
        def _():
            zero_spectrum(f_ref)
    else:
        *tabs, o_ref, a_ref = tabs
    inv, fwd = [t[0] for t in tabs[:5]], [t[0] for t in tabs[5:]]
    pair, per_step = unit

    def activate(c, slot):
        kept_rows = {}
        for u, y, lane, at in registers(pair, lanes):
            new = []
            for j, s in enumerate(z_inverse(*(a_ref[(slot, k) + at] for k in range(5)))):
                g = gelu(s + p_ref[y, c + u, SUB * j:SUB * j + SUB, lane:lane + LANES])
                new.append(g)
                if first:
                    v_ref[y, c + u, SUB * j:SUB * j + SUB, lane:lane + LANES] = g
                else:
                    kept_rows[j] = kept_rows.get(j, ()) + (g,)
            if first:
                for k, v in enumerate(z_forward(new)):
                    u_ref[(slot, k) + at] = v
            elif lane + LANES == lanes:
                for j, row in kept_rows.items():
                    store_field(o_ref, y, c + u, SUB * j, row, batch)
                kept_rows = {}

    def body(i, _):
        c = i * per_step
        count = per_step // pair
        for n in range(count + 2):
            if n < count:
                inverse_stage(s_ref, start + c + n * pair, pair, inv, a_ref.at[n])
            if 0 < n <= count:
                activate(c + (n - 1) * pair, n - 1)
            if first and n > 1:
                forward_stage(u_ref.at[n - 2], fwd, f_ref, start + c + (n - 2) * pair, pair)
        return 0
    lax.fori_loop(0, width // per_step, body, 0)

    if first:
        @pl.when((pl.program_id(1) == pl.num_programs(1) - 1) & (start > 0))
        def _():
            copies = [pltpu.make_async_copy(f_all.at[g], f_hbm.at[g], f_sem.at[g]) for g in range(f_all.shape[0])]
            for g, copy in enumerate(copies):
                pl.when(group == g)(copy.start)

            @pl.when(group == len(copies) - 1)
            def _():
                for copy in copies:
                    copy.wait()


def store_field(o_ref, y, c, z, row, batch):
    lane = lax.broadcasted_iota(jnp.int32, row[0].shape, 1)
    for x in range(X_GROUP):
        at, off = divmod(x * batch, LANES)
        piece = row[at]
        if off + batch > LANES:
            piece = jnp.where(lane < off, row[at + 1], piece)
        if off:
            piece = pltpu.roll(piece, LANES - off, 1)
        o_ref[x, y, c, z:z + SUB, :] = piece[:, :batch]


def split_dot(left, right):
    a, b, c = left
    d1, d2, d3 = split3(right)
    return dot(a, d1) + dot(a, d2) + dot(a, d3) + dot(b, d1) + dot(b, d2) + dot(c, d1)


def x_forward(m_ref, f_ref, s_ref, slot):
    groups, width, lanes = f_ref.shape[0], f_ref.shape[1], f_ref.shape[-1]
    batch = lanes // X_GROUP
    halves = range(f_ref.shape[4])
    rights = []
    for h in halves:
        rows = []
        for g in range(groups):
            for x in range(X_GROUP):
                for p in range(2):
                    rows.append(jnp.concatenate([f_ref[g, c, 0, p, h, :, x * batch:(x + 1) * batch] for c in range(width)], -1))
        rights.append(jnp.concatenate(rows, 0))
    for h in halves:
        out = split_dot((m_ref[0], m_ref[1], m_ref[2]), rights[h])
        s_ref[:, slot, :, h * SUB:(h + 1) * SUB, :] = out.reshape(s_ref.shape[0], 2, SUB, width * batch)


def x_inverse(m_ref, t_ref, slot, s_ref):
    groups, width, lanes = s_ref.shape[0], s_ref.shape[2], s_ref.shape[-1]
    batch = lanes // X_GROUP
    halves = range(s_ref.shape[5])
    outs = []
    for h in halves:
        right = t_ref[:, slot, :, h * SUB:(h + 1) * SUB, :].reshape(t_ref.shape[0] * 2 * SUB, width * batch)
        outs.append(split_dot((m_ref[0], m_ref[1], m_ref[2]), right).reshape(groups, X_GROUP, 2, SUB, width * batch))
    for h in halves:
        for g in range(groups):
            for p in range(2):
                for c in range(width):
                    row = jnp.concatenate([outs[h][g, x, p, :, c * batch:(c + 1) * batch] for x in range(X_GROUP)], -1)
                    for i, d in enumerate(split3(row)):
                        s_ref[g, i, c, 0, p, h] = d


def mix(s_ref, re_w, im_w, t_ref, to, chunk, rows, re_rows, im_rows, re_s, im_s, re_t, im_t):
    own, _, _, n_ky, lanes = s_ref.shape
    width = re_w.shape[2]
    batch = lanes // width
    some = chunk[1] - chunk[0]
    part_modes = some * n_ky
    pick, modes = slice(*chunk), slice(0, own * part_modes)

    for w_ref, out in ((re_w, re_rows), (im_w, im_rows)):
        def lay(c, _):
            for k in range(own):
                for ky in range(n_ky):
                    at = (k * n_ky + ky) * SUB
                    rows[at:at + SUB, 0:width] = w_ref[k, ky, c]
            mat = jnp.concatenate([rows[pl.ds((k * n_ky + h * SUB) * SUB + kz, SUB, stride=SUB), :]
                                   for k in range(own) for kz in KZ_ORDER[pick] for h in range(n_ky // SUB)], 0)
            out[c, :, modes] = mat.T[0:out.shape[1]]
            return 0
        lax.fori_loop(0, width, lay, 0)
    for p, out in enumerate((re_s, im_s)):
        out[:, modes] = jnp.concatenate([s_ref[k, pick, p].reshape(part_modes, lanes) for k in range(own)], 0).T
    pair = 1

    def outputs(i, _):
        d = i * pair

        def inner(c, acc):
            at = pl.ds(pl.multiple_of(c * batch, SUB), batch)
            a, b = re_s[at, modes], im_s[at, modes]
            new = []
            for u in range(pair):
                p = jnp.broadcast_to(re_rows[c, pl.ds(d + u, 1), modes], a.shape)
                q = jnp.broadcast_to(im_rows[c, pl.ds(d + u, 1), modes], a.shape)
                new += [acc[2 * u] + (a * p - b * q), acc[2 * u + 1] + (a * q + b * p)]
            return tuple(new)
        zero = jnp.zeros((batch, own * part_modes), F32)
        acc = lax.fori_loop(0, width, inner, (zero,) * (2 * pair), unroll=True)
        for u in range(pair):
            at = pl.ds(pl.multiple_of((d + u) * batch, SUB), batch)
            re_t[at, modes] = acc[2 * u]
            im_t[at, modes] = acc[2 * u + 1]
        return 0
    lax.fori_loop(0, width // pair, outputs, 0)
    for p, got in enumerate((re_t, im_t)):
        back = got[:, modes].T
        for k in range(own):
            t_ref[to[k], pick, p] = back[k * part_modes:(k + 1) * part_modes].reshape(some, n_ky, lanes)


class Place:
    def __init__(self):
        xs, ys = lax.axis_index('xs'), lax.axis_index('ys')
        data = lax.axis_index('data')
        c, x, y = xs % 2, xs // 2, ys
        self.core = (data, ys, 2 * x + 1 - c)
        self.x_chip = (data, ys, 2 * (1 - x) + c)
        self.y_chip = (data, 1 - ys, xs)
        p, q = lambda a, b: 2 * a + b, lambda a, b: 4 + 2 * a + b
        self.mine = SUB * c
        self.table = 2 * xs + ys
        self.order = (p(1 - x, 1 - y), q(1 - y, 1 - x), p(1 - x, y), q(1 - y, x),
                      p(x, 1 - y), q(y, 1 - x), p(x, y), q(y, x))

    def enter(self):
        barrier = pltpu.get_barrier_semaphore()
        for device in (self.core, self.x_chip, self.y_chip):
            pl.semaphore_signal(barrier, inc=1, device_id=device, device_id_type=pl.DeviceIdType.MESH)
        pl.semaphore_wait(barrier, 3)


def remote(src, dst, send, recv, device):
    return pltpu.make_async_remote_copy(src_ref=src, dst_ref=dst, send_sem=send, recv_sem=recv, device_id=device,
                                        device_id_type=pl.DeviceIdType.MESH)


def step_and_last():
    return pl.program_id(0), pl.num_programs(0) - 1


def chunk_of(ref, k, chunk):
    low, high = chunk
    return ref.at[k, pl.ds(low, high - low)]


def reduce_kernel(first, m_hbm, f_ref, x_ref, w_ref, out_ref, p_ref, m_ref, m_sem, d_ref, s_ref, r1, r2, r3,
                  send1, recv1, send2, recv2, send3, recv3):
    me = Place()
    step, last = step_and_last()
    slots = s_ref.shape[1]
    two, three = [], []

    def to_core(slot):
        return [remote(s_ref.at[SUB + me.order[t], slot], r1.at[t, slot], send1.at[slot, t], recv1.at[slot, t], me.core)
                for t in range(SUB)]
    for h, chunk in enumerate(REDUCE_CHUNKS):
        mine = [chunk_of(s_ref, k, chunk) for k in me.order]
        two.append([remote(mine[t], chunk_of(r2, t, chunk), send2.at[h, t], recv2.at[h, t], (me.x_chip, me.y_chip)[t % 2])
                    for t in range(4)])
        three.append([remote(mine[4 + t], chunk_of(r3, t, chunk), send3.at[h, t], recv3.at[h, t], (me.y_chip, me.x_chip)[t])
                      for t in range(2)])

    def add(dst, a, b):
        def row(i, _):
            dst[i] = a[i] + b[i]
            return 0
        lax.fori_loop(0, dst.shape[0], row, 0)

    def from_core(h):
        arriving = [to_core(slot) for slot in range(*REDUCE_CHUNKS[h])]
        for t in range(SUB):
            for copies in arriving:
                copies[t].wait_recv()
            to = chunk_of(s_ref, me.order[t], REDUCE_CHUNKS[h])
            add(to, to, chunk_of(r1, t, REDUCE_CHUNKS[h]))
            if t < 4:
                two[h][t].start()

    def from_chip(h, these=(0, 1)):
        for t in these:
            two[h][t].wait_recv()
            to = chunk_of(s_ref, me.order[4 + t], REDUCE_CHUNKS[h])
            add(to, to, chunk_of(r2, t, REDUCE_CHUNKS[h]))
            if t < 2:
                three[h][t].start()

    def finish(h):
        from_chip(h, (2, 3))
        for t in range(2):
            three[h][t].wait_recv()
            add(*(chunk_of(ref, k, REDUCE_CHUNKS[h]) for ref, k in ((out_ref, t), (s_ref, me.order[6 + t]), (r3, t))))

    def begin():
        table = pltpu.make_async_copy(m_hbm.at[me.table], m_ref, m_sem)
        table.start()
        me.enter()
        table.wait()

    events = ((0, begin), (2, lambda: from_core(0)), (slots - 3, lambda: from_chip(0)), (slots - 2, lambda: from_core(1)),
              (slots, lambda: from_core(2)), (slots + 3, lambda: finish(0)), (slots + 5, lambda: from_chip(1)),
              (slots + 12, lambda: from_chip(2)))
    for at, event in events:
        pl.when(step == at)(event)

    @pl.when(step < slots)
    def _():
        x_forward(m_ref, f_ref, s_ref, step)
        for copy in to_core(step):
            copy.start()

    @pl.when(step >= slots)
    def _():
        channel_product(first, x_ref, w_ref, p_ref.at[0], d_ref)

    @pl.when(step == last)
    def _():
        finish(1)
        finish(2)
        for copies in [to_core(slot) for slot in range(slots)] + two + three:
            for copy in copies:
                copy.wait_send()


def gather_kernel(first, layer, m_hbm, s_ref, re_hbm, im_hbm, x_ref, w_ref, p_in, parts_ref, p_ref, m_ref, m_sem, d_ref, t_ref,
                  re_w, im_w, rows, re_rows, im_rows, re_s, im_s, re_t, im_t, w_sem, send_sem, recv_sem):
    me = Place()
    step, last = step_and_last()
    p3, q3, p2, q2, p1, q1, p0, q0 = me.order
    plan = [(p0, me.y_chip, 0), (q0, me.x_chip, 0), (p0, me.x_chip, 0), (q0, me.y_chip, 0), (p0, me.core, SUB), (q0, me.core, SUB),
            (p1, me.x_chip, 0), (q1, me.y_chip, 0)] + [(k, me.core, SUB) for k in (p1, q1, p2, q2, p3, q3)]
    copies = [[remote(chunk_of(t_ref, k, chunk), chunk_of(t_ref, k + up, chunk), send_sem.at[h, n], recv_sem.at[h, n], device)
               for n, (k, device, up) in enumerate(plan)] for h, chunk in enumerate(GATHER_CHUNKS)]
    weights = [pltpu.make_async_copy(hbm.at[layer, me.mine + k], to.at[i], w_sem.at[n, i])
               for n, (hbm, to) in enumerate(((re_hbm, re_w), (im_hbm, im_w))) for i, k in enumerate((p0, q0))]
    weights.append(pltpu.make_async_copy(m_hbm.at[me.table], m_ref, m_sem))

    def mixed(h):
        mix(s_ref, re_w, im_w, t_ref, (p0, q0), MIX_CHUNKS[h], rows, re_rows, im_rows, re_s, im_s, re_t, im_t)

    def send(h):
        for copy in copies[h][:6]:
            copy.start()

    def begin():
        for copy in weights:
            copy.start()
        me.enter()
        for copy in weights:
            copy.wait()
        mixed(0)
        send(0)

    def follow(h):
        pass_on(h)
        send(h + 1)

    def pass_on(h):
        for n in range(2):
            copies[h][n].wait_recv()
            copies[h][6 + n].start()
            copies[h][SUB + n].start()

    def finish(h):
        for n, arrived in enumerate((2, 3, 6, 7)):
            copies[h][arrived].wait_recv()
            copies[h][10 + n].start()
        for n in (4, 5, *range(SUB, len(plan))):
            copies[h][n].wait_recv()

    x_from = last + 1 - t_ref.shape[1]
    for at, event in ((0, begin), (1, lambda: mixed(1)), (5, lambda: follow(0)), (x_from, lambda: finish(0)),
                      (x_from + 1, lambda: follow(1)), (x_from + 4, lambda: finish(1)), (x_from + 5, lambda: pass_on(2)),
                      (x_from + 6, lambda: finish(2))):
        pl.when(step == at)(event)

    @pl.when((step >= 2) & (step < x_from + 4))
    def _():
        channel_product(first, x_ref, w_ref, p_ref.at[0], d_ref)

    @pl.when(step >= x_from)
    def _():
        x_inverse(m_ref, t_ref, step - x_from, parts_ref)

    @pl.when(step == last)
    def _():
        for some in copies:
            for copy in some:
                copy.wait_send()


def block(shape, index, slot=None, **kwargs):
    def index_map(*at):
        return tuple(0 if k == 'o' else slot(at[0]) if k == 's' else at['ijk'.index(k)] for k in index)
    return pl.BlockSpec(shape, index_map, **kwargs)


def point_table_kernel(w_ref, b_ref, out_ref):
    layers, width = b_ref.shape
    rows = width * SUB

    def spread(shape, axis):
        at = [lax.broadcasted_iota(jnp.int32, shape, k) for k in range(2)]
        return jnp.where(at[axis] // SUB == at[1 - axis], 1.0, 0.0).astype(BF16)
    down, across = spread((rows, width), 0), spread((width, rows), 1)
    at = [lax.broadcasted_iota(jnp.int32, (rows, rows), k) % SUB for k in range(2)]
    column = lax.broadcasted_iota(jnp.int32, (rows, out_ref.shape[-1] + CUT - 2 * rows), 1)
    for layer in range(layers):
        weights, biases = split3(HALF * w_ref[layer].T), split3(HALF * b_ref[layer:layer + 1])
        shift = sum(jnp.where(column == i, jnp.sum(down.astype(F32) * b.astype(F32), 1, keepdims=True), 0.0)
                    for i, b in enumerate(biases))
        a, b, c = (jnp.where(at[0] == at[1], dot(dot(down, w).astype(BF16), across), 0.0) for w in weights)
        none = jnp.zeros_like(a)
        for i, parts in enumerate(((a, a[:, :CUT]), (b, b[:, :CUT]), (c, none[:, :CUT]),
                                   (a[:, CUT:], a, shift), (b[:, CUT:], none, jnp.zeros_like(shift)))):
            out_ref[layer, i] = jnp.concatenate(parts, 1).astype(BF16)


def solution(mesh):
    row_devs, col_devs = mesh.shape['ys'], mesh.shape['xs']

    def local_layers(field, spec_real, spec_imag, mix_weight, bias):
        batch, x_loc, y_loc, grid_z, width = field.shape
        modes = spec_real.shape[3]
        grid_x, grid_y = x_loc * col_devs, y_loc * row_devs
        groups, blocks = x_loc // X_GROUP, y_loc // Y_BLOCK
        lanes = X_GROUP * batch
        kx, ky = kept(modes, grid_x), kept(modes, grid_y)
        n_kx, n_ky = len(kx), len(ky)
        fwd_np, inv_np = all_tables(blocks, ky, grid_y, grid_z, grid_x * grid_y * grid_z)
        fwd, inv = [jnp.asarray(t) for t in fwd_np], [jnp.asarray(t) for t in inv_np]

        turn = 2.0 * math.pi * (kx[:, None] * np.arange(grid_x)[None, :] % grid_x) / grid_x
        cos, sin = np.cos(turn), np.sin(turn)
        fwd_x = np.stack([np.stack([cos, sin], -1), np.stack([-sin, cos], -1)], 1)
        inv_x = np.transpose(fwd_x, (2, 3, 0, 1))
        fwd_x = fwd_x.reshape(n_kx, 2, col_devs, x_loc, 2).transpose(2, 0, 1, 3, 4).reshape(col_devs, 2 * n_kx, 2 * x_loc)
        inv_x = inv_x.reshape(col_devs, 2 * x_loc, 2 * n_kx)
        odd_rows = np.where(np.arange(2 * SUB * x_loc) % 2, -1.0, 1.0)[:, None]

        def x_tables(tables, axis):
            out = []
            for xs in range(col_devs):
                t = np.roll(np.kron(tables[xs], np.eye(SUB)), SUB * n_kx * (xs % 2), axis)
                out += [np.stack(pieces(t * sign)) for sign in (1.0, odd_rows)]
            return jnp.asarray(np.stack(out))
        fwd_x, inv_x = x_tables(fwd_x, 0), x_tables(inv_x, 1)
        params = pltpu.CompilerParams(vmem_limit_bytes=VMEM_LIMIT)
        point_w = pl.pallas_call(
            point_table_kernel, out_shape=jax.ShapeDtypeStruct((2, 5, width * SUB, width * SUB + CUT), BF16),
            compiler_params=params, name='point_table')(mix_weight, bias)

        real_w, imag_w = (jnp.swapaxes(w, 3, 4) for w in (spec_real, spec_imag))
        v = jnp.swapaxes(jnp.moveaxis(field, 0, -1), 2, 3)
        grid = (groups, blocks, 2)
        part_width = width // 2
        spec_shape = jax.ShapeDtypeStruct((groups, width, 256, lanes), F32)
        in_block = block((X_GROUP, Y_BLOCK, part_width, grid_z, batch), 'ijkoo')
        mid_block = block((1, Y_BLOCK, part_width, grid_z, lanes), 'ijkoo')
        part_block = block((1, ADDENDS, width, CLASS_ROWS[-1], lanes), 'ioooo')
        mid_shape = jax.ShapeDtypeStruct((groups, y_loc, width, grid_z, lanes), F32)
        anywhere = pl.BlockSpec(memory_space=pl.ANY)

        def stage(unit):
            return pltpu.VMEM((unit[1] // unit[0], 5, Y_BLOCK * SUB, unit[0] * lanes), F32)

        units = y_loc // HALF_BLOCK

        def unit_block(first, steps, base, count):
            shape = (HALF_BLOCK, width, grid_z) + ((batch,) if first else (lanes,))

            def index_map(j):
                n = jnp.clip(j - steps, 0, count - 1) + base
                return n // units, n % units, 0, 0, 0
            return pl.BlockSpec((X_GROUP if first else 1,) + shape, index_map)

        def table_specs(tables):
            return [block((1,) + t.shape[1:], 'joo') for t in tables]

        f = pl.pallas_call(
            functools.partial(forward_kernel, FORWARD_UNIT), grid=grid[:2], out_shape=spec_shape,
            in_specs=[block((X_GROUP, Y_BLOCK, width, grid_z, batch), 'ijooo')] + table_specs(fwd),
            out_specs=block((1, width, 256, lanes), 'iooo'),
            scratch_shapes=[stage(FORWARD_UNIT)], compiler_params=params, name='forward')(v, *fwd)

        own, slots, halves = 2, SUB, n_ky // SUB
        unit = (slots, 2, n_ky, width * batch)
        own_block = block((own,) + unit, 'ooooo')

        def w_block(layer):
            return block((1,) + point_w.shape[1:], 'sooo', lambda j: layer)
        dma = pltpu.SemaphoreType.DMA
        x_scratch = [pltpu.VMEM(fwd_x.shape[1:], BF16), dma]
        half_rows = pltpu.VMEM((2, width * SUB, HALF_BLOCK * lanes), F32)

        def exchange(number):
            return pltpu.CompilerParams(vmem_limit_bytes=VMEM_LIMIT, collective_id=number, has_side_effects=True)

        def across(f, layer, source):
            first, early = layer == 0, REDUCE_UNITS[layer]
            late = groups * units - early
            s, p = pl.pallas_call(
                functools.partial(reduce_kernel, first), grid=(slots + early,),
                out_shape=(jax.ShapeDtypeStruct((own,) + unit, F32), mid_shape),
                in_specs=[anywhere,
                          block((groups, width, 1, 2, halves, SUB, lanes), 'oosoooo', lambda j: jnp.minimum(j, slots - 1)),
                          unit_block(first, slots, 0, early), w_block(layer)],
                out_specs=(own_block, unit_block(False, slots, 0, early)),
                scratch_shapes=x_scratch + [half_rows] + [pltpu.VMEM((n,) + unit, F32) for n in (n_kx, SUB, 4, 2)]
                + [dma((slots, SUB))] * 2 + [dma((len(REDUCE_CHUNKS), n)) for n in (4, 4, 2, 2)],
                compiler_params=exchange(2 * layer), name='reduce')(
                    fwd_x, f.reshape(groups, width, slots, 2, halves, SUB, lanes), source, point_w)
            parts, p = pl.pallas_call(
                functools.partial(gather_kernel, first, layer), grid=(late + 6,),
                out_shape=(jax.ShapeDtypeStruct((groups, ADDENDS, width, slots, 2, halves, SUB, lanes), BF16), mid_shape),
                in_specs=[anywhere, own_block, anywhere, anywhere, unit_block(first, 2, early, late), w_block(layer), anywhere],
                out_specs=(block((groups, ADDENDS, width, 1, 2, halves, SUB, lanes), 'ooosoooo', lambda j: jnp.maximum(j - late + 2, 0)),
                           unit_block(False, 2, early, late)),
                input_output_aliases={6: 1},
                scratch_shapes=x_scratch + [half_rows, pltpu.VMEM((n_kx,) + unit, F32)]
                + [pltpu.VMEM((own, n_ky, width, SUB, width), F32)] * 2
                + [pltpu.VMEM((own * n_ky * SUB, LANES), F32)] + [pltpu.VMEM((width, 24, LANES), F32)] * 2
                + [pltpu.VMEM((width * batch, LANES), F32)] * 4
                + [dma((2, 2))] + [dma((len(GATHER_CHUNKS), 14))] * 2,
                compiler_params=exchange(2 * layer + 1), name='gather')(
                    inv_x, s, real_w, imag_w, source, point_w, p)
            return parts.reshape(groups, ADDENDS, width, CLASS_ROWS[-1], lanes), p

        parts, p = across(f, 0, v)
        v1, f = pl.pallas_call(
            functools.partial(layer_kernel, FIRST_UNIT, True), grid=grid, out_shape=(mid_shape, spec_shape),
            in_specs=[mid_block, part_block] + table_specs(inv) + table_specs(fwd),
            out_specs=(mid_block, anywhere),
            scratch_shapes=[stage(FIRST_UNIT)] * 2 + [pltpu.VMEM(spec_shape.shape, F32), pltpu.SemaphoreType.DMA((groups,))],
            compiler_params=params, name='layer_first')(p, parts, *inv, *fwd)
        parts, p = across(f, 1, v1)
        out = pl.pallas_call(
            functools.partial(layer_kernel, LAST_UNIT, False), grid=grid,
            out_shape=jax.ShapeDtypeStruct((x_loc, y_loc, width, grid_z, batch), F32),
            in_specs=[mid_block, part_block] + table_specs(inv), out_specs=in_block, scratch_shapes=[stage(LAST_UNIT)],
            compiler_params=params, name='layer_last')(p, parts, *inv)
        return jnp.moveaxis(jnp.swapaxes(out, 2, 3), -1, 0)

    field_spec = P('data', 'xs', 'ys', None, None)
    return jax.shard_map(local_layers, mesh=mesh, in_specs=(field_spec, P(), P(), P(), P()), out_specs=field_spec, check_vma=False)
```

```python
import functools
import math

import jax
import jax.numpy as jnp
import ml_dtypes
import numpy as np
from jax import lax
from jax.experimental import pallas as pl
from jax.experimental.pallas import tpu as pltpu
from jax.sharding import PartitionSpec as P

F32 = jnp.float32
BF16 = jnp.bfloat16
VMEM_LIMIT = 64 * 1024 * 1024 - 65536

SUB = 8
X_GROUP = 8
Y_BLOCK = 4
HALF_BLOCK = 2
Z_BLOCK = 8
KZ_CLASS = ((0, 5), (1, 6, 4), (2, 7, 3))
KZ_ORDER = tuple(kz for group in KZ_CLASS for kz in group)
CLASS_ROWS = (0, 64, 160, 256)
LANES = 128
ADDENDS = 3
CUT = 96
HALF = 0.5
REDUCE_UNITS = (20, 22)
REDUCE_CHUNKS = ((0, 1), (1, 3), (3, 8))
GATHER_CHUNKS = ((0, 4), (4, 6), (6, 8))
MIX_CHUNKS = ((0, 4), (4, 8))
FORWARD_UNIT = (2, 10)
FIRST_UNIT = (2, 10)
LAST_UNIT = (1, 10)
ROOT5_4 = math.sqrt(5.0) / 4.0
SIN_1 = math.sin(2.0 * math.pi / 5.0)
SIN_RATIO = math.sin(4.0 * math.pi / 5.0) / SIN_1


def kz_sign(kz):
    return 0 if kz % 5 == 0 else (1 if kz % 5 < 3 else -1)


def kept(modes, size):
    return np.concatenate([np.arange(modes), np.arange(size - modes, size)])


def pieces(table):
    rest = np.asarray(table, np.float32)
    out = []
    for _ in range(ADDENDS):
        out.append(rest.astype(ml_dtypes.bfloat16))
        rest = rest - out[-1].astype(np.float32)
    return out


def yz_angles(kz, y_pos, ky, grid_y, grid_z):
    z_pos = np.arange(Z_BLOCK)
    turn = (ky[:, None, None] * y_pos[None, :, None] % grid_y) / grid_y + kz * z_pos[None, None, :] / grid_z
    return 2.0 * math.pi * turn


def forward_table(group, y_pos, ky, grid_y, grid_z):
    rows = []
    for kz in group:
        t, s = yz_angles(kz, y_pos, ky, grid_y, grid_z), kz_sign(kz)
        real, imag = [np.cos(t)], [-np.sin(t)]
        if s:
            real.append(-s * SIN_1 * np.sin(t))
            imag.append(-s * SIN_1 * np.cos(t))
        rows += [np.stack(part, 1).reshape(len(ky), -1) for part in (real, imag)]
    return np.concatenate(rows, 0)


def inverse_table(group, y_pos, ky, grid_y, grid_z, points):
    cols = []
    for kz in group:
        t, s = yz_angles(kz, y_pos, ky, grid_y, grid_z).transpose(1, 2, 0), kz_sign(kz)
        w = (HALF if kz == 0 else 1.0) / points
        real, imag = [w * np.cos(t)], [-w * np.sin(t)]
        if s:
            real.append(s * SIN_1 * w * np.sin(t))
            imag.append(s * SIN_1 * w * np.cos(t))
        cols += [np.stack(part, 0).reshape(-1, len(ky)) for part in (real, imag)]
    return np.concatenate(cols, 1)


def all_tables(blocks, ky, grid_y, grid_z, points):
    fwd, inv = [[], [], []], [[], [], [], [], []]
    for block in range(blocks):
        y_pos = np.arange(Y_BLOCK) + block * Y_BLOCK
        for k, group in enumerate(KZ_CLASS):
            a, b, c = pieces(forward_table(group, y_pos, ky, grid_y, grid_z))
            n = np.zeros_like(a)
            if k == 0:
                fwd[k].append(np.concatenate([a, a, a, b, b, c], 1))
            else:
                fwd[k].append(np.block([[a, a, a, b], [c, b, n, n]]))
            a, b, c = pieces(inverse_table(group, y_pos, ky, grid_y, grid_z, points))
            n = np.zeros_like(a)
            if k == 0:
                inv[0].append(np.block([[a, a, a], [b, b, n], [c, n, n]]))
            else:
                inv[2 * k - 1].append(np.block([[a, a], [b, b]]))
                inv[2 * k].append(np.concatenate([c, a], 1))
    return [np.stack(t) for t in fwd], [np.stack(t) for t in inv]


def split3(v):
    d1 = v.astype(BF16)
    rest = v - d1.astype(F32)
    d2 = rest.astype(BF16)
    return d1, d2, (rest - d2.astype(F32)).astype(BF16)


def dot(a, b):
    return jnp.dot(a, b, preferred_element_type=F32)


def z_forward(v):
    v0, v1, v2, v3, v4 = v
    t1, t2, e1, e2 = v1 + v4, v2 + v3, v1 - v4, v2 - v3
    total = t1 + t2
    mid, dif = v0 - 0.25 * total, ROOT5_4 * (t1 - t2)
    return v0 + total, mid + dif, e1 + SIN_RATIO * e2, mid - dif, SIN_RATIO * e1 - e2


def z_inverse(a0, a1, b1, a2, b2):
    total = a1 + a2
    mid, dif = a0 - 0.25 * total, ROOT5_4 * (a1 - a2)
    p, q = mid + dif, mid - dif
    r, s = b1 + SIN_RATIO * b2, SIN_RATIO * b1 - b2
    return a0 + total, p - r, q - s, q + s, p + r


def split_tiles(u_ref, channels):
    rows, lanes = u_ref.shape[1:]
    out = [[], [], []]
    for k in channels:
        for r in range(0, rows, 2 * SUB):
            cells = [split3(u_ref[k, r:r + 2 * SUB, lane:lane + LANES]) for lane in range(0, lanes, LANES)]
            for i in range(ADDENDS):
                out[i].append(jnp.concatenate([cell[i] for cell in cells], -1))
    return [jnp.concatenate(rows, 0) for rows in out]


def add_tiles(o, n, lanes, first=0):
    for r in range(0, n, SUB):
        for lane in range(0, lanes, LANES):
            cells = [o[b + r:b + r + SUB, lane:lane + LANES] for b in range(0, o.shape[0], n)]
            yield r, lane, functools.reduce(jnp.add, cells)


def forward_stage(u_ref, tables, f_ref, c, pair):
    lanes = f_ref.shape[-1]
    for k, channels in enumerate(((0,), (1, 2), (3, 4))):
        d = split_tiles(u_ref, channels)
        o = dot(tables[k], jnp.concatenate([d[i] for i in ((0, 1, 2, 0) if k else (0, 1, 2, 0, 1, 0))], 0))
        n = CLASS_ROWS[k + 1] - CLASS_ROWS[k]
        for r, lane, v in add_tiles(o, n, pair * lanes):
            at = (c + lane // lanes, slice(CLASS_ROWS[k] + r, CLASS_ROWS[k] + r + SUB), slice(lane % lanes, lane % lanes + LANES))
            f_ref[at] += v


def inverse_stage(s_ref, c, pair, tables, u_ref):
    n, lanes = u_ref.shape[1:]

    def part(i, k):
        return jnp.concatenate([s_ref[0, i, c + u, CLASS_ROWS[k]:CLASS_ROWS[k + 1]] for u in range(pair)], -1)
    o = dot(tables[0], jnp.concatenate([part(i, 0) for i in range(ADDENDS)], 0))
    for r, lane, v in add_tiles(o, n, lanes):
        u_ref[0, r:r + SUB, lane:lane + LANES] = v
    for k in (1, 2):
        d1, d2, d3 = (part(i, k) for i in range(ADDENDS))
        o = jnp.concatenate([dot(tables[2 * k - 1], jnp.concatenate([d1, d2], 0)),
                             dot(tables[2 * k], jnp.concatenate([d1, d3], 0))], 0)
        for r, lane, v in add_tiles(o, 2 * n, lanes):
            u_ref[2 * k - 1 + r // n, r % n:r % n + SUB, lane:lane + LANES] = v


def registers(pair, lanes):
    for u in range(pair):
        for y in range(Y_BLOCK):
            for lane in range(0, lanes, LANES):
                yield u, y, lane, (slice(y * SUB, (y + 1) * SUB), slice(u * lanes + lane, u * lanes + lane + LANES))


def gelu(h):
    k = 2.0 * math.sqrt(2.0 / math.pi)
    return h + h * jnp.tanh(h * (k + (4.0 * 0.044715 * k) * (h * h)))


def field_lanes(x_ref, y, c):
    return jnp.concatenate([x_ref[x, y, c] for x in range(X_GROUP)], -1)


def zero_spectrum(f_ref):
    def clear(c, _):
        f_ref[c] = jnp.zeros(f_ref.shape[1:], F32)
        return 0
    lax.fori_loop(0, f_ref.shape[0], clear, 0)


def forward_kernel(unit, x_ref, t0, t1, t2, f_ref, u_ref):
    f_ref = f_ref.at[0]
    width, lanes = x_ref.shape[2], f_ref.shape[-1]
    pair, per_step = unit
    tables = (t0[0], t1[0], t2[0])

    @pl.when(pl.program_id(1) == 0)
    def _():
        zero_spectrum(f_ref)

    def load(c, slot):
        for u in range(pair):
            for y in range(Y_BLOCK):
                row = field_lanes(x_ref, y, c + u)
                for k, v in enumerate(z_forward([row[SUB * j:SUB * j + SUB] for j in range(5)])):
                    u_ref[slot, k, y * SUB:(y + 1) * SUB, u * lanes:(u + 1) * lanes] = v

    def body(i, _):
        c = i * per_step
        count = per_step // pair
        for n in range(count + 1):
            if n < count:
                load(c + n * pair, n)
            if n:
                forward_stage(u_ref.at[n - 1], tables, f_ref, c + (n - 1) * pair, pair)
        return 0
    lax.fori_loop(0, width // per_step, body, 0)


def channel_product(first, x_ref, w_ref, p_ref, d_ref):
    blocks, width, depth, lanes = p_ref.shape
    rows = width * SUB
    ones = jnp.ones((w_ref.shape[-1] + CUT - 2 * rows, blocks * lanes), BF16)
    left = [w_ref[0, i] for i in range(w_ref.shape[1])]

    def load(j):
        z = slice(j * SUB, (j + 1) * SUB)
        if first:
            v = [x_ref[x, y, :, z, :] for y in range(blocks) for x in range(X_GROUP)]
        else:
            v = [x_ref[0, y, :, z, :] for y in range(blocks)]
        d_ref[j % 2] = jnp.concatenate(v, -1).reshape(rows, blocks * lanes)

    def product(j):
        d1, d2, d3 = split3(d_ref[j % 2])
        low, high = jnp.concatenate([d1, d2[:CUT]], 0), jnp.concatenate([d2[CUT:], d3, ones], 0)
        p = functools.reduce(jnp.add, [dot(w, low if i < ADDENDS else high) for i, w in enumerate(left)])
        for y in range(blocks):
            p_ref[y, :, j * SUB:(j + 1) * SUB, :] = p[:, y * lanes:(y + 1) * lanes].reshape(width, SUB, lanes)
    count = depth // SUB
    for j in range(count + 1):
        if j < count:
            load(j)
        if j:
            product(j - 1)


def layer_kernel(unit, first, *refs):
    p_ref, s_ref, *tabs = refs
    p_ref = p_ref.at[0]
    width, lanes = p_ref.shape[1], p_ref.shape[-1]
    batch = lanes // X_GROUP
    start = pl.program_id(1) * width
    if first:
        *tabs, v_ref, f_hbm, a_ref, u_ref, f_all, f_sem = tabs
        v_ref = v_ref.at[0]
        group = pl.program_id(0)
        f_ref = f_all.at[group, pl.ds(start, width)]

        @pl.when(pl.program_id(2) == 0)
        def _():
            zero_spectrum(f_ref)
    else:
        *tabs, o_ref, a_ref = tabs
    inv, fwd = [t[0] for t in tabs[:5]], [t[0] for t in tabs[5:]]
    pair, per_step = unit

    def activate(c, slot):
        kept_rows = {}
        for u, y, lane, at in registers(pair, lanes):
            new = []
            for j, s in enumerate(z_inverse(*(a_ref[(slot, k) + at] for k in range(5)))):
                g = gelu(s + p_ref[y, c + u, SUB * j:SUB * j + SUB, lane:lane + LANES])
                new.append(g)
                if first:
                    v_ref[y, c + u, SUB * j:SUB * j + SUB, lane:lane + LANES] = g
                else:
                    kept_rows[j] = kept_rows.get(j, ()) + (g,)
            if first:
                for k, v in enumerate(z_forward(new)):
                    u_ref[(slot, k) + at] = v
            elif lane + LANES == lanes:
                for j, row in kept_rows.items():
                    store_field(o_ref, y, c + u, SUB * j, row, batch)
                kept_rows = {}

    def body(i, _):
        c = i * per_step
        count = per_step // pair
        for n in range(count + 2):
            if n < count:
                inverse_stage(s_ref, c + n * pair, pair, inv, a_ref.at[n])
            if 0 < n <= count:
                activate(c + (n - 1) * pair, n - 1)
            if first and n > 1:
                forward_stage(u_ref.at[n - 2], fwd, f_ref, c + (n - 2) * pair, pair)
        return 0
    lax.fori_loop(0, width // per_step, body, 0)

    if first:
        @pl.when((pl.program_id(2) == pl.num_programs(2) - 1) & (start > 0))
        def _():
            copies = [pltpu.make_async_copy(f_all.at[g], f_hbm.at[g], f_sem.at[g]) for g in range(f_all.shape[0])]
            for g, copy in enumerate(copies):
                pl.when(group == g)(copy.start)

            @pl.when(group == len(copies) - 1)
            def _():
                for copy in copies:
                    copy.wait()


def store_field(o_ref, y, c, z, row, batch):
    lane = lax.broadcasted_iota(jnp.int32, row[0].shape, 1)
    for x in range(X_GROUP):
        at, off = divmod(x * batch, LANES)
        piece = row[at]
        if off + batch > LANES:
            piece = jnp.where(lane < off, row[at + 1], piece)
        if off:
            piece = pltpu.roll(piece, LANES - off, 1)
        o_ref[x, y, c, z:z + SUB, :] = piece[:, :batch]


def split_dot(left, right):
    a, b, c = left
    d1, d2, d3 = split3(right)
    return dot(a, d1) + dot(a, d2) + dot(a, d3) + dot(b, d1) + dot(b, d2) + dot(c, d1)


def x_forward(m_ref, f_ref, s_ref, slot):
    groups, width, lanes = f_ref.shape[0], f_ref.shape[1], f_ref.shape[-1]
    batch = lanes // X_GROUP
    halves = range(f_ref.shape[4])
    rights = []
    for h in halves:
        rows = []
        for g in range(groups):
            for x in range(X_GROUP):
                for p in range(2):
                    rows.append(jnp.concatenate([f_ref[g, c, 0, p, h, :, x * batch:(x + 1) * batch] for c in range(width)], -1))
        rights.append(jnp.concatenate(rows, 0))
    for h in halves:
        out = split_dot((m_ref[0], m_ref[1], m_ref[2]), rights[h])
        s_ref[:, slot, :, h * SUB:(h + 1) * SUB, :] = out.reshape(s_ref.shape[0], 2, SUB, width * batch)


def x_inverse(m_ref, t_ref, slot, s_ref):
    groups, width, lanes = s_ref.shape[0], s_ref.shape[2], s_ref.shape[-1]
    batch = lanes // X_GROUP
    halves = range(s_ref.shape[5])
    outs = []
    for h in halves:
        right = t_ref[:, slot, :, h * SUB:(h + 1) * SUB, :].reshape(t_ref.shape[0] * 2 * SUB, width * batch)
        outs.append(split_dot((m_ref[0], m_ref[1], m_ref[2]), right).reshape(groups, X_GROUP, 2, SUB, width * batch))
    for h in halves:
        for g in range(groups):
            for p in range(2):
                for c in range(width):
                    row = jnp.concatenate([outs[h][g, x, p, :, c * batch:(c + 1) * batch] for x in range(X_GROUP)], -1)
                    for i, d in enumerate(split3(row)):
                        s_ref[g, i, c, 0, p, h] = d


def mix(s_ref, re_w, im_w, t_ref, to, chunk, rows, re_rows, im_rows, re_s, im_s, re_t, im_t):
    own, _, _, n_ky, lanes = s_ref.shape
    width = re_w.shape[2]
    batch = lanes // width
    some = chunk[1] - chunk[0]
    part_modes = some * n_ky
    pick, modes = slice(*chunk), slice(0, own * part_modes)

    for w_ref, out in ((re_w, re_rows), (im_w, im_rows)):
        def lay(c, _):
            for k in range(own):
                for ky in range(n_ky):
                    at = (k * n_ky + ky) * SUB
                    rows[at:at + SUB, 0:width] = w_ref[k, ky, c]
            mat = jnp.concatenate([rows[pl.ds((k * n_ky + h * SUB) * SUB + kz, SUB, stride=SUB), :]
                                   for k in range(own) for kz in KZ_ORDER[pick] for h in range(n_ky // SUB)], 0)
            out[c, :, modes] = mat.T[0:out.shape[1]]
            return 0
        lax.fori_loop(0, width, lay, 0)
    for p, out in enumerate((re_s, im_s)):
        out[:, modes] = jnp.concatenate([s_ref[k, pick, p].reshape(part_modes, lanes) for k in range(own)], 0).T
    pair = 1

    def outputs(i, _):
        d = i * pair

        def inner(c, acc):
            at = pl.ds(pl.multiple_of(c * batch, SUB), batch)
            a, b = re_s[at, modes], im_s[at, modes]
            new = []
            for u in range(pair):
                p = jnp.broadcast_to(re_rows[c, pl.ds(d + u, 1), modes], a.shape)
                q = jnp.broadcast_to(im_rows[c, pl.ds(d + u, 1), modes], a.shape)
                new += [acc[2 * u] + (a * p - b * q), acc[2 * u + 1] + (a * q + b * p)]
            return tuple(new)
        zero = jnp.zeros((batch, own * part_modes), F32)
        acc = lax.fori_loop(0, width, inner, (zero,) * (2 * pair), unroll=True)
        for u in range(pair):
            at = pl.ds(pl.multiple_of((d + u) * batch, SUB), batch)
            re_t[at, modes] = acc[2 * u]
            im_t[at, modes] = acc[2 * u + 1]
        return 0
    lax.fori_loop(0, width // pair, outputs, 0)
    for p, got in enumerate((re_t, im_t)):
        back = got[:, modes].T
        for k in range(own):
            t_ref[to[k], pick, p] = back[k * part_modes:(k + 1) * part_modes].reshape(some, n_ky, lanes)


class Place:
    def __init__(self):
        xs, ys = lax.axis_index('xs'), lax.axis_index('ys')
        data = lax.axis_index('data')
        c, x, y = xs % 2, xs // 2, ys
        self.core = (data, ys, 2 * x + 1 - c)
        self.x_chip = (data, ys, 2 * (1 - x) + c)
        self.y_chip = (data, 1 - ys, xs)
        p, q = lambda a, b: 2 * a + b, lambda a, b: 4 + 2 * a + b
        self.mine = SUB * c
        self.table = 2 * xs + ys
        self.order = (p(1 - x, 1 - y), q(1 - y, 1 - x), p(1 - x, y), q(1 - y, x),
                      p(x, 1 - y), q(y, 1 - x), p(x, y), q(y, x))

    def enter(self):
        barrier = pltpu.get_barrier_semaphore()
        for device in (self.core, self.x_chip, self.y_chip):
            pl.semaphore_signal(barrier, inc=1, device_id=device, device_id_type=pl.DeviceIdType.MESH)
        pl.semaphore_wait(barrier, 3)


def remote(src, dst, send, recv, device):
    return pltpu.make_async_remote_copy(src_ref=src, dst_ref=dst, send_sem=send, recv_sem=recv, device_id=device,
                                        device_id_type=pl.DeviceIdType.MESH)


def run(event):
    event()


def step_and_last():
    return pl.program_id(0), pl.num_programs(0) - 1


def chunk_of(ref, k, chunk):
    low, high = chunk
    return ref.at[k, pl.ds(low, high - low)]


def reduce_kernel(first, m_hbm, f_ref, x_ref, w_ref, out_ref, p_ref, m_ref, m_sem, d_ref, s_ref, r1, r2, r3,
                  send1, recv1, send2, recv2, send3, recv3):
    me = Place()
    step, last = step_and_last()
    slots = s_ref.shape[1]
    two, three = [], []

    def to_core(slot):
        return [remote(s_ref.at[SUB + me.order[t], slot], r1.at[t, slot], send1.at[slot, t], recv1.at[slot, t], me.core)
                for t in range(SUB)]
    for h, chunk in enumerate(REDUCE_CHUNKS):
        mine = [chunk_of(s_ref, k, chunk) for k in me.order]
        two.append([remote(mine[t], chunk_of(r2, t, chunk), send2.at[h, t], recv2.at[h, t], (me.x_chip, me.y_chip)[t % 2])
                    for t in range(4)])
        three.append([remote(mine[4 + t], chunk_of(r3, t, chunk), send3.at[h, t], recv3.at[h, t], (me.y_chip, me.x_chip)[t])
                      for t in range(2)])

    def add(dst, a, b):
        def row(i, _):
            dst[i] = a[i] + b[i]
            return 0
        lax.fori_loop(0, dst.shape[0], row, 0)

    def from_core(h):
        arriving = [to_core(slot) for slot in range(*REDUCE_CHUNKS[h])]
        for t in range(SUB):
            for copies in arriving:
                copies[t].wait_recv()
            to = chunk_of(s_ref, me.order[t], REDUCE_CHUNKS[h])
            add(to, to, chunk_of(r1, t, REDUCE_CHUNKS[h]))
            if t < 4:
                two[h][t].start()

    def from_chip(h, these=(0, 1)):
        for t in these:
            two[h][t].wait_recv()
            to = chunk_of(s_ref, me.order[4 + t], REDUCE_CHUNKS[h])
            add(to, to, chunk_of(r2, t, REDUCE_CHUNKS[h]))
            if t < 2:
                three[h][t].start()

    def finish(h):
        from_chip(h, (2, 3))
        for t in range(2):
            three[h][t].wait_recv()
            add(*(chunk_of(ref, k, REDUCE_CHUNKS[h]) for ref, k in ((out_ref, t), (s_ref, me.order[6 + t]), (r3, t))))

    def begin():
        table = pltpu.make_async_copy(m_hbm.at[me.table], m_ref, m_sem)
        table.start()
        me.enter()
        table.wait()

    events = ((0, begin), (1, lambda: from_core(0)), (3, lambda: (from_chip(0), from_core(1))),
              (slots, lambda: (from_chip(1), from_core(2))), (slots + 2, lambda: finish(0)), (slots + 6, lambda: finish(1)),
              (slots + 10, lambda: from_chip(2)))
    for at, event in events:
        pl.when(step == at)(functools.partial(run, event))

    @pl.when(step < slots)
    def _():
        x_forward(m_ref, f_ref, s_ref, step)
        for copy in to_core(step):
            copy.start()

    @pl.when(step >= slots)
    def _():
        channel_product(first, x_ref, w_ref, p_ref.at[0], d_ref)

    @pl.when(step == last)
    def _():
        finish(2)
        for copies in [to_core(slot) for slot in range(slots)] + two + three:
            for copy in copies:
                copy.wait_send()


def gather_kernel(first, layer, m_hbm, s_ref, re_hbm, im_hbm, x_ref, w_ref, p_in, parts_ref, p_ref, m_ref, m_sem, d_ref, t_ref,
                  re_w, im_w, rows, re_rows, im_rows, re_s, im_s, re_t, im_t, w_sem, send_sem, recv_sem):
    me = Place()
    step, last = step_and_last()
    p3, q3, p2, q2, p1, q1, p0, q0 = me.order
    plan = [(p0, me.y_chip, 0), (q0, me.x_chip, 0), (p0, me.x_chip, 0), (q0, me.y_chip, 0), (p0, me.core, SUB), (q0, me.core, SUB),
            (p1, me.x_chip, 0), (q1, me.y_chip, 0)] + [(k, me.core, SUB) for k in (p1, q1, p2, q2, p3, q3)]
    copies = [[remote(chunk_of(t_ref, k, chunk), chunk_of(t_ref, k + up, chunk), send_sem.at[h, n], recv_sem.at[h, n], device)
               for n, (k, device, up) in enumerate(plan)] for h, chunk in enumerate(GATHER_CHUNKS)]
    weights = [pltpu.make_async_copy(hbm.at[layer, me.mine + k], to.at[i], w_sem.at[n, i])
               for n, (hbm, to) in enumerate(((re_hbm, re_w), (im_hbm, im_w))) for i, k in enumerate((p0, q0))]
    weights.append(pltpu.make_async_copy(m_hbm.at[me.table], m_ref, m_sem))

    def mixed(h):
        mix(s_ref, re_w, im_w, t_ref, (p0, q0), MIX_CHUNKS[h], rows, re_rows, im_rows, re_s, im_s, re_t, im_t)

    def send(h):
        for copy in copies[h][:6]:
            copy.start()

    def begin():
        for copy in weights:
            copy.start()
        me.enter()
        for copy in weights:
            copy.wait()
        mixed(0)
        send(0)

    def follow(h):
        pass_on(h)
        send(h + 1)

    def pass_on(h):
        for n in range(2):
            copies[h][n].wait_recv()
            copies[h][6 + n].start()
            copies[h][SUB + n].start()

    def finish(h):
        for n, arrived in enumerate((2, 3, 6, 7)):
            copies[h][arrived].wait_recv()
            copies[h][10 + n].start()
        for n in (4, 5, *range(SUB, len(plan))):
            copies[h][n].wait_recv()

    x_from = last + 1 - t_ref.shape[1]
    for at, event in ((0, begin), (1, lambda: mixed(1)), (5, lambda: follow(0)), (x_from, lambda: finish(0)),
                      (x_from + 1, lambda: follow(1)), (x_from + 4, lambda: finish(1)), (x_from + 5, lambda: pass_on(2)),
                      (x_from + 6, lambda: finish(2))):
        pl.when(step == at)(event)

    @pl.when((step >= 2) & (step < x_from + 4))
    def _():
        channel_product(first, x_ref, w_ref, p_ref.at[0], d_ref)

    @pl.when(step >= x_from)
    def _():
        x_inverse(m_ref, t_ref, step - x_from, parts_ref)

    @pl.when(step == last)
    def _():
        for some in copies:
            for copy in some:
                copy.wait_send()


def block(shape, index, slot=None, **kwargs):
    def index_map(*at):
        return tuple(0 if k == 'o' else slot(at[0]) if k == 's' else at['ijk'.index(k)] for k in index)
    return pl.BlockSpec(shape, index_map, **kwargs)


def point_table_kernel(w_ref, b_ref, out_ref):
    layers, width = b_ref.shape
    rows = width * SUB

    def spread(shape, axis):
        at = [lax.broadcasted_iota(jnp.int32, shape, k) for k in range(2)]
        return jnp.where(at[axis] // SUB == at[1 - axis], 1.0, 0.0).astype(BF16)
    down, across = spread((rows, width), 0), spread((width, rows), 1)
    at = [lax.broadcasted_iota(jnp.int32, (rows, rows), k) % SUB for k in range(2)]
    column = lax.broadcasted_iota(jnp.int32, (rows, out_ref.shape[-1] + CUT - 2 * rows), 1)
    for layer in range(layers):
        weights, biases = split3(HALF * w_ref[layer].T), split3(HALF * b_ref[layer:layer + 1])
        shift = sum(jnp.where(column == i, jnp.sum(down.astype(F32) * b.astype(F32), 1, keepdims=True), 0.0)
                    for i, b in enumerate(biases))
        a, b, c = (jnp.where(at[0] == at[1], dot(dot(down, w).astype(BF16), across), 0.0) for w in weights)
        none = jnp.zeros_like(a)
        for i, parts in enumerate(((a, a[:, :CUT]), (b, b[:, :CUT]), (c, none[:, :CUT]),
                                   (a[:, CUT:], a, shift), (b[:, CUT:], none, jnp.zeros_like(shift)))):
            out_ref[layer, i] = jnp.concatenate(parts, 1).astype(BF16)


def solution(mesh):
    row_devs, col_devs = mesh.shape['ys'], mesh.shape['xs']

    def local_layers(field, spec_real, spec_imag, mix_weight, bias):
        batch, x_loc, y_loc, grid_z, width = field.shape
        modes = spec_real.shape[3]
        grid_x, grid_y = x_loc * col_devs, y_loc * row_devs
        groups, blocks = x_loc // X_GROUP, y_loc // Y_BLOCK
        lanes = X_GROUP * batch
        kx, ky = kept(modes, grid_x), kept(modes, grid_y)
        n_kx, n_ky = len(kx), len(ky)
        fwd_np, inv_np = all_tables(blocks, ky, grid_y, grid_z, grid_x * grid_y * grid_z)
        fwd, inv = [jnp.asarray(t) for t in fwd_np], [jnp.asarray(t) for t in inv_np]

        turn = 2.0 * math.pi * (kx[:, None] * np.arange(grid_x)[None, :] % grid_x) / grid_x
        cos, sin = np.cos(turn), np.sin(turn)
        fwd_x = np.stack([np.stack([cos, sin], -1), np.stack([-sin, cos], -1)], 1)
        inv_x = np.transpose(fwd_x, (2, 3, 0, 1))
        fwd_x = fwd_x.reshape(n_kx, 2, col_devs, x_loc, 2).transpose(2, 0, 1, 3, 4).reshape(col_devs, 2 * n_kx, 2 * x_loc)
        inv_x = inv_x.reshape(col_devs, 2 * x_loc, 2 * n_kx)
        odd_rows = np.where(np.arange(2 * SUB * x_loc) % 2, -1.0, 1.0)[:, None]

        def x_tables(tables, axis):
            out = []
            for xs in range(col_devs):
                t = np.roll(np.kron(tables[xs], np.eye(SUB)), SUB * n_kx * (xs % 2), axis)
                out += [np.stack(pieces(t * sign)) for sign in (1.0, odd_rows)]
            return jnp.asarray(np.stack(out))
        fwd_x, inv_x = x_tables(fwd_x, 0), x_tables(inv_x, 1)
        params = pltpu.CompilerParams(vmem_limit_bytes=VMEM_LIMIT)
        point_w = pl.pallas_call(
            point_table_kernel, out_shape=jax.ShapeDtypeStruct((2, 5, width * SUB, width * SUB + CUT), BF16),
            compiler_params=params, name='point_table')(mix_weight, bias)

        real_w, imag_w = (jnp.swapaxes(w, 3, 4) for w in (spec_real, spec_imag))
        v = jnp.swapaxes(jnp.moveaxis(field, 0, -1), 2, 3)
        grid = (groups, 2, blocks)
        part_width = width // 2
        spec_shape = jax.ShapeDtypeStruct((groups, width, 256, lanes), F32)
        in_block = block((X_GROUP, Y_BLOCK, part_width, grid_z, batch), 'ikjoo')
        mid_block = block((1, Y_BLOCK, part_width, grid_z, lanes), 'ikjoo')
        part_block = block((1, ADDENDS, part_width, CLASS_ROWS[-1], lanes), 'iojoo')
        mid_shape = jax.ShapeDtypeStruct((groups, y_loc, width, grid_z, lanes), F32)
        anywhere = pl.BlockSpec(memory_space=pl.ANY)

        def stage(unit):
            return pltpu.VMEM((unit[1] // unit[0], 5, Y_BLOCK * SUB, unit[0] * lanes), F32)

        units = y_loc // HALF_BLOCK

        def unit_block(first, steps, base, count):
            shape = (HALF_BLOCK, width, grid_z) + ((batch,) if first else (lanes,))

            def index_map(j):
                n = jnp.clip(j - steps, 0, count - 1) + base
                return n // units, n % units, 0, 0, 0
            return pl.BlockSpec((X_GROUP if first else 1,) + shape, index_map)

        def table_specs(tables, index):
            return [block((1,) + t.shape[1:], index) for t in tables]

        f = pl.pallas_call(
            functools.partial(forward_kernel, FORWARD_UNIT), grid=(groups, blocks), out_shape=spec_shape,
            in_specs=[block((X_GROUP, Y_BLOCK, width, grid_z, batch), 'ijooo')] + table_specs(fwd, 'joo'),
            out_specs=block((1, width, 256, lanes), 'iooo'),
            scratch_shapes=[stage(FORWARD_UNIT)], compiler_params=params, name='forward')(v, *fwd)

        own, slots, halves = 2, SUB, n_ky // SUB
        unit = (slots, 2, n_ky, width * batch)
        own_block = block((own,) + unit, 'ooooo')

        def w_block(layer):
            return block((1,) + point_w.shape[1:], 'sooo', lambda j: layer)
        dma = pltpu.SemaphoreType.DMA
        x_scratch = [pltpu.VMEM(fwd_x.shape[1:], BF16), dma]
        half_rows = pltpu.VMEM((2, width * SUB, HALF_BLOCK * lanes), F32)

        def exchange(number):
            return pltpu.CompilerParams(vmem_limit_bytes=VMEM_LIMIT, collective_id=number, has_side_effects=True)

        def across(f, layer, source):
            first, early = layer == 0, REDUCE_UNITS[layer]
            late = groups * units - early
            s, p = pl.pallas_call(
                functools.partial(reduce_kernel, first), grid=(slots + early,),
                out_shape=(jax.ShapeDtypeStruct((own,) + unit, F32), mid_shape),
                in_specs=[anywhere,
                          block((groups, width, 1, 2, halves, SUB, lanes), 'oosoooo', lambda j: jnp.minimum(j, slots - 1)),
                          unit_block(first, slots, 0, early), w_block(layer)],
                out_specs=(own_block, unit_block(False, slots, 0, early)),
                scratch_shapes=x_scratch + [half_rows] + [pltpu.VMEM((n,) + unit, F32) for n in (n_kx, SUB, 4, 2)]
                + [dma((slots, SUB))] * 2 + [dma((len(REDUCE_CHUNKS), n)) for n in (4, 4, 2, 2)],
                compiler_params=exchange(2 * layer), name='reduce')(
                    fwd_x, f.reshape(groups, width, slots, 2, halves, SUB, lanes), source, point_w)
            parts, p = pl.pallas_call(
                functools.partial(gather_kernel, first, layer), grid=(late + 6,),
                out_shape=(jax.ShapeDtypeStruct((groups, ADDENDS, width, slots, 2, halves, SUB, lanes), BF16), mid_shape),
                in_specs=[anywhere, own_block, anywhere, anywhere, unit_block(first, 2, early, late), w_block(layer), anywhere],
                out_specs=(block((groups, ADDENDS, width, 1, 2, halves, SUB, lanes), 'ooosoooo', lambda j: jnp.maximum(j - late + 2, 0)),
                           unit_block(False, 2, early, late)),
                input_output_aliases={6: 1},
                scratch_shapes=x_scratch + [half_rows, pltpu.VMEM((n_kx,) + unit, F32)]
                + [pltpu.VMEM((own, n_ky, width, SUB, width), F32)] * 2
                + [pltpu.VMEM((own * n_ky * SUB, LANES), F32)] + [pltpu.VMEM((width, 24, LANES), F32)] * 2
                + [pltpu.VMEM((width * batch, LANES), F32)] * 4
                + [dma((2, 2))] + [dma((len(GATHER_CHUNKS), 14))] * 2,
                compiler_params=exchange(2 * layer + 1), name='gather')(
                    inv_x, s, real_w, imag_w, source, point_w, p)
            return parts.reshape(groups, ADDENDS, width, CLASS_ROWS[-1], lanes), p

        parts, p = across(f, 0, v)
        v1, f = pl.pallas_call(
            functools.partial(layer_kernel, FIRST_UNIT, True), grid=grid, out_shape=(mid_shape, spec_shape),
            in_specs=[mid_block, part_block] + table_specs(inv + fwd, 'koo'),
            out_specs=(mid_block, anywhere),
            scratch_shapes=[stage(FIRST_UNIT)] * 2 + [pltpu.VMEM(spec_shape.shape, F32), pltpu.SemaphoreType.DMA((groups,))],
            compiler_params=params, name='layer_first')(p, parts, *inv, *fwd)
        parts, p = across(f, 1, v1)
        out = pl.pallas_call(
            functools.partial(layer_kernel, LAST_UNIT, False), grid=grid,
            out_shape=jax.ShapeDtypeStruct((x_loc, y_loc, width, grid_z, batch), F32),
            in_specs=[mid_block, part_block] + table_specs(inv, 'koo'), out_specs=in_block, scratch_shapes=[stage(LAST_UNIT)],
            compiler_params=params, name='layer_last')(p, parts, *inv)
        return jnp.moveaxis(jnp.swapaxes(out, 2, 3), -1, 0)

    field_spec = P('data', 'xs', 'ys', None, None)
    return jax.shard_map(local_layers, mesh=mesh, in_specs=(field_spec, P(), P(), P(), P()), out_specs=field_spec, check_vma=False)
```

```python
import functools
import math

import jax
import jax.numpy as jnp
import ml_dtypes
import numpy as np
from jax import lax
from jax.experimental import pallas as pl
from jax.experimental.pallas import tpu as pltpu
from jax.sharding import PartitionSpec as P

F32 = jnp.float32
BF16 = jnp.bfloat16
VMEM_LIMIT = 64 * 1024 * 1024 - 65536

SUB = 8
X_GROUP = 8
Y_BLOCK = 4
HALF_BLOCK = 2
Z_BLOCK = 8
KZ_CLASS = ((0, 5), (1, 6, 4), (2, 7, 3))
KZ_ORDER = tuple(kz for group in KZ_CLASS for kz in group)
CLASS_ROWS = (0, 64, 160, 256)
LANES = 128
ADDENDS = 3
CUT = 96
HALF = 0.5
REDUCE_UNITS = 22
REDUCE_CHUNKS = ((0, 2), (2, 6), (6, 8))
GATHER_CHUNKS = ((0, 4), (4, 6), (6, 8))
MIX_CHUNKS = ((0, 4), (4, 8))
FORWARD_UNIT = (2, 20)
FIRST_UNIT = (2, 10)
LAST_UNIT = (1, 10)
ROOT5_4 = math.sqrt(5.0) / 4.0
SIN_1 = math.sin(2.0 * math.pi / 5.0)
SIN_RATIO = math.sin(4.0 * math.pi / 5.0) / SIN_1


def kz_sign(kz):
    return 0 if kz % 5 == 0 else (1 if kz % 5 < 3 else -1)


def kept(modes, size):
    return np.concatenate([np.arange(modes), np.arange(size - modes, size)])


def pieces(table):
    rest = np.asarray(table, np.float32)
    out = []
    for _ in range(ADDENDS):
        out.append(rest.astype(ml_dtypes.bfloat16))
        rest = rest - out[-1].astype(np.float32)
    return out


def yz_angles(kz, y_pos, ky, grid_y, grid_z):
    z_pos = np.arange(Z_BLOCK)
    turn = (ky[:, None, None] * y_pos[None, :, None] % grid_y) / grid_y + kz * z_pos[None, None, :] / grid_z
    return 2.0 * math.pi * turn


def forward_table(group, y_pos, ky, grid_y, grid_z):
    rows = []
    for kz in group:
        t, s = yz_angles(kz, y_pos, ky, grid_y, grid_z), kz_sign(kz)
        real, imag = [np.cos(t)], [-np.sin(t)]
        if s:
            real.append(-s * SIN_1 * np.sin(t))
            imag.append(-s * SIN_1 * np.cos(t))
        rows += [np.stack(part, 1).reshape(len(ky), -1) for part in (real, imag)]
    return np.concatenate(rows, 0)


def inverse_table(group, y_pos, ky, grid_y, grid_z, points):
    cols = []
    for kz in group:
        t, s = yz_angles(kz, y_pos, ky, grid_y, grid_z).transpose(1, 2, 0), kz_sign(kz)
        w = (HALF if kz == 0 else 1.0) / points
        real, imag = [w * np.cos(t)], [-w * np.sin(t)]
        if s:
            real.append(s * SIN_1 * w * np.sin(t))
            imag.append(s * SIN_1 * w * np.cos(t))
        cols += [np.stack(part, 0).reshape(-1, len(ky)) for part in (real, imag)]
    return np.concatenate(cols, 1)


def all_tables(blocks, ky, grid_y, grid_z, points):
    fwd, inv = [[], [], []], [[], [], [], [], []]
    for block in range(blocks):
        y_pos = np.arange(Y_BLOCK) + block * Y_BLOCK
        for k, group in enumerate(KZ_CLASS):
            a, b, c = pieces(forward_table(group, y_pos, ky, grid_y, grid_z))
            n = np.zeros_like(a)
            if k == 0:
                fwd[k].append(np.concatenate([a, a, a, b, b, c], 1))
            else:
                fwd[k].append(np.block([[a, a, a, b], [c, b, n, n]]))
            a, b, c = pieces(inverse_table(group, y_pos, ky, grid_y, grid_z, points))
            n = np.zeros_like(a)
            if k == 0:
                inv[0].append(np.block([[a, a, a], [b, b, n], [c, n, n]]))
            else:
                inv[2 * k - 1].append(np.block([[a, a], [b, b]]))
                inv[2 * k].append(np.concatenate([c, a], 1))
    return [np.stack(t) for t in fwd], [np.stack(t) for t in inv]


def split3(v):
    d1 = v.astype(BF16)
    rest = v - d1.astype(F32)
    d2 = rest.astype(BF16)
    return d1, d2, (rest - d2.astype(F32)).astype(BF16)


def dot(a, b):
    return jnp.dot(a, b, preferred_element_type=F32)


def z_forward(v):
    v0, v1, v2, v3, v4 = v
    t1, t2, e1, e2 = v1 + v4, v2 + v3, v1 - v4, v2 - v3
    total = t1 + t2
    mid, dif = v0 - 0.25 * total, ROOT5_4 * (t1 - t2)
    return v0 + total, mid + dif, e1 + SIN_RATIO * e2, mid - dif, SIN_RATIO * e1 - e2


def z_inverse(a0, a1, b1, a2, b2):
    total = a1 + a2
    mid, dif = a0 - 0.25 * total, ROOT5_4 * (a1 - a2)
    p, q = mid + dif, mid - dif
    r, s = b1 + SIN_RATIO * b2, SIN_RATIO * b1 - b2
    return a0 + total, p - r, q - s, q + s, p + r


def split_tiles(u_ref, channels):
    rows, lanes = u_ref.shape[1:]
    out = [[], [], []]
    for k in channels:
        for r in range(0, rows, 2 * SUB):
            cells = [split3(u_ref[k, r:r + 2 * SUB, lane:lane + LANES]) for lane in range(0, lanes, LANES)]
            for i in range(ADDENDS):
                out[i].append(jnp.concatenate([cell[i] for cell in cells], -1))
    return [jnp.concatenate(rows, 0) for rows in out]


def add_tiles(o, n, lanes, first=0):
    for r in range(0, n, SUB):
        for lane in range(0, lanes, LANES):
            cells = [o[b + r:b + r + SUB, lane:lane + LANES] for b in range(0, o.shape[0], n)]
            yield r, lane, functools.reduce(jnp.add, cells)


def forward_stage(u_ref, tables, f_ref, c, pair):
    lanes = f_ref.shape[-1]
    for k, channels in enumerate(((0,), (1, 2), (3, 4))):
        d = split_tiles(u_ref, channels)
        o = dot(tables[k], jnp.concatenate([d[i] for i in ((0, 1, 2, 0) if k else (0, 1, 2, 0, 1, 0))], 0))
        n = CLASS_ROWS[k + 1] - CLASS_ROWS[k]
        for r, lane, v in add_tiles(o, n, pair * lanes):
            at = (c + lane // lanes, slice(CLASS_ROWS[k] + r, CLASS_ROWS[k] + r + SUB), slice(lane % lanes, lane % lanes + LANES))
            f_ref[at] += v


def inverse_stage(s_ref, c, pair, tables, u_ref):
    n, lanes = u_ref.shape[1:]

    def part(i, k):
        return jnp.concatenate([s_ref[0, i, c + u, CLASS_ROWS[k]:CLASS_ROWS[k + 1]] for u in range(pair)], -1)
    o = dot(tables[0], jnp.concatenate([part(i, 0) for i in range(ADDENDS)], 0))
    for r, lane, v in add_tiles(o, n, lanes):
        u_ref[0, r:r + SUB, lane:lane + LANES] = v
    for k in (1, 2):
        d1, d2, d3 = (part(i, k) for i in range(ADDENDS))
        o = jnp.concatenate([dot(tables[2 * k - 1], jnp.concatenate([d1, d2], 0)),
                             dot(tables[2 * k], jnp.concatenate([d1, d3], 0))], 0)
        for r, lane, v in add_tiles(o, 2 * n, lanes):
            u_ref[2 * k - 1 + r // n, r % n:r % n + SUB, lane:lane + LANES] = v


def registers(pair, lanes):
    for u in range(pair):
        for y in range(Y_BLOCK):
            for lane in range(0, lanes, LANES):
                yield u, y, lane, (slice(y * SUB, (y + 1) * SUB), slice(u * lanes + lane, u * lanes + lane + LANES))


def gelu(h):
    k = 2.0 * math.sqrt(2.0 / math.pi)
    return h + h * jnp.tanh(h * (k + (4.0 * 0.044715 * k) * (h * h)))


def field_lanes(x_ref, y, c):
    return jnp.concatenate([x_ref[x, y, c] for x in range(X_GROUP)], -1)


def zero_spectrum(f_ref):
    def clear(c, _):
        f_ref[c] = jnp.zeros(f_ref.shape[1:], F32)
        return 0
    lax.fori_loop(0, f_ref.shape[0], clear, 0)


def forward_kernel(unit, x_ref, t0, t1, t2, f_ref, u_ref):
    f_ref = f_ref.at[0]
    width, lanes = x_ref.shape[2], f_ref.shape[-1]
    pair, per_step = unit
    tables = (t0[0], t1[0], t2[0])

    @pl.when(pl.program_id(1) == 0)
    def _():
        zero_spectrum(f_ref)

    def load(c, slot):
        for u in range(pair):
            for y in range(Y_BLOCK):
                row = field_lanes(x_ref, y, c + u)
                for k, v in enumerate(z_forward([row[SUB * j:SUB * j + SUB] for j in range(5)])):
                    u_ref[slot, k, y * SUB:(y + 1) * SUB, u * lanes:(u + 1) * lanes] = v

    def body(i, _):
        c = i * per_step
        count = per_step // pair
        for n in range(count + 1):
            if n < count:
                load(c + n * pair, n)
            if n:
                forward_stage(u_ref.at[n - 1], tables, f_ref, c + (n - 1) * pair, pair)
        return 0
    lax.fori_loop(0, width // per_step, body, 0)


def channel_product(first, x_ref, w_ref, p_ref, d_ref):
    blocks, width, depth, lanes = p_ref.shape
    rows = width * SUB
    ones = jnp.ones((w_ref.shape[-1] + CUT - 2 * rows, blocks * lanes), BF16)
    left = [w_ref[0, i] for i in range(w_ref.shape[1])]

    def load(j):
        z = slice(j * SUB, (j + 1) * SUB)
        if first:
            v = [x_ref[x, y, :, z, :] for y in range(blocks) for x in range(X_GROUP)]
        else:
            v = [x_ref[0, y, :, z, :] for y in range(blocks)]
        d_ref[j % 2] = jnp.concatenate(v, -1).reshape(rows, blocks * lanes)

    def product(j):
        d1, d2, d3 = split3(d_ref[j % 2])
        low, high = jnp.concatenate([d1, d2[:CUT]], 0), jnp.concatenate([d2[CUT:], d3, ones], 0)
        p = functools.reduce(jnp.add, [dot(w, low if i < ADDENDS else high) for i, w in enumerate(left)])
        for y in range(blocks):
            p_ref[y, :, j * SUB:(j + 1) * SUB, :] = p[:, y * lanes:(y + 1) * lanes].reshape(width, SUB, lanes)
    count = depth // SUB
    for j in range(count + 1):
        if j < count:
            load(j)
        if j:
            product(j - 1)


def layer_kernel(unit, first, *refs):
    p_ref, s_ref, *tabs = refs
    p_ref = p_ref.at[0]
    width, lanes = p_ref.shape[1], p_ref.shape[-1]
    batch = lanes // X_GROUP
    if first:
        start = pl.program_id(1) * width
        *tabs, v_ref, f_hbm, a_ref, u_ref, f_all, f_sem = tabs
        v_ref = v_ref.at[0]
        group = pl.program_id(0)
        f_ref = f_all.at[group, pl.ds(start, width)]

        @pl.when(pl.program_id(2) == 0)
        def _():
            zero_spectrum(f_ref)
    else:
        start = pl.program_id(2) * width
        *tabs, o_ref, a_ref = tabs
    inv, fwd = [t[0] for t in tabs[:5]], [t[0] for t in tabs[5:]]
    pair, per_step = unit

    def activate(c, slot):
        kept_rows = {}
        for u, y, lane, at in registers(pair, lanes):
            new = []
            for j, s in enumerate(z_inverse(*(a_ref[(slot, k) + at] for k in range(5)))):
                g = gelu(s + p_ref[y, c + u, SUB * j:SUB * j + SUB, lane:lane + LANES])
                new.append(g)
                if first:
                    v_ref[y, c + u, SUB * j:SUB * j + SUB, lane:lane + LANES] = g
                else:
                    kept_rows[j] = kept_rows.get(j, ()) + (g,)
            if first:
                for k, v in enumerate(z_forward(new)):
                    u_ref[(slot, k) + at] = v
            elif lane + LANES == lanes:
                for j, row in kept_rows.items():
                    store_field(o_ref, y, c + u, SUB * j, row, batch)
                kept_rows = {}

    def body(i, _):
        c = i * per_step
        count = per_step // pair
        for n in range(count + 2):
            if n < count:
                inverse_stage(s_ref, (0 if first else start) + c + n * pair, pair, inv, a_ref.at[n])
            if 0 < n <= count:
                activate(c + (n - 1) * pair, n - 1)
            if first and n > 1:
                forward_stage(u_ref.at[n - 2], fwd, f_ref, c + (n - 2) * pair, pair)
        return 0
    lax.fori_loop(0, width // per_step, body, 0)

    if first:
        @pl.when((pl.program_id(2) == pl.num_programs(2) - 1) & (start > 0))
        def _():
            copies = [pltpu.make_async_copy(f_all.at[g], f_hbm.at[g], f_sem.at[g]) for g in range(f_all.shape[0])]
            for g, copy in enumerate(copies):
                pl.when(group == g)(copy.start)

            @pl.when(group == len(copies) - 1)
            def _():
                for copy in copies:
                    copy.wait()


def store_field(o_ref, y, c, z, row, batch):
    lane = lax.broadcasted_iota(jnp.int32, row[0].shape, 1)
    for x in range(X_GROUP):
        at, off = divmod(x * batch, LANES)
        piece = row[at]
        if off + batch > LANES:
            piece = jnp.where(lane < off, row[at + 1], piece)
        if off:
            piece = pltpu.roll(piece, LANES - off, 1)
        o_ref[x, y, c, z:z + SUB, :] = piece[:, :batch]


def split_dot(left, right):
    a, b, c = left
    d1, d2, d3 = split3(right)
    return dot(a, d1) + dot(a, d2) + dot(a, d3) + dot(b, d1) + dot(b, d2) + dot(c, d1)


def x_forward(m_ref, f_ref, s_ref, slot):
    groups, width, lanes = f_ref.shape[0], f_ref.shape[1], f_ref.shape[-1]
    batch = lanes // X_GROUP
    halves = range(f_ref.shape[4])
    rights = []
    for h in halves:
        rows = []
        for g in range(groups):
            for x in range(X_GROUP):
                for p in range(2):
                    rows.append(jnp.concatenate([f_ref[g, c, 0, p, h, :, x * batch:(x + 1) * batch] for c in range(width)], -1))
        rights.append(jnp.concatenate(rows, 0))
    for h in halves:
        out = split_dot((m_ref[0], m_ref[1], m_ref[2]), rights[h])
        s_ref[:, slot, :, h * SUB:(h + 1) * SUB, :] = out.reshape(s_ref.shape[0], 2, SUB, width * batch)


def x_inverse(m_ref, t_ref, slot, s_ref):
    groups, width, lanes = s_ref.shape[0], s_ref.shape[2], s_ref.shape[-1]
    batch = lanes // X_GROUP
    halves = range(s_ref.shape[5])
    outs = []
    for h in halves:
        right = t_ref[:, slot, :, h * SUB:(h + 1) * SUB, :].reshape(t_ref.shape[0] * 2 * SUB, width * batch)
        outs.append(split_dot((m_ref[0], m_ref[1], m_ref[2]), right).reshape(groups, X_GROUP, 2, SUB, width * batch))
    for h in halves:
        for g in range(groups):
            for p in range(2):
                for c in range(width):
                    row = jnp.concatenate([outs[h][g, x, p, :, c * batch:(c + 1) * batch] for x in range(X_GROUP)], -1)
                    for i, d in enumerate(split3(row)):
                        s_ref[g, i, c, 0, p, h] = d


def mix(s_ref, re_w, im_w, t_ref, to, chunk, rows, re_rows, im_rows, re_s, im_s, re_t, im_t):
    own, _, _, n_ky, lanes = s_ref.shape
    width = re_w.shape[2]
    batch = lanes // width
    some = chunk[1] - chunk[0]
    part_modes = some * n_ky
    pick, modes = slice(*chunk), slice(0, own * part_modes)

    for w_ref, out in ((re_w, re_rows), (im_w, im_rows)):
        def lay(c, _):
            for k in range(own):
                for ky in range(n_ky):
                    at = (k * n_ky + ky) * SUB
                    rows[at:at + SUB, 0:width] = w_ref[k, ky, c]
            mat = jnp.concatenate([rows[pl.ds((k * n_ky + h * SUB) * SUB + kz, SUB, stride=SUB), :]
                                   for k in range(own) for kz in KZ_ORDER[pick] for h in range(n_ky // SUB)], 0)
            out[c, :, modes] = mat.T[0:out.shape[1]]
            return 0
        lax.fori_loop(0, width, lay, 0)
    for p, out in enumerate((re_s, im_s)):
        out[:, modes] = jnp.concatenate([s_ref[k, pick, p].reshape(part_modes, lanes) for k in range(own)], 0).T
    pair = 1

    def outputs(i, _):
        d = i * pair

        def inner(c, acc):
            at = pl.ds(pl.multiple_of(c * batch, SUB), batch)
            a, b = re_s[at, modes], im_s[at, modes]
            new = []
            for u in range(pair):
                p = jnp.broadcast_to(re_rows[c, pl.ds(d + u, 1), modes], a.shape)
                q = jnp.broadcast_to(im_rows[c, pl.ds(d + u, 1), modes], a.shape)
                new += [acc[2 * u] + (a * p - b * q), acc[2 * u + 1] + (a * q + b * p)]
            return tuple(new)
        zero = jnp.zeros((batch, own * part_modes), F32)
        acc = lax.fori_loop(0, width, inner, (zero,) * (2 * pair), unroll=True)
        for u in range(pair):
            at = pl.ds(pl.multiple_of((d + u) * batch, SUB), batch)
            re_t[at, modes] = acc[2 * u]
            im_t[at, modes] = acc[2 * u + 1]
        return 0
    lax.fori_loop(0, width // pair, outputs, 0)
    for p, got in enumerate((re_t, im_t)):
        back = got[:, modes].T
        for k in range(own):
            t_ref[to[k], pick, p] = back[k * part_modes:(k + 1) * part_modes].reshape(some, n_ky, lanes)


class Place:
    def __init__(self):
        xs, ys = lax.axis_index('xs'), lax.axis_index('ys')
        data = lax.axis_index('data')
        c, x, y = xs % 2, xs // 2, ys
        self.core = (data, ys, 2 * x + 1 - c)
        self.x_chip = (data, ys, 2 * (1 - x) + c)
        self.y_chip = (data, 1 - ys, xs)
        p, q = lambda a, b: 2 * a + b, lambda a, b: 4 + 2 * a + b
        self.mine = SUB * c
        self.table = 2 * xs + ys
        self.order = (p(1 - x, 1 - y), q(1 - y, 1 - x), p(1 - x, y), q(1 - y, x),
                      p(x, 1 - y), q(y, 1 - x), p(x, y), q(y, x))

    def enter(self):
        barrier = pltpu.get_barrier_semaphore()
        for device in (self.core, self.x_chip, self.y_chip):
            pl.semaphore_signal(barrier, inc=1, device_id=device, device_id_type=pl.DeviceIdType.MESH)
        pl.semaphore_wait(barrier, 3)


def remote(src, dst, send, recv, device):
    return pltpu.make_async_remote_copy(src_ref=src, dst_ref=dst, send_sem=send, recv_sem=recv, device_id=device,
                                        device_id_type=pl.DeviceIdType.MESH)


def step_and_last():
    return pl.program_id(0), pl.num_programs(0) - 1


def chunk_of(ref, k, chunk):
    low, high = chunk
    return ref.at[k, pl.ds(low, high - low)]


def reduce_kernel(first, m_hbm, f_ref, x_ref, w_ref, out_ref, p_ref, m_ref, m_sem, d_ref, s_ref, r1, r2, r3,
                  send1, recv1, send2, recv2, send3, recv3):
    me = Place()
    step, last = step_and_last()
    slots = s_ref.shape[1]
    two, three = [], []

    def to_core(slot):
        return [remote(s_ref.at[SUB + me.order[t], slot], r1.at[t, slot], send1.at[slot, t], recv1.at[slot, t], me.core)
                for t in range(SUB)]
    for h, chunk in enumerate(REDUCE_CHUNKS):
        mine = [chunk_of(s_ref, k, chunk) for k in me.order]
        two.append([remote(mine[t], chunk_of(r2, t, chunk), send2.at[h, t], recv2.at[h, t], (me.x_chip, me.y_chip)[t % 2])
                    for t in range(4)])
        three.append([remote(mine[4 + t], chunk_of(r3, t, chunk), send3.at[h, t], recv3.at[h, t], (me.y_chip, me.x_chip)[t])
                      for t in range(2)])

    def add(dst, a, b):
        def row(i, _):
            dst[i] = a[i] + b[i]
            return 0
        lax.fori_loop(0, dst.shape[0], row, 0)

    def from_core(h):
        arriving = [to_core(slot) for slot in range(*REDUCE_CHUNKS[h])]
        for t in range(SUB):
            for copies in arriving:
                copies[t].wait_recv()
            to = chunk_of(s_ref, me.order[t], REDUCE_CHUNKS[h])
            add(to, to, chunk_of(r1, t, REDUCE_CHUNKS[h]))
            if t < len(two[h]):
                two[h][t].start()

    def from_chip(h, these=(0, 1)):
        for t in these:
            two[h][t].wait_recv()
            to = chunk_of(s_ref, me.order[4 + t], REDUCE_CHUNKS[h])
            add(to, to, chunk_of(r2, t, REDUCE_CHUNKS[h]))
            if t < len(three[h]):
                three[h][t].start()

    def finish(h):
        from_chip(h, (2, 3))
        for t in range(2):
            three[h][t].wait_recv()
            add(*(chunk_of(ref, k, REDUCE_CHUNKS[h]) for ref, k in ((out_ref, t), (s_ref, me.order[6 + t]), (r3, t))))

    def begin():
        table = pltpu.make_async_copy(m_hbm.at[me.table], m_ref, m_sem)
        table.start()
        me.enter()
        table.wait()

    events = ((0, begin), (2, lambda: from_core(0)), (slots - 3, lambda: from_chip(0)), (slots - 2, lambda: from_core(1)),
              (slots, lambda: from_core(2)), (slots + 3, lambda: finish(0)), (slots + 5, lambda: from_chip(1)),
              (slots + 12, lambda: from_chip(2)))
    for at, event in events:
        pl.when(step == at)(event)

    @pl.when(step < slots)
    def _():
        x_forward(m_ref, f_ref, s_ref, step)
        for copy in to_core(step):
            copy.start()

    @pl.when(step >= slots)
    def _():
        channel_product(first, x_ref, w_ref, p_ref.at[0], d_ref)

    @pl.when(step == last)
    def _():
        finish(1)
        finish(2)
        for copies in [to_core(slot) for slot in range(slots)] + two + three:
            for copy in copies:
                copy.wait_send()


def gather_kernel(first, layer, m_hbm, s_ref, re_hbm, im_hbm, x_ref, w_ref, p_in, parts_ref, p_ref, m_ref, m_sem, d_ref, t_ref,
                  re_w, im_w, rows, re_rows, im_rows, re_s, im_s, re_t, im_t, w_sem, send_sem, recv_sem):
    me = Place()
    step, last = step_and_last()
    p3, q3, p2, q2, p1, q1, p0, q0 = me.order
    plan = [(p0, me.y_chip, 0), (q0, me.x_chip, 0), (p0, me.x_chip, 0), (q0, me.y_chip, 0), (p0, me.core, SUB), (q0, me.core, SUB),
            (p1, me.x_chip, 0), (q1, me.y_chip, 0)] + [(k, me.core, SUB) for k in (p1, q1, p2, q2, p3, q3)]
    copies = [[remote(chunk_of(t_ref, k, chunk), chunk_of(t_ref, k + up, chunk), send_sem.at[h, n], recv_sem.at[h, n], device)
               for n, (k, device, up) in enumerate(plan)] for h, chunk in enumerate(GATHER_CHUNKS)]
    weights = [pltpu.make_async_copy(hbm.at[layer, me.mine + k], to.at[i], w_sem.at[n, i])
               for n, (hbm, to) in enumerate(((re_hbm, re_w), (im_hbm, im_w))) for i, k in enumerate((p0, q0))]
    weights.append(pltpu.make_async_copy(m_hbm.at[me.table], m_ref, m_sem))

    def mixed(h):
        mix(s_ref, re_w, im_w, t_ref, (p0, q0), MIX_CHUNKS[h], rows, re_rows, im_rows, re_s, im_s, re_t, im_t)

    def send(h):
        for copy in copies[h][:6]:
            copy.start()

    def begin():
        for copy in weights:
            copy.start()
        me.enter()
        for copy in weights:
            copy.wait()
        mixed(0)
        send(0)

    def follow(h):
        pass_on(h)
        send(h + 1)

    def pass_on(h):
        for n in range(2):
            copies[h][n].wait_recv()
            copies[h][6 + n].start()
            copies[h][SUB + n].start()

    def finish(h):
        for n, arrived in enumerate((2, 3, 6, 7)):
            copies[h][arrived].wait_recv()
            copies[h][10 + n].start()
        for n in (4, 5, *range(SUB, len(plan))):
            copies[h][n].wait_recv()

    x_from = last + 1 - t_ref.shape[1]
    for at, event in ((0, begin), (1, lambda: mixed(1)), (5, lambda: follow(0)), (x_from, lambda: finish(0)),
                      (x_from + 1, lambda: follow(1)), (x_from + 4, lambda: finish(1)), (x_from + 5, lambda: pass_on(2)),
                      (x_from + 6, lambda: finish(2))):
        pl.when(step == at)(event)

    @pl.when((step >= 2) & (step < x_from + 4))
    def _():
        channel_product(first, x_ref, w_ref, p_ref.at[0], d_ref)

    @pl.when(step >= x_from)
    def _():
        x_inverse(m_ref, t_ref, step - x_from, parts_ref)

    @pl.when(step == last)
    def _():
        for some in copies:
            for copy in some:
                copy.wait_send()


def block(shape, index, slot=None, **kwargs):
    def index_map(*at):
        return tuple(0 if k == 'o' else slot(at[0]) if k == 's' else at['ijk'.index(k)] for k in index)
    return pl.BlockSpec(shape, index_map, **kwargs)


def point_table_kernel(w_ref, b_ref, out_ref):
    layers, width = b_ref.shape
    rows = width * SUB

    def spread(shape, axis):
        at = [lax.broadcasted_iota(jnp.int32, shape, k) for k in range(2)]
        return jnp.where(at[axis] // SUB == at[1 - axis], 1.0, 0.0).astype(BF16)
    down, across = spread((rows, width), 0), spread((width, rows), 1)
    at = [lax.broadcasted_iota(jnp.int32, (rows, rows), k) % SUB for k in range(2)]
    column = lax.broadcasted_iota(jnp.int32, (rows, out_ref.shape[-1] + CUT - 2 * rows), 1)
    for layer in range(layers):
        weights, biases = split3(HALF * w_ref[layer].T), split3(HALF * b_ref[layer:layer + 1])
        shift = sum(jnp.where(column == i, jnp.sum(down.astype(F32) * b.astype(F32), 1, keepdims=True), 0.0)
                    for i, b in enumerate(biases))
        a, b, c = (jnp.where(at[0] == at[1], dot(dot(down, w).astype(BF16), across), 0.0) for w in weights)
        none = jnp.zeros_like(a)
        for i, parts in enumerate(((a, a[:, :CUT]), (b, b[:, :CUT]), (c, none[:, :CUT]),
                                   (a[:, CUT:], a, shift), (b[:, CUT:], none, jnp.zeros_like(shift)))):
            out_ref[layer, i] = jnp.concatenate(parts, 1).astype(BF16)


def solution(mesh):
    row_devs, col_devs = mesh.shape['ys'], mesh.shape['xs']

    def local_layers(field, spec_real, spec_imag, mix_weight, bias):
        batch, x_loc, y_loc, grid_z, width = field.shape
        modes = spec_real.shape[3]
        grid_x, grid_y = x_loc * col_devs, y_loc * row_devs
        groups, blocks = x_loc // X_GROUP, y_loc // Y_BLOCK
        lanes = X_GROUP * batch
        kx, ky = kept(modes, grid_x), kept(modes, grid_y)
        n_kx, n_ky = len(kx), len(ky)
        fwd_np, inv_np = all_tables(blocks, ky, grid_y, grid_z, grid_x * grid_y * grid_z)
        fwd, inv = [jnp.asarray(t) for t in fwd_np], [jnp.asarray(t) for t in inv_np]

        turn = 2.0 * math.pi * (kx[:, None] * np.arange(grid_x)[None, :] % grid_x) / grid_x
        cos, sin = np.cos(turn), np.sin(turn)
        fwd_x = np.stack([np.stack([cos, sin], -1), np.stack([-sin, cos], -1)], 1)
        inv_x = np.transpose(fwd_x, (2, 3, 0, 1))
        fwd_x = fwd_x.reshape(n_kx, 2, col_devs, x_loc, 2).transpose(2, 0, 1, 3, 4).reshape(col_devs, 2 * n_kx, 2 * x_loc)
        inv_x = inv_x.reshape(col_devs, 2 * x_loc, 2 * n_kx)
        odd_rows = np.where(np.arange(2 * SUB * x_loc) % 2, -1.0, 1.0)[:, None]

        def x_tables(tables, axis):
            out = []
            for xs in range(col_devs):
                t = np.roll(np.kron(tables[xs], np.eye(SUB)), SUB * n_kx * (xs % 2), axis)
                out += [np.stack(pieces(t * sign)) for sign in (1.0, odd_rows)]
            return jnp.asarray(np.stack(out))
        fwd_x, inv_x = x_tables(fwd_x, 0), x_tables(inv_x, 1)
        params = pltpu.CompilerParams(vmem_limit_bytes=VMEM_LIMIT)
        point_w = pl.pallas_call(
            point_table_kernel, out_shape=jax.ShapeDtypeStruct((2, 5, width * SUB, width * SUB + CUT), BF16),
            compiler_params=params, name='point_table')(mix_weight, bias)

        real_w, imag_w = (jnp.swapaxes(w, 3, 4) for w in (spec_real, spec_imag))
        v = jnp.swapaxes(jnp.moveaxis(field, 0, -1), 2, 3)
        grid = (groups, 2, blocks)
        part_width = width // 2
        spec_shape = jax.ShapeDtypeStruct((groups, width, 256, lanes), F32)
        mid_block = block((1, Y_BLOCK, part_width, grid_z, lanes), 'ikjoo')
        part_block = block((1, ADDENDS, part_width, CLASS_ROWS[-1], lanes), 'iojoo')
        mid_shape = jax.ShapeDtypeStruct((groups, y_loc, width, grid_z, lanes), F32)
        anywhere = pl.BlockSpec(memory_space=pl.ANY)

        def stage(unit):
            return pltpu.VMEM((unit[1] // unit[0], 5, Y_BLOCK * SUB, unit[0] * lanes), F32)

        units = y_loc // HALF_BLOCK

        def unit_block(first, steps, base, count):
            shape = (HALF_BLOCK, width, grid_z) + ((batch,) if first else (lanes,))

            def index_map(j):
                n = jnp.clip(j - steps, 0, count - 1) + base
                return n // units, n % units, *(0,) * len(shape[1:])
            return pl.BlockSpec((X_GROUP if first else 1,) + shape, index_map)

        def table_specs(tables, index):
            return [block((1,) + t.shape[1:], index) for t in tables]

        f = pl.pallas_call(
            functools.partial(forward_kernel, FORWARD_UNIT), grid=(groups, blocks), out_shape=spec_shape,
            in_specs=[block((X_GROUP, Y_BLOCK, width, grid_z, batch), 'ijooo')] + table_specs(fwd, 'joo'),
            out_specs=block((1, width, 256, lanes), 'iooo'),
            scratch_shapes=[stage(FORWARD_UNIT)], compiler_params=params, name='forward')(v, *fwd)

        own, slots, halves = 2, SUB, n_ky // SUB
        unit = (slots, 2, n_ky, width * batch)
        own_block = block((own,) + unit, 'ooooo')

        def w_block(layer):
            return block((1,) + point_w.shape[1:], 'sooo', lambda j: layer)
        dma = pltpu.SemaphoreType.DMA
        x_scratch = [pltpu.VMEM(fwd_x.shape[1:], BF16), dma]
        half_rows = pltpu.VMEM((2, width * SUB, HALF_BLOCK * lanes), F32)

        def exchange(number):
            return pltpu.CompilerParams(vmem_limit_bytes=VMEM_LIMIT, collective_id=number, has_side_effects=True)

        def across(f, layer, source):
            first, early = layer == 0, REDUCE_UNITS
            late = groups * units - early
            s, p = pl.pallas_call(
                functools.partial(reduce_kernel, first), grid=(slots + early,),
                out_shape=(jax.ShapeDtypeStruct((own,) + unit, F32), mid_shape),
                in_specs=[anywhere,
                          block((groups, width, 1, 2, halves, SUB, lanes), 'oosoooo', lambda j: jnp.minimum(j, slots - 1)),
                          unit_block(first, slots, 0, early), w_block(layer)],
                out_specs=(own_block, unit_block(False, slots, 0, early)),
                scratch_shapes=x_scratch + [half_rows] + [pltpu.VMEM((n,) + unit, F32) for n in (n_kx, SUB, 4, 2)]
                + [dma((slots, SUB))] * 2 + [dma((len(REDUCE_CHUNKS), n)) for n in (4, 4, 2, 2)],
                compiler_params=exchange(2 * layer), name='reduce')(
                    fwd_x, f.reshape(groups, width, slots, 2, halves, SUB, lanes), source, point_w)
            parts, p = pl.pallas_call(
                functools.partial(gather_kernel, first, layer), grid=(late + 6,),
                out_shape=(jax.ShapeDtypeStruct((groups, ADDENDS, width, slots, 2, halves, SUB, lanes), BF16), mid_shape),
                in_specs=[anywhere, own_block, anywhere, anywhere, unit_block(first, 2, early, late), w_block(layer), anywhere],
                out_specs=(block((groups, ADDENDS, width, 1, 2, halves, SUB, lanes), 'ooosoooo', lambda j: jnp.maximum(j - late + 2, 0)),
                           unit_block(False, 2, early, late)),
                input_output_aliases={6: 1},
                scratch_shapes=x_scratch + [half_rows, pltpu.VMEM((n_kx,) + unit, F32)]
                + [pltpu.VMEM((own, n_ky, width, SUB, width), F32)] * 2
                + [pltpu.VMEM((own * n_ky * SUB, LANES), F32)] + [pltpu.VMEM((width, 24, LANES), F32)] * 2
                + [pltpu.VMEM((width * batch, LANES), F32)] * 4
                + [dma((2, 2))] + [dma((len(GATHER_CHUNKS), 14))] * 2,
                compiler_params=exchange(2 * layer + 1), name='gather')(
                    inv_x, s, real_w, imag_w, source, point_w, p)
            return parts.reshape(groups, ADDENDS, width, CLASS_ROWS[-1], lanes), p

        parts, p = across(f, 0, v)
        v1, f = pl.pallas_call(
            functools.partial(layer_kernel, FIRST_UNIT, True), grid=grid, out_shape=(mid_shape, spec_shape),
            in_specs=[mid_block, part_block] + table_specs(inv + fwd, 'koo'),
            out_specs=(mid_block, anywhere),
            scratch_shapes=[stage(FIRST_UNIT)] * 2 + [pltpu.VMEM(spec_shape.shape, F32), pltpu.SemaphoreType.DMA((groups,))],
            compiler_params=params, name='layer_first')(p, parts, *inv, *fwd)
        parts, p = across(f, 1, v1)
        out = pl.pallas_call(
            functools.partial(layer_kernel, LAST_UNIT, False), grid=(groups, blocks, 2),
            out_shape=jax.ShapeDtypeStruct((x_loc, y_loc, width, grid_z, batch), F32),
            in_specs=[block((1, Y_BLOCK, part_width, grid_z, lanes), 'ijkoo'),
                      block((1, ADDENDS, width, CLASS_ROWS[-1], lanes), 'ioooo')] + table_specs(inv, 'joo'),
            out_specs=block((X_GROUP, Y_BLOCK, part_width, grid_z, batch), 'ijkoo'), scratch_shapes=[stage(LAST_UNIT)],
            compiler_params=params, name='layer_last')(p, parts, *inv)
        return jnp.moveaxis(jnp.swapaxes(out, 2, 3), -1, 0)

    field_spec = P('data', 'xs', 'ys', None, None)
    return jax.shard_map(local_layers, mesh=mesh, in_specs=(field_spec, P(), P(), P(), P()), out_specs=field_spec, check_vma=False)
```

```python
import functools
import math

import jax
import jax.numpy as jnp
import ml_dtypes
import numpy as np
from jax import lax
from jax.experimental import pallas as pl
from jax.experimental.pallas import tpu as pltpu
from jax.sharding import PartitionSpec as P

F32 = jnp.float32
BF16 = jnp.bfloat16
VMEM_LIMIT = 64 * 1024 * 1024 - 65536

SUB = 8
X_GROUP = 8
Y_BLOCK = 4
HALF_BLOCK = 2
Z_BLOCK = 8
KZ_CLASS = ((0, 5), (1, 6, 4), (2, 7, 3))
KZ_ORDER = tuple(kz for group in KZ_CLASS for kz in group)
CLASS_ROWS = (0, 64, 160, 256)
LANES = 128
ADDENDS = 3
CUT = 96
HALF = 0.5
REDUCE_UNITS = (20, 22)
REDUCE_CHUNKS = ((0, 2), (2, 6), (6, 8))
GATHER_CHUNKS = ((0, 4), (4, 6), (6, 8))
MIX_CHUNKS = ((0, 4), (4, 8))
FORWARD_UNIT = (2, 20)
FIRST_UNIT = (2, 10)
LAST_UNIT = (1, 10)
ROOT5_4 = math.sqrt(5.0) / 4.0
SIN_1 = math.sin(2.0 * math.pi / 5.0)
SIN_RATIO = math.sin(4.0 * math.pi / 5.0) / SIN_1


def kz_sign(kz):
    return 0 if kz % 5 == 0 else (1 if kz % 5 < 3 else -1)


def kept(modes, size):
    return np.concatenate([np.arange(modes), np.arange(size - modes, size)])


def pieces(table):
    rest = np.asarray(table, np.float32)
    out = []
    for _ in range(ADDENDS):
        out.append(rest.astype(ml_dtypes.bfloat16))
        rest = rest - out[-1].astype(np.float32)
    return out


def yz_angles(kz, y_pos, ky, grid_y, grid_z):
    z_pos = np.arange(Z_BLOCK)
    turn = (ky[:, None, None] * y_pos[None, :, None] % grid_y) / grid_y + kz * z_pos[None, None, :] / grid_z
    return 2.0 * math.pi * turn


def forward_table(group, y_pos, ky, grid_y, grid_z):
    rows = []
    for kz in group:
        t, s = yz_angles(kz, y_pos, ky, grid_y, grid_z), kz_sign(kz)
        real, imag = [np.cos(t)], [-np.sin(t)]
        if s:
            real.append(-s * SIN_1 * np.sin(t))
            imag.append(-s * SIN_1 * np.cos(t))
        rows += [np.stack(part, 1).reshape(len(ky), -1) for part in (real, imag)]
    return np.concatenate(rows, 0)


def inverse_table(group, y_pos, ky, grid_y, grid_z, points):
    cols = []
    for kz in group:
        t, s = yz_angles(kz, y_pos, ky, grid_y, grid_z).transpose(1, 2, 0), kz_sign(kz)
        w = (HALF if kz == 0 else 1.0) / points
        real, imag = [w * np.cos(t)], [-w * np.sin(t)]
        if s:
            real.append(s * SIN_1 * w * np.sin(t))
            imag.append(s * SIN_1 * w * np.cos(t))
        cols += [np.stack(part, 0).reshape(-1, len(ky)) for part in (real, imag)]
    return np.concatenate(cols, 1)


def all_tables(blocks, ky, grid_y, grid_z, points):
    fwd, inv = [[], [], []], [[], [], [], [], []]
    for block in range(blocks):
        y_pos = np.arange(Y_BLOCK) + block * Y_BLOCK
        for k, group in enumerate(KZ_CLASS):
            a, b, c = pieces(forward_table(group, y_pos, ky, grid_y, grid_z))
            n = np.zeros_like(a)
            if k == 0:
                fwd[k].append(np.concatenate([a, a, a, b, b, c], 1))
            else:
                fwd[k].append(np.block([[a, a, a, b], [c, b, n, n]]))
            a, b, c = pieces(inverse_table(group, y_pos, ky, grid_y, grid_z, points))
            n = np.zeros_like(a)
            if k == 0:
                inv[0].append(np.block([[a, a, a], [b, b, n], [c, n, n]]))
            else:
                inv[2 * k - 1].append(np.block([[a, a], [b, b]]))
                inv[2 * k].append(np.concatenate([c, a], 1))
    return [np.stack(t) for t in fwd], [np.stack(t) for t in inv]


def split3(v):
    d1 = v.astype(BF16)
    rest = v - d1.astype(F32)
    d2 = rest.astype(BF16)
    return d1, d2, (rest - d2.astype(F32)).astype(BF16)


def dot(a, b):
    return jnp.dot(a, b, preferred_element_type=F32)


def z_forward(v):
    v0, v1, v2, v3, v4 = v
    t1, t2, e1, e2 = v1 + v4, v2 + v3, v1 - v4, v2 - v3
    total = t1 + t2
    mid, dif = v0 - 0.25 * total, ROOT5_4 * (t1 - t2)
    return v0 + total, mid + dif, e1 + SIN_RATIO * e2, mid - dif, SIN_RATIO * e1 - e2


def z_inverse(a0, a1, b1, a2, b2):
    total = a1 + a2
    mid, dif = a0 - 0.25 * total, ROOT5_4 * (a1 - a2)
    p, q = mid + dif, mid - dif
    r, s = b1 + SIN_RATIO * b2, SIN_RATIO * b1 - b2
    return a0 + total, p - r, q - s, q + s, p + r


def split_tiles(u_ref, channels):
    rows, lanes = u_ref.shape[1:]
    out = [[], [], []]
    for k in channels:
        for r in range(0, rows, 2 * SUB):
            cells = [split3(u_ref[k, r:r + 2 * SUB, lane:lane + LANES]) for lane in range(0, lanes, LANES)]
            for i in range(ADDENDS):
                out[i].append(jnp.concatenate([cell[i] for cell in cells], -1))
    return [jnp.concatenate(rows, 0) for rows in out]


def add_tiles(o, n, lanes, first=0):
    for r in range(0, n, SUB):
        for lane in range(0, lanes, LANES):
            cells = [o[b + r:b + r + SUB, lane:lane + LANES] for b in range(0, o.shape[0], n)]
            yield r, lane, functools.reduce(jnp.add, cells)


def forward_stage(u_ref, tables, f_ref, c, pair):
    lanes = f_ref.shape[-1]
    for k, channels in enumerate(((0,), (1, 2), (3, 4))):
        d = split_tiles(u_ref, channels)
        o = dot(tables[k], jnp.concatenate([d[i] for i in ((0, 1, 2, 0) if k else (0, 1, 2, 0, 1, 0))], 0))
        n = CLASS_ROWS[k + 1] - CLASS_ROWS[k]
        for r, lane, v in add_tiles(o, n, pair * lanes):
            at = (c + lane // lanes, slice(CLASS_ROWS[k] + r, CLASS_ROWS[k] + r + SUB), slice(lane % lanes, lane % lanes + LANES))
            f_ref[at] += v


def inverse_stage(s_ref, c, pair, tables, u_ref):
    n, lanes = u_ref.shape[1:]

    def part(i, k):
        return jnp.concatenate([s_ref[0, i, c + u, CLASS_ROWS[k]:CLASS_ROWS[k + 1]] for u in range(pair)], -1)
    o = dot(tables[0], jnp.concatenate([part(i, 0) for i in range(ADDENDS)], 0))
    for r, lane, v in add_tiles(o, n, lanes):
        u_ref[0, r:r + SUB, lane:lane + LANES] = v
    for k in (1, 2):
        d1, d2, d3 = (part(i, k) for i in range(ADDENDS))
        o = jnp.concatenate([dot(tables[2 * k - 1], jnp.concatenate([d1, d2], 0)),
                             dot(tables[2 * k], jnp.concatenate([d1, d3], 0))], 0)
        for r, lane, v in add_tiles(o, 2 * n, lanes):
            u_ref[2 * k - 1 + r // n, r % n:r % n + SUB, lane:lane + LANES] = v


def registers(pair, lanes):
    for u in range(pair):
        for y in range(Y_BLOCK):
            for lane in range(0, lanes, LANES):
                yield u, y, lane, (slice(y * SUB, (y + 1) * SUB), slice(u * lanes + lane, u * lanes + lane + LANES))


def gelu(h):
    k = 2.0 * math.sqrt(2.0 / math.pi)
    return h + h * jnp.tanh(h * (k + (4.0 * 0.044715 * k) * (h * h)))


def field_lanes(x_ref, y, c):
    return jnp.concatenate([x_ref[x, y, c] for x in range(X_GROUP)], -1)


def zero_spectrum(f_ref):
    def clear(c, _):
        f_ref[c] = jnp.zeros(f_ref.shape[1:], F32)
        return 0
    lax.fori_loop(0, f_ref.shape[0], clear, 0)


def forward_kernel(unit, x_ref, t0, t1, t2, f_ref, u_ref):
    f_ref = f_ref.at[0]
    width, lanes = x_ref.shape[2], f_ref.shape[-1]
    pair, per_step = unit
    tables = (t0[0], t1[0], t2[0])

    @pl.when(pl.program_id(1) == 0)
    def _():
        zero_spectrum(f_ref)

    def load(c, slot):
        for u in range(pair):
            for y in range(Y_BLOCK):
                row = field_lanes(x_ref, y, c + u)
                for k, v in enumerate(z_forward([row[SUB * j:SUB * j + SUB] for j in range(5)])):
                    u_ref[slot, k, y * SUB:(y + 1) * SUB, u * lanes:(u + 1) * lanes] = v

    def body(i, _):
        c = i * per_step
        count = per_step // pair
        for n in range(count + 1):
            if n < count:
                load(c + n * pair, n)
            if n:
                forward_stage(u_ref.at[n - 1], tables, f_ref, c + (n - 1) * pair, pair)
        return 0
    lax.fori_loop(0, width // per_step, body, 0)


def channel_product(first, x_ref, w_ref, p_ref, d_ref):
    blocks, width, depth, lanes = p_ref.shape
    rows = width * SUB
    ones = jnp.ones((w_ref.shape[-1] + CUT - 2 * rows, blocks * lanes), BF16)
    left = [w_ref[0, i] for i in range(w_ref.shape[1])]

    def load(j):
        z = slice(j * SUB, (j + 1) * SUB)
        if first:
            v = [x_ref[x, y, :, z, :] for y in range(blocks) for x in range(X_GROUP)]
        else:
            v = [x_ref[0, y, :, z, :] for y in range(blocks)]
        d_ref[j % 2] = jnp.concatenate(v, -1).reshape(rows, blocks * lanes)

    def product(j):
        d1, d2, d3 = split3(d_ref[j % 2])
        low, high = jnp.concatenate([d1, d2[:CUT]], 0), jnp.concatenate([d2[CUT:], d3, ones], 0)
        p = functools.reduce(jnp.add, [dot(w, low if i < ADDENDS else high) for i, w in enumerate(left)])
        for y in range(blocks):
            p_ref[y, :, j * SUB:(j + 1) * SUB, :] = p[:, y * lanes:(y + 1) * lanes].reshape(width, SUB, lanes)
    count = depth // SUB
    for j in range(count + 1):
        if j < count:
            load(j)
        if j:
            product(j - 1)


def layer_kernel(unit, first, *refs):
    p_ref, s_ref, *tabs = refs
    p_ref = p_ref.at[0]
    width, lanes = p_ref.shape[1], p_ref.shape[-1]
    batch = lanes // X_GROUP
    if first:
        start = pl.program_id(1) * width
        *tabs, v_ref, f_hbm, a_ref, u_ref, f_all, f_sem = tabs
        v_ref = v_ref.at[0]
        group = pl.program_id(0)
        f_ref = f_all.at[group, pl.ds(start, width)]

        @pl.when(pl.program_id(2) == 0)
        def _():
            zero_spectrum(f_ref)
    else:
        start = pl.program_id(2) * width
        *tabs, o_ref, a_ref = tabs
    inv, fwd = [t[0] for t in tabs[:5]], [t[0] for t in tabs[5:]]
    pair, per_step = unit

    def activate(c, slot):
        kept_rows = {}
        for u, y, lane, at in registers(pair, lanes):
            new = []
            for j, s in enumerate(z_inverse(*(a_ref[(slot, k) + at] for k in range(5)))):
                g = gelu(s + p_ref[y, c + u, SUB * j:SUB * j + SUB, lane:lane + LANES])
                new.append(g)
                if first:
                    v_ref[y, c + u, SUB * j:SUB * j + SUB, lane:lane + LANES] = g
                else:
                    kept_rows[j] = kept_rows.get(j, ()) + (g,)
            if first:
                for k, v in enumerate(z_forward(new)):
                    u_ref[(slot, k) + at] = v
            elif lane + LANES == lanes:
                for j, row in kept_rows.items():
                    store_field(o_ref, y, c + u, SUB * j, row, batch)
                kept_rows = {}

    def body(i, _):
        c = i * per_step
        count = per_step // pair
        for n in range(count + 2):
            if n < count:
                inverse_stage(s_ref, (0 if first else start) + c + n * pair, pair, inv, a_ref.at[n])
            if 0 < n <= count:
                activate(c + (n - 1) * pair, n - 1)
            if first and n > 1:
                forward_stage(u_ref.at[n - 2], fwd, f_ref, c + (n - 2) * pair, pair)
        return 0
    lax.fori_loop(0, width // per_step, body, 0)

    if first:
        @pl.when((pl.program_id(2) == pl.num_programs(2) - 1) & (start > 0))
        def _():
            copies = [pltpu.make_async_copy(f_all.at[g], f_hbm.at[g], f_sem.at[g]) for g in range(f_all.shape[0])]
            for g, copy in enumerate(copies):
                pl.when(group == g)(copy.start)

            @pl.when(group == len(copies) - 1)
            def _():
                for copy in copies:
                    copy.wait()


def store_field(o_ref, y, c, z, row, batch):
    lane = lax.broadcasted_iota(jnp.int32, row[0].shape, 1)
    for x in range(X_GROUP):
        at, off = divmod(x * batch, LANES)
        piece = row[at]
        if off + batch > LANES:
            piece = jnp.where(lane < off, row[at + 1], piece)
        if off:
            piece = pltpu.roll(piece, LANES - off, 1)
        o_ref[x, y, c, z:z + SUB, :] = piece[:, :batch]


def split_dot(left, right):
    a, b, c = left
    d1, d2, d3 = split3(right)
    return dot(a, d1) + dot(a, d2) + dot(a, d3) + dot(b, d1) + dot(b, d2) + dot(c, d1)


def x_forward(m_ref, f_ref, s_ref, slot):
    groups, width, lanes = f_ref.shape[0], f_ref.shape[1], f_ref.shape[-1]
    batch = lanes // X_GROUP
    halves = range(f_ref.shape[4])
    rights = []
    for h in halves:
        rows = []
        for g in range(groups):
            for x in range(X_GROUP):
                for p in range(2):
                    rows.append(jnp.concatenate([f_ref[g, c, 0, p, h, :, x * batch:(x + 1) * batch] for c in range(width)], -1))
        rights.append(jnp.concatenate(rows, 0))
    for h in halves:
        out = split_dot((m_ref[0], m_ref[1], m_ref[2]), rights[h])
        s_ref[:, slot, :, h * SUB:(h + 1) * SUB, :] = out.reshape(s_ref.shape[0], 2, SUB, width * batch)


def x_inverse(m_ref, t_ref, slot, s_ref):
    groups, width, lanes = s_ref.shape[0], s_ref.shape[2], s_ref.shape[-1]
    batch = lanes // X_GROUP
    halves = range(s_ref.shape[5])
    outs = []
    for h in halves:
        right = t_ref[:, slot, :, h * SUB:(h + 1) * SUB, :].reshape(t_ref.shape[0] * 2 * SUB, width * batch)
        outs.append(split_dot((m_ref[0], m_ref[1], m_ref[2]), right).reshape(groups, X_GROUP, 2, SUB, width * batch))
    for h in halves:
        for g in range(groups):
            for p in range(2):
                for c in range(width):
                    row = jnp.concatenate([outs[h][g, x, p, :, c * batch:(c + 1) * batch] for x in range(X_GROUP)], -1)
                    for i, d in enumerate(split3(row)):
                        s_ref[g, i, c, 0, p, h] = d


def mix(s_ref, re_w, im_w, t_ref, to, chunk, rows, re_rows, im_rows, re_s, im_s, re_t, im_t):
    own, _, _, n_ky, lanes = s_ref.shape
    width = re_w.shape[2]
    batch = lanes // width
    some = chunk[1] - chunk[0]
    part_modes = some * n_ky
    pick, modes = slice(*chunk), slice(0, own * part_modes)

    for w_ref, out in ((re_w, re_rows), (im_w, im_rows)):
        def lay(c, _):
            for k in range(own):
                for ky in range(n_ky):
                    at = (k * n_ky + ky) * SUB
                    rows[at:at + SUB, 0:width] = w_ref[k, ky, c]
            mat = jnp.concatenate([rows[pl.ds((k * n_ky + h * SUB) * SUB + kz, SUB, stride=SUB), :]
                                   for k in range(own) for kz in KZ_ORDER[pick] for h in range(n_ky // SUB)], 0)
            out[c, :, modes] = mat.T[0:out.shape[1]]
            return 0
        lax.fori_loop(0, width, lay, 0)
    for p, out in enumerate((re_s, im_s)):
        out[:, modes] = jnp.concatenate([s_ref[k, pick, p].reshape(part_modes, lanes) for k in range(own)], 0).T
    pair = 1

    def outputs(i, _):
        d = i * pair

        def inner(c, acc):
            at = pl.ds(pl.multiple_of(c * batch, SUB), batch)
            a, b = re_s[at, modes], im_s[at, modes]
            new = []
            for u in range(pair):
                p = jnp.broadcast_to(re_rows[c, pl.ds(d + u, 1), modes], a.shape)
                q = jnp.broadcast_to(im_rows[c, pl.ds(d + u, 1), modes], a.shape)
                new += [acc[2 * u] + (a * p - b * q), acc[2 * u + 1] + (a * q + b * p)]
            return tuple(new)
        zero = jnp.zeros((batch, own * part_modes), F32)
        acc = lax.fori_loop(0, width, inner, (zero,) * (2 * pair), unroll=True)
        for u in range(pair):
            at = pl.ds(pl.multiple_of((d + u) * batch, SUB), batch)
            re_t[at, modes] = acc[2 * u]
            im_t[at, modes] = acc[2 * u + 1]
        return 0
    lax.fori_loop(0, width // pair, outputs, 0)
    for p, got in enumerate((re_t, im_t)):
        back = got[:, modes].T
        for k in range(own):
            t_ref[to[k], pick, p] = back[k * part_modes:(k + 1) * part_modes].reshape(some, n_ky, lanes)


class Place:
    def __init__(self):
        xs, ys = lax.axis_index('xs'), lax.axis_index('ys')
        data = lax.axis_index('data')
        c, x, y = xs % 2, xs // 2, ys
        self.core = (data, ys, 2 * x + 1 - c)
        self.x_chip = (data, ys, 2 * (1 - x) + c)
        self.y_chip = (data, 1 - ys, xs)
        p, q = lambda a, b: 2 * a + b, lambda a, b: 4 + 2 * a + b
        self.mine = SUB * c
        self.table = 2 * xs + ys
        self.order = (p(1 - x, 1 - y), q(1 - y, 1 - x), p(1 - x, y), q(1 - y, x),
                      p(x, 1 - y), q(y, 1 - x), p(x, y), q(y, x))

    def enter(self):
        barrier = pltpu.get_barrier_semaphore()
        for device in (self.core, self.x_chip, self.y_chip):
            pl.semaphore_signal(barrier, inc=1, device_id=device, device_id_type=pl.DeviceIdType.MESH)
        pl.semaphore_wait(barrier, 3)


def remote(src, dst, send, recv, device):
    return pltpu.make_async_remote_copy(src_ref=src, dst_ref=dst, send_sem=send, recv_sem=recv, device_id=device,
                                        device_id_type=pl.DeviceIdType.MESH)


def step_and_last():
    return pl.program_id(0), pl.num_programs(0) - 1


def chunk_of(ref, k, chunk):
    low, high = chunk
    return ref.at[k, pl.ds(low, high - low)]


def reduce_kernel(first, m_hbm, f_ref, x_ref, w_ref, out_ref, p_ref, m_ref, m_sem, d_ref, s_ref, r1, r2, r3,
                  send1, recv1, send2, recv2, send3, recv3):
    me = Place()
    step, last = step_and_last()
    slots = s_ref.shape[1]
    two, three = [], []

    def to_core(slot):
        return [remote(s_ref.at[SUB + me.order[t], slot], r1.at[t, slot], send1.at[slot, t], recv1.at[slot, t], me.core)
                for t in range(SUB)]
    for h, chunk in enumerate(REDUCE_CHUNKS):
        mine = [chunk_of(s_ref, k, chunk) for k in me.order]
        two.append([remote(mine[t], chunk_of(r2, t, chunk), send2.at[h, t], recv2.at[h, t], (me.x_chip, me.y_chip)[t % 2])
                    for t in range(4)])
        three.append([remote(mine[4 + t], chunk_of(r3, t, chunk), send3.at[h, t], recv3.at[h, t], (me.y_chip, me.x_chip)[t])
                      for t in range(2)])

    def add(dst, a, b):
        def row(i, _):
            dst[i] = a[i] + b[i]
            return 0
        lax.fori_loop(0, dst.shape[0], row, 0)

    def from_core(h):
        arriving = [to_core(slot) for slot in range(*REDUCE_CHUNKS[h])]
        for t in range(SUB):
            for copies in arriving:
                copies[t].wait_recv()
            to = chunk_of(s_ref, me.order[t], REDUCE_CHUNKS[h])
            add(to, to, chunk_of(r1, t, REDUCE_CHUNKS[h]))
            if t < len(two[h]):
                two[h][t].start()

    def from_chip(h, these=(0, 1)):
        for t in these:
            two[h][t].wait_recv()
            to = chunk_of(s_ref, me.order[4 + t], REDUCE_CHUNKS[h])
            add(to, to, chunk_of(r2, t, REDUCE_CHUNKS[h]))
            if t < len(three[h]):
                three[h][t].start()

    def finish(h):
        from_chip(h, (2, 3))
        for t in range(2):
            three[h][t].wait_recv()
            add(*(chunk_of(ref, k, REDUCE_CHUNKS[h]) for ref, k in ((out_ref, t), (s_ref, me.order[6 + t]), (r3, t))))

    def begin():
        table = pltpu.make_async_copy(m_hbm.at[me.table], m_ref, m_sem)
        table.start()
        me.enter()
        table.wait()

    events = ((0, begin), (2, lambda: from_core(0)), (slots - 3, lambda: from_chip(0)), (slots - 2, lambda: from_core(1)),
              (slots, lambda: from_core(2)), (slots + 3, lambda: finish(0)), (slots + 5, lambda: from_chip(1)),
              (slots + 12, lambda: from_chip(2)))
    for at, event in events:
        pl.when(step == at)(event)

    @pl.when(step < slots)
    def _():
        x_forward(m_ref, f_ref, s_ref, step)
        for copy in to_core(step):
            copy.start()

    @pl.when(step >= slots)
    def _():
        channel_product(first, x_ref, w_ref, p_ref.at[0], d_ref)

    @pl.when(step == last)
    def _():
        finish(1)
        finish(2)
        for copies in [to_core(slot) for slot in range(slots)] + two + three:
            for copy in copies:
                copy.wait_send()


def gather_kernel(first, layer, m_hbm, s_ref, re_hbm, im_hbm, x_ref, w_ref, p_in, parts_ref, p_ref, m_ref, m_sem, d_ref, t_ref,
                  re_w, im_w, rows, re_rows, im_rows, re_s, im_s, re_t, im_t, w_sem, send_sem, recv_sem):
    me = Place()
    step, last = step_and_last()
    p3, q3, p2, q2, p1, q1, p0, q0 = me.order
    plan = [(p0, me.y_chip, 0), (q0, me.x_chip, 0), (p0, me.x_chip, 0), (q0, me.y_chip, 0), (p0, me.core, SUB), (q0, me.core, SUB),
            (p1, me.x_chip, 0), (q1, me.y_chip, 0)] + [(k, me.core, SUB) for k in (p1, q1, p2, q2, p3, q3)]
    copies = [[remote(chunk_of(t_ref, k, chunk), chunk_of(t_ref, k + up, chunk), send_sem.at[h, n], recv_sem.at[h, n], device)
               for n, (k, device, up) in enumerate(plan)] for h, chunk in enumerate(GATHER_CHUNKS)]
    weights = [pltpu.make_async_copy(hbm.at[layer, me.mine + k], to.at[i], w_sem.at[n, i])
               for n, (hbm, to) in enumerate(((re_hbm, re_w), (im_hbm, im_w))) for i, k in enumerate((p0, q0))]
    weights.append(pltpu.make_async_copy(m_hbm.at[me.table], m_ref, m_sem))

    def mixed(h):
        mix(s_ref, re_w, im_w, t_ref, (p0, q0), MIX_CHUNKS[h], rows, re_rows, im_rows, re_s, im_s, re_t, im_t)

    def send(h):
        for copy in copies[h][:6]:
            copy.start()

    def begin():
        for copy in weights:
            copy.start()
        me.enter()
        for copy in weights:
            copy.wait()
        mixed(0)
        send(0)

    def follow(h):
        pass_on(h)
        send(h + 1)

    def pass_on(h):
        for n in range(2):
            copies[h][n].wait_recv()
            copies[h][6 + n].start()
            copies[h][SUB + n].start()

    def finish(h):
        for n, arrived in enumerate((2, 3, 6, 7)):
            copies[h][arrived].wait_recv()
            copies[h][10 + n].start()
        for n in (4, 5, *range(SUB, len(plan))):
            copies[h][n].wait_recv()

    x_from = last + 1 - t_ref.shape[1]
    for at, event in ((0, begin), (1, lambda: mixed(1)), (5, lambda: follow(0)), (x_from, lambda: finish(0)),
                      (x_from + 1, lambda: follow(1)), (x_from + 4, lambda: finish(1)), (x_from + 5, lambda: pass_on(2)),
                      (x_from + 6, lambda: finish(2))):
        pl.when(step == at)(event)

    @pl.when((step >= 2) & (step < x_from + 4))
    def _():
        channel_product(first, x_ref, w_ref, p_ref.at[0], d_ref)

    @pl.when(step >= x_from)
    def _():
        x_inverse(m_ref, t_ref, step - x_from, parts_ref)

    @pl.when(step == last)
    def _():
        for some in copies:
            for copy in some:
                copy.wait_send()


def block(shape, index, slot=None, **kwargs):
    def index_map(*at):
        return tuple(0 if k == 'o' else slot(at[0]) if k == 's' else at['ijk'.index(k)] for k in index)
    return pl.BlockSpec(shape, index_map, **kwargs)


def point_table_kernel(w_ref, b_ref, out_ref):
    layers, width = b_ref.shape
    rows = width * SUB

    def spread(shape, axis):
        at = [lax.broadcasted_iota(jnp.int32, shape, k) for k in range(2)]
        return jnp.where(at[axis] // SUB == at[1 - axis], 1.0, 0.0).astype(BF16)
    down, across = spread((rows, width), 0), spread((width, rows), 1)
    at = [lax.broadcasted_iota(jnp.int32, (rows, rows), k) % SUB for k in range(2)]
    column = lax.broadcasted_iota(jnp.int32, (rows, out_ref.shape[-1] + CUT - 2 * rows), 1)
    for layer in range(layers):
        weights, biases = split3(HALF * w_ref[layer].T), split3(HALF * b_ref[layer:layer + 1])
        shift = sum(jnp.where(column == i, jnp.sum(down.astype(F32) * b.astype(F32), 1, keepdims=True), 0.0)
                    for i, b in enumerate(biases))
        a, b, c = (jnp.where(at[0] == at[1], dot(dot(down, w).astype(BF16), across), 0.0) for w in weights)
        none = jnp.zeros_like(a)
        for i, parts in enumerate(((a, a[:, :CUT]), (b, b[:, :CUT]), (c, none[:, :CUT]),
                                   (a[:, CUT:], a, shift), (b[:, CUT:], none, jnp.zeros_like(shift)))):
            out_ref[layer, i] = jnp.concatenate(parts, 1).astype(BF16)


def solution(mesh):
    row_devs, col_devs = mesh.shape['ys'], mesh.shape['xs']

    def local_layers(field, spec_real, spec_imag, mix_weight, bias):
        batch, x_loc, y_loc, grid_z, width = field.shape
        modes = spec_real.shape[3]
        grid_x, grid_y = x_loc * col_devs, y_loc * row_devs
        groups, blocks = x_loc // X_GROUP, y_loc // Y_BLOCK
        lanes = X_GROUP * batch
        kx, ky = kept(modes, grid_x), kept(modes, grid_y)
        n_kx, n_ky = len(kx), len(ky)
        fwd_np, inv_np = all_tables(blocks, ky, grid_y, grid_z, grid_x * grid_y * grid_z)
        fwd, inv = [jnp.asarray(t) for t in fwd_np], [jnp.asarray(t) for t in inv_np]

        turn = 2.0 * math.pi * (kx[:, None] * np.arange(grid_x)[None, :] % grid_x) / grid_x
        cos, sin = np.cos(turn), np.sin(turn)
        fwd_x = np.stack([np.stack([cos, sin], -1), np.stack([-sin, cos], -1)], 1)
        inv_x = np.transpose(fwd_x, (2, 3, 0, 1))
        fwd_x = fwd_x.reshape(n_kx, 2, col_devs, x_loc, 2).transpose(2, 0, 1, 3, 4).reshape(col_devs, 2 * n_kx, 2 * x_loc)
        inv_x = inv_x.reshape(col_devs, 2 * x_loc, 2 * n_kx)
        odd_rows = np.where(np.arange(2 * SUB * x_loc) % 2, -1.0, 1.0)[:, None]

        def x_tables(tables, axis):
            out = []
            for xs in range(col_devs):
                t = np.roll(np.kron(tables[xs], np.eye(SUB)), SUB * n_kx * (xs % 2), axis)
                out += [np.stack(pieces(t * sign)) for sign in (1.0, odd_rows)]
            return jnp.asarray(np.stack(out))
        fwd_x, inv_x = x_tables(fwd_x, 0), x_tables(inv_x, 1)
        params = pltpu.CompilerParams(vmem_limit_bytes=VMEM_LIMIT)
        point_w = pl.pallas_call(
            point_table_kernel, out_shape=jax.ShapeDtypeStruct((2, 5, width * SUB, width * SUB + CUT), BF16),
            compiler_params=params, name='point_table')(mix_weight, bias)

        real_w, imag_w = (jnp.swapaxes(w, 3, 4) for w in (spec_real, spec_imag))
        v = jnp.swapaxes(jnp.moveaxis(field, 0, -1), 2, 3)
        grid = (groups, 2, blocks)
        part_width = width // 2
        spec_shape = jax.ShapeDtypeStruct((groups, width, 256, lanes), F32)
        mid_block = block((1, Y_BLOCK, part_width, grid_z, lanes), 'ikjoo')
        part_block = block((1, ADDENDS, part_width, CLASS_ROWS[-1], lanes), 'iojoo')
        mid_shape = jax.ShapeDtypeStruct((groups, y_loc, width, grid_z, lanes), F32)
        anywhere = pl.BlockSpec(memory_space=pl.ANY)

        def stage(unit):
            return pltpu.VMEM((unit[1] // unit[0], 5, Y_BLOCK * SUB, unit[0] * lanes), F32)

        units = y_loc // HALF_BLOCK

        def unit_block(first, steps, base, count):
            shape = (HALF_BLOCK, width, grid_z) + ((batch,) if first else (lanes,))

            def index_map(j):
                n = jnp.clip(j - steps, 0, count - 1) + base
                return n // units, n % units, *(0,) * len(shape[1:])
            return pl.BlockSpec((X_GROUP if first else 1,) + shape, index_map)

        def table_specs(tables, index):
            return [block((1,) + t.shape[1:], index) for t in tables]

        f = pl.pallas_call(
            functools.partial(forward_kernel, FORWARD_UNIT), grid=(groups, blocks), out_shape=spec_shape,
            in_specs=[block((X_GROUP, Y_BLOCK, width, grid_z, batch), 'ijooo')] + table_specs(fwd, 'joo'),
            out_specs=block((1, width, 256, lanes), 'iooo'),
            scratch_shapes=[stage(FORWARD_UNIT)], compiler_params=params, name='forward')(v, *fwd)

        own, slots, halves = 2, SUB, n_ky // SUB
        unit = (slots, 2, n_ky, width * batch)
        own_block = block((own,) + unit, 'ooooo')

        def w_block(layer):
            return block((1,) + point_w.shape[1:], 'sooo', lambda j: layer)
        dma = pltpu.SemaphoreType.DMA
        x_scratch = [pltpu.VMEM(fwd_x.shape[1:], BF16), dma]
        half_rows = pltpu.VMEM((2, width * SUB, HALF_BLOCK * lanes), F32)

        def exchange(number):
            return pltpu.CompilerParams(vmem_limit_bytes=VMEM_LIMIT, collective_id=number, has_side_effects=True)

        def across(f, layer, source):
            first, early = layer == 0, REDUCE_UNITS[layer]
            late = groups * units - early
            s, p = pl.pallas_call(
                functools.partial(reduce_kernel, first), grid=(slots + early,),
                out_shape=(jax.ShapeDtypeStruct((own,) + unit, F32), mid_shape),
                in_specs=[anywhere,
                          block((groups, width, 1, 2, halves, SUB, lanes), 'oosoooo', lambda j: jnp.minimum(j, slots - 1)),
                          unit_block(first, slots, 0, early), w_block(layer)],
                out_specs=(own_block, unit_block(False, slots, 0, early)),
                scratch_shapes=x_scratch + [half_rows] + [pltpu.VMEM((n,) + unit, F32) for n in (n_kx, SUB, 4, 2)]
                + [dma((slots, SUB))] * 2 + [dma((len(REDUCE_CHUNKS), n)) for n in (4, 4, 2, 2)],
                compiler_params=exchange(2 * layer), name='reduce')(
                    fwd_x, f.reshape(groups, width, slots, 2, halves, SUB, lanes), source, point_w)
            parts, p = pl.pallas_call(
                functools.partial(gather_kernel, first, layer), grid=(late + 6,),
                out_shape=(jax.ShapeDtypeStruct((groups, ADDENDS, width, slots, 2, halves, SUB, lanes), BF16), mid_shape),
                in_specs=[anywhere, own_block, anywhere, anywhere, unit_block(first, 2, early, late), w_block(layer), anywhere],
                out_specs=(block((groups, ADDENDS, width, 1, 2, halves, SUB, lanes), 'ooosoooo', lambda j: jnp.maximum(j - late + 2, 0)),
                           unit_block(False, 2, early, late)),
                input_output_aliases={6: 1},
                scratch_shapes=x_scratch + [half_rows, pltpu.VMEM((n_kx,) + unit, F32)]
                + [pltpu.VMEM((own, n_ky, width, SUB, width), F32)] * 2
                + [pltpu.VMEM((own * n_ky * SUB, LANES), F32)] + [pltpu.VMEM((width, 24, LANES), F32)] * 2
                + [pltpu.VMEM((width * batch, LANES), F32)] * 4
                + [dma((2, 2))] + [dma((len(GATHER_CHUNKS), 14))] * 2,
                compiler_params=exchange(2 * layer + 1), name='gather')(
                    inv_x, s, real_w, imag_w, source, point_w, p)
            return parts.reshape(groups, ADDENDS, width, CLASS_ROWS[-1], lanes), p

        parts, p = across(f, 0, v)
        v1, f = pl.pallas_call(
            functools.partial(layer_kernel, FIRST_UNIT, True), grid=grid, out_shape=(mid_shape, spec_shape),
            in_specs=[mid_block, part_block] + table_specs(inv + fwd, 'koo'),
            out_specs=(mid_block, anywhere),
            scratch_shapes=[stage(FIRST_UNIT)] * 2 + [pltpu.VMEM(spec_shape.shape, F32), pltpu.SemaphoreType.DMA((groups,))],
            compiler_params=params, name='layer_first')(p, parts, *inv, *fwd)
        parts, p = across(f, 1, v1)
        out = pl.pallas_call(
            functools.partial(layer_kernel, LAST_UNIT, False), grid=(groups, blocks, 2),
            out_shape=jax.ShapeDtypeStruct((x_loc, y_loc, width, grid_z, batch), F32),
            in_specs=[block((1, Y_BLOCK, part_width, grid_z, lanes), 'ijkoo'),
                      block((1, ADDENDS, width, CLASS_ROWS[-1], lanes), 'ioooo')] + table_specs(inv, 'joo'),
            out_specs=block((X_GROUP, Y_BLOCK, part_width, grid_z, batch), 'ijkoo'), scratch_shapes=[stage(LAST_UNIT)],
            compiler_params=params, name='layer_last')(p, parts, *inv)
        return jnp.moveaxis(jnp.swapaxes(out, 2, 3), -1, 0)

    field_spec = P('data', 'xs', 'ys', None, None)
    return jax.shard_map(local_layers, mesh=mesh, in_specs=(field_spec, P(), P(), P(), P()), out_specs=field_spec, check_vma=False)
```
